32 devices in a mesh: gx: 4 (over x, core), gy: 4 (over z), gz: 2 (over y).
Axes of the slice: x: 2, y: 2, z: 4, core: 2. Of those that a mesh axis runs over, the one named last changes fastest.
Arguments:
- occupied: float32 [16, 16, 16, 256], P(None, 'gx', 'gy', 'gz'), may hold values from -6 to 6
- virtual: float32 [16, 16, 16, 256], P(None, 'gx', 'gy', 'gz'), may hold values from -6 to 6
- kernel_fields: float32 [4, 16, 16, 256], P(None, 'gx', 'gy', 'gz'), may hold values from -1.5 to 1.5
- density_grad: float32 [3, 16, 16, 256], P(None, 'gx', 'gy', 'gz'), may hold values from -6 to 6
Outputs:
- potential: float32 [256, 16, 16, 256], P(None, 'gx', 'gy', 'gz')
- casida: float32 [256, 256], P(('gx', 'gy', 'gz'))
The draws below stay inside these ranges and needn't reach their ends.
All inputs are finite; a program needn't handle non-finite values.
Results may differ from the reference program's by a relative error of at most 0.00013.
Values sent between devices are 32-bit elements; how exact they have to be, the bound alone decides.
A program may use at most 64 MiB of HBM per device.

```python
import jax
import jax.numpy as jnp
from jax import lax

NOCC = 16
NVIR = 16
NX = 16
NY = 16
NZ = 256


def steps_of(rng, extent, split, low, high):
    loudness = 1.0
    for axis_at, blocks in split:
        steps = jax.random.uniform(jax.random.fold_in(jax.random.fold_in(rng, 6), axis_at), (blocks,), jnp.float32, low / len(split), high / len(split))
        loudness = loudness * jnp.repeat(jnp.exp(steps), extent[axis_at] // blocks).reshape((-1,) + (1,) * (len(extent) - 1 - axis_at))
    return loudness


def scatter_about(own_key, extent, scale, most, split=(), held_as=jnp.bfloat16):
    gain = steps_of(own_key, extent, split, -0.22, 0.18) if split else 1.0
    array = jax.random.normal(own_key, extent, jnp.float32) * scale * gain
    return jnp.minimum(jnp.maximum(array, -most), most).astype(held_as)


def setup_inputs(seed: int = 0) -> dict:
    keys = jax.random.split(jax.random.key(seed), 5)
    occupied = scatter_about(keys[0], (NOCC, NX, NY, NZ), 1.0, 6.0, ((1, 4), (2, 4), (3, 2)), jnp.float32)
    virtual = scatter_about(keys[1], (NVIR, NX, NY, NZ), 1.0, 6.0, ((1, 4), (2, 4), (3, 2)), jnp.float32)
    kernel_fields = jnp.clip(jax.random.uniform(keys[2], (4, NX, NY, NZ), jnp.float32, -1.5, 1.5) * steps_of(keys[2], (4, NX, NY, NZ), ((1, 4), (2, 4), (3, 2)), -0.4, 0.0), -1.5, 1.5)
    density_grad = scatter_about(keys[3], (3, NX, NY, NZ), 1.0, 6.0, ((1, 4), (2, 4), (3, 2)), jnp.float32)
    return {"occupied": occupied, "virtual": virtual, "kernel_fields": kernel_fields, "density_grad": density_grad}


def derivative(values, dimension):
    inner_diff = jnp.roll(values, -1, dimension) - jnp.roll(values, 1, dimension)
    outer_diff = jnp.roll(values, -2, dimension) - jnp.roll(values, 2, dimension)
    return (8.0 * inner_diff - outer_diff) / 12.0


def respond(densities, kernel_fields, density_grad):
    slopes = [derivative(densities, dimension + 1) for dimension in range(3)]
    aligned = density_grad[0] * slopes[0] + density_grad[1] * slopes[1] + density_grad[2] * slopes[2]
    scalar = kernel_fields[1] * densities + kernel_fields[2] * aligned
    fluxes = [scalar * density_grad[dimension] + kernel_fields[3] * slopes[dimension] for dimension in range(3)]
    divergence = derivative(fluxes[0], 1) + derivative(fluxes[1], 2) + derivative(fluxes[2], 3)
    return kernel_fields[0] * densities + kernel_fields[1] * aligned - divergence


def reference(occupied, virtual, kernel_fields, density_grad):
    def pair_block(orbital):
        return respond(orbital[None] * virtual, kernel_fields, density_grad)

    potential = lax.map(pair_block, occupied).reshape((NOCC * NVIR, NX, NY, NZ))
    flat_potential = potential.reshape((NOCC * NVIR, NX * NY * NZ))

    def rows_of(orbital):
        densities = (orbital[None] * virtual).reshape((NVIR, NX * NY * NZ))
        return lax.dot_general(densities, flat_potential, (((1,), (1,)), ((), ())), precision=lax.Precision.HIGHEST, preferred_element_type=jnp.float32)

    casida = lax.map(rows_of, occupied).reshape((NOCC * NVIR, NOCC * NVIR)) * (1.0 / (NX * NY * NZ))
    return potential, casida
```

```python
import functools

import jax
import jax.numpy as jnp
from jax import lax
from jax.experimental import pallas as pl
from jax.experimental.pallas import tpu as pltpu
from jax.sharding import PartitionSpec as P

MESH = pl.DeviceIdType.MESH
F32 = jnp.float32
BF16 = jnp.bfloat16
SHIFTS = (1, -1, 2, -2)
MIB = 1024 * 1024


def difference(f):
    return 8.0 * (f(1) - f(-1)) - (f(2) - f(-2))


def lanes_of(shape):
    return lax.broadcasted_iota(jnp.int32, shape, len(shape) - 1)


def edge_terms(gap, lane):
    axis = gap.ndim - 1
    lanes = gap.shape[axis]
    at = lane & 3
    two = jnp.where(at >= 2, -pltpu.roll(gap, lanes - 2, axis), pltpu.roll(gap, 2, axis))
    one = jnp.where(at == 3, pltpu.roll(gap, lanes - 1, axis), -pltpu.roll(gap, 1, axis))
    return two + jnp.where((at == 3) | (at == 0), 8.0 * one, 0.0)


def split(v):
    hi = v.astype(BF16)
    return hi, (v - hi.astype(F32)).astype(BF16)


def dot(a, b):
    return lax.dot_general(a, b, (((1,), (1,)), ((), ())), preferred_element_type=F32)


def flow_kernel(
    occ_in, vir_in, ker_in, grd_in,
    f0, f1, base, corr, cas,
    occ, vir, ker, grd, W, N, oS, vS, S0, S2, AL, C, A0, A1,
    pk, wz, pkn, px, py, E2, ez, L, S1a, S1b, Rha, Rla, Rhb, Rlb, LE, RE, RL,
    acc, part, got, acc2, got2,
    send, recv, own, send1, recv1, send2, recv2,
):
    nx, ny, nz = (lax.axis_size(a) for a in ("gx", "gy", "gz"))
    gx, gy, gz = (lax.axis_index(a) for a in ("gx", "gy", "gz"))
    bx, by = base.shape[0], base.shape[1]
    cells = bx * by
    lanes = occ.shape[1]
    half = lanes // 2
    nocc, nvir = occ.shape[0] // cells, vir.shape[0] // cells
    pairs = nocc * nvir
    rows_out = cas.shape[0]
    n_plane = nx * nz
    me = gx * nz + gz

    def plane(d):
        t = lax.rem(me + d, n_plane)
        tx, tz = t // nz, lax.rem(t, nz)
        return tx, tz, {"gx": tx, "gy": gy, "gz": tz}

    def column(d):
        t = lax.rem(gy + d, ny)
        return t, {"gx": gx, "gy": t, "gz": gz}

    def beside(axis, side):
        v, n = {"gx": (gx, nx), "gy": (gy, ny), "gz": (gz, nz)}[axis]
        where = {"gx": gx, "gy": gy, "gz": gz}
        where[axis] = lax.rem(v + 1, n) if side == 0 else lax.rem(v + n - 1, n)
        return where

    taken = [
        pltpu.make_async_copy(a, b, own.at[k])
        for k, (a, b) in enumerate(((occ_in, occ), (vir_in, vir), (ker_in, ker), (grd_in, grd)))
    ]
    for c in taken:
        c.start()
    barrier = pltpu.get_barrier_semaphore()
    for d in range(1, n_plane):
        pl.semaphore_signal(barrier, inc=1, device_id=plane(d)[2], device_id_type=MESH)
    for d in range(1, ny):
        pl.semaphore_signal(barrier, inc=1, device_id=column(d)[1], device_id_type=MESH)

    acc[...] = jnp.zeros_like(acc)
    for r in (Rhb, Rlb):
        r[...] = jnp.zeros_like(r)
    S1b[...] = jnp.zeros_like(S1b)
    L[0, 1] = jnp.zeros_like(L[0, 1])
    E2[...] = jnp.zeros_like(E2)
    lane = lanes_of((nvir, lanes))
    lane1 = lanes_of((1, lanes))
    at_edge = (lane < 2) | (lane >= lanes - 2)
    slot = lax.rem((lane + 2) // 4, lanes // 4)

    for c in taken:
        c.wait()
    packed = jnp.zeros((nocc, lanes), F32)
    for c in range(cells):
        x, y = divmod(c, by)
        o = occ[pl.ds(c, nocc, stride=cells), :]
        v = vir[pl.ds(c, nvir, stride=cells), :]
        W[x + 4, y + 4, 0:nocc] = o
        W[x + 4, y + 4, nocc:nocc + nvir] = v
        packed += pltpu.roll(jnp.where(at_edge, o, 0.0), 4 * c, 1)
        packed += pltpu.roll(jnp.where(at_edge, v, 0.0), 4 * c + half, 1)
        g = [grd[pl.ds(k * cells + c, 1), :] for k in range(3)]
        f = [ker[pl.ds(k * cells + c, 1), :] for k in range(4)]
        k1, k2, k3 = f[1] * (1.0 / 12.0), f[2] * (1.0 / 144.0), f[3] * (1.0 / 144.0)
        C[x, y] = jnp.concatenate(g + [k1, k2, k3, f[0], f[0]], axis=0)
        for m, ref in ((0, A0.at[x + 2, y]), (1, A1.at[x, y + 2])):
            q = k2 * g[m]
            a = [q * g[k] + k3 if k == m else q * g[k] for k in range(3)]
            ref[...] = jnp.concatenate(a + [k1 * g[m]], axis=0)
    pk[...] = packed
    pl.semaphore_wait(barrier, n_plane - 1 + ny - 1)

    copies = []

    def put(src, dst, device):
        k = len(copies)
        c = pltpu.make_async_remote_copy(
            src_ref=src, dst_ref=dst, send_sem=send.at[k], recv_sem=recv.at[k],
            device_id=device, device_id_type=MESH,
        )
        c.start()
        copies.append(c)
        return c

    in_x, in_y = pl.ds(4, bx), pl.ds(4, by)

    def near_src(b, side):
        return pl.ds(b + 2, 2) if side == 0 else pl.ds(4, 2)

    def near_dst(b, side):
        return pl.ds(2, 2) if side == 0 else pl.ds(b + 4, 2)

    def far_src(b, side):
        return pl.ds(b, 2) if side == 0 else pl.ds(6, 2)

    def far_dst(b, side):
        return pl.ds(0, 2) if side == 0 else pl.ds(b + 6, 2)

    def arm_src(b, side):
        return pl.ds(b, 2) if side == 0 else pl.ds(2, 2)

    def arm_dst(b, side):
        return pl.ds(0, 2) if side == 0 else pl.ds(b + 2, 2)

    zsides = range(1 if nz == 2 else 2)
    both = range(2)
    near_y = [
        put(W.at[in_x, near_src(by, s)], W.at[in_x, near_dst(by, s)], beside("gy", s)) for s in both
    ]
    z_in = [put(pk, wz.at[s], beside("gz", s)) for s in zsides]
    near_x = [
        put(W.at[near_src(bx, s), in_y], W.at[near_dst(bx, s), in_y], beside("gx", s)) for s in both
    ]
    arm_x = [put(A0.at[arm_src(bx, s)], A0.at[arm_dst(bx, s)], beside("gx", s)) for s in both]
    arm_y = [
        put(A1.at[:, arm_src(by, s)], A1.at[:, arm_dst(by, s)], beside("gy", s)) for s in both
    ]
    far_x = [
        put(W.at[far_src(bx, s), in_y], W.at[far_dst(bx, s), in_y], beside("gx", s)) for s in both
    ]
    far_y = [
        put(W.at[in_x, far_src(by, s)], W.at[in_x, far_dst(by, s)], beside("gy", s)) for s in both
    ]

    def multiply(count, place):
        def body(t, carry):
            x, y = place(t)
            v = W[x, y, nocc:nocc + nvir]
            for i in range(nocc):
                N[x, y, i] = W[x, y, i:i + 1] * v
            return carry

        lax.fori_loop(0, count, body, 0)

    def rim(t, b, lo, hi):
        return jnp.where(t < 2, t + lo, t + hi)

    multiply(cells, lambda t: (4 + t // by, 4 + lax.rem(t, by)))

    for c in z_in:
        c.wait_recv()
    low = (lanes_of((nocc, lanes)) & 3) < 2
    z_edges = wz[0] if nz == 2 else jnp.where(low, wz[1], wz[0])
    pkn[...] = z_edges
    turn_x = [put(pkn, px.at[s], beside("gx", s)) for s in both]
    turn_y = [put(pkn, py.at[s], beside("gy", s)) for s in both]

    def prepare(x, y, edges, c, fold):
        ao = pltpu.roll(edges, lax.rem(lanes - 4 * c, lanes), 1)
        av = pltpu.roll(edges, lax.rem(lanes + half - 4 * c, lanes), 1)
        o_own, v_own = W[x, y, 0:nocc], W[x, y, nocc:nocc + nvir]
        for k, s in enumerate(SHIFTS):
            m = lane < s if s > 0 else lane >= lanes + s
            scale = 8.0 if abs(s) == 1 else 1.0
            factor = scale if fold is None else scale * fold
            oS[k, x - 2, y - 2] = factor * pltpu.roll(jnp.where(m, ao, o_own), (-s) % lanes, 1)
            vS[k, x - 2, y - 2] = pltpu.roll(jnp.where(m, av, v_own), (-s) % lanes, 1)

    def prepare_center(t, carry):
        prepare(4 + t // by, 4 + lax.rem(t, by), pkn[...], t, None)
        return carry

    lax.fori_loop(0, cells, prepare_center, 0, unroll=2)

    own_o, own_v = pk[...], pltpu.roll(pk[...], half, 1)
    nb_o, nb_v = z_edges, pltpu.roll(z_edges, half, 1)
    for i in range(nocc):
        gap = nb_o[i:i + 1] * nb_v - own_o[i:i + 1] * own_v
        e = jnp.where(slot < cells, edge_terms(gap, lane), 0.0)
        hi, lo = split(e)
        LE[i * nvir:(i + 1) * nvir] = hi
        LE[pairs + i * nvir:pairs + (i + 1) * nvir] = lo

    for c in near_x:
        c.wait_recv()
    multiply(4 * by, lambda t: (rim(t // by, bx, 2, bx + 2), 4 + lax.rem(t, by)))

    def slope_z(x, y, i, shifted):
        p = [oS[k, x - 2, y - 2, i:i + 1] * shifted[k] for k in range(4)]
        return (p[0] - p[1]) - (p[2] - p[3])

    def first_pass(x, carry):
        for y in range(by):
            g0, g2 = C[x, y, 0:1], C[x, y, 2:3]
            shifted = [vS[k, x + 2, y + 2] for k in range(4)]
            h, at = y // 2, (y % 2) * 2 * lanes
            for i in range(nocc):
                r = i * nvir
                n = N[x + 4, y + 4, i]
                hi, lo = split(n)
                L[x, h, r:r + nvir, at:at + lanes] = hi
                L[x, h, pairs + r:pairs + r + nvir, at:at + lanes] = lo
                s2 = slope_z(x + 4, y + 4, i, shifted)
                S2[x, y, i] = s2
                s0 = difference(lambda t: N[x + 4 + t, y + 4, i])
                S0[x, y, i] = s0
                hi, lo = split(s0)
                L[x, h, r:r + nvir, at + lanes:at + 2 * lanes] = hi
                L[x, h, pairs + r:pairs + r + nvir, at + lanes:at + 2 * lanes] = lo
                AL[x, y, i] = g0 * s0 + g2 * s2
        return carry

    lax.fori_loop(0, bx, first_pass, 0)

    for c in turn_x + arm_x:
        c.wait_recv()

    def prepare_x(t, carry):
        k, y = t // by, lax.rem(t, by)
        side = k // 2
        c = jnp.where(k < 2, k + bx - 2, k - 2) * by + y
        a = rim(k, bx, 0, bx)
        prepare(a + 2, 4 + y, px[side], c, A0[a, y, 2:3])
        return carry

    lax.fori_loop(0, 4 * by, prepare_x, 0, unroll=2)

    for c in near_y:
        c.wait_recv()
    corner = [
        put(
            W.at[near_src(bx, sx), near_dst(by, sy)],
            W.at[near_dst(bx, sx), near_dst(by, sy)],
            beside("gx", sx),
        )
        for sy in both
        for sx in both
    ]
    multiply(4 * bx, lambda t: (4 + t // 4, rim(lax.rem(t, 4), by, 2, by + 2)))

    def second_pass_cell(x, y, S1, Rh, Rl):
        g0, g1, g2, k1, k2, k3, kk = (C[x, y, k:k + 1] for k in range(7))
        at, at1 = (y % 2) * 2 * lanes, (y % 2) * lanes
        c = x * by + y
        for i in range(nocc):
            r = i * nvir
            n = N[x + 4, y + 4, i]
            s1 = difference(lambda t: N[x + 4, y + 4 + t, i])
            al = AL[x, y, i] + g1 * s1
            sc = k1 * n + k2 * al
            fl0 = sc * g0 + k3 * S0[x, y, i]
            fl1 = sc * g1 + k3 * s1
            fl2 = sc * g2 + k3 * S2[x, y, i]
            f0[x + 2, y, i] = fl0
            f1[x, y + 2, i] = fl1
            turned = difference(lambda t: pltpu.roll(fl2, (-t) % lanes, 1))
            b = (kk * n + k1 * al) - turned
            base[x, y, i] = b
            deep = 4 * c + half * (2 * i // nocc)
            s = c + cells * (2 * i // nocc)
            j = i % (nocc // 2)
            E2[j] = jnp.where(slot == s, pltpu.roll(fl2, deep, 1), E2[j])
            hi, lo = split(s1)
            S1[r:r + nvir, at1:at1 + lanes] = hi
            S1[pairs + r:pairs + r + nvir, at1:at1 + lanes] = lo
            for v, to in ((b, at), (fl0, at + lanes), (fl1, 4 * lanes + at1)):
                hi, lo = split(v)
                Rh[r:r + nvir, to:to + lanes] = hi
                Rl[r:r + nvir, to:to + lanes] = lo

    def gather(left, S1, Rh, Rl):
        k = 4 * lanes
        top = dot(left[...], Rh[:, 0:k]) + dot(S1[...], Rh[:, k:k + 2 * lanes])
        low_part = dot(left[0:pairs], Rl[:, 0:k]) + dot(S1[0:pairs], Rl[:, k:k + 2 * lanes])
        acc[...] += (top[0:pairs] + top[pairs:]) + low_part

    def second_pass(x, carry):
        gather(L.at[jnp.maximum(x - 1, 0), 1], S1b, Rhb, Rlb)
        for y in range(0, 2):
            second_pass_cell(x, y, S1a, Rha, Rla)
        gather(L.at[x, 0], S1a, Rha, Rla)
        for y in range(2, 4):
            second_pass_cell(x, y, S1b, Rhb, Rlb)
        return carry

    lax.fori_loop(0, bx, second_pass, 0)
    z_out = [put(E2, ez.at[s], beside("gz", s)) for s in zsides]
    gather(L.at[bx - 1, 1], S1b, Rhb, Rlb)
    for i in range(nocc):
        e = E2[i % (nocc // 2)]
        if 2 * i >= nocc:
            e = pltpu.roll(e, half, 1)
        hi, lo = split(e)
        RE[i * nvir:(i + 1) * nvir] = hi
        RL[i * nvir:(i + 1) * nvir] = lo
    ends = dot(LE[...], RE[...])
    total = acc[...] + (ends[0:pairs] + ends[pairs:]) + dot(LE[0:pairs], RL[...])
    for tx in range(nx):
        for ty in range(ny):
            for tz in range(nz):
                r = ((tx * ny + ty) * nz + tz) * rows_out
                part[tx, ty, tz] = total[r:r + rows_out]
    first = []
    for d in range(1, n_plane):
        tx, tz, target = plane(d)
        c = pltpu.make_async_remote_copy(
            src_ref=part.at[tx, :, tz], dst_ref=got.at[d],
            send_sem=send1.at[d], recv_sem=recv1.at[d],
            device_id=target, device_id_type=MESH,
        )
        c.start()
        first.append(c)

    def arm_pass(count, place, A, out):
        def body(t, carry):
            x, y, a, b = place(t)
            shifted = [vS[k, x - 2, y - 2] for k in range(4)]
            c0, c1, c3 = A[a, b, 0:1], A[a, b, 1:2], A[a, b, 3:4]
            for i in range(nocc):
                s0 = difference(lambda t: N[x + t, y, i])
                s1 = difference(lambda t: N[x, y + t, i])
                out[a, b, i] = (c0 * s0 + c1 * s1) + (slope_z(x, y, i, shifted) + c3 * N[x, y, i])
            return carry

        lax.fori_loop(0, count, body, 0)

    for c in far_x + corner:
        c.wait_recv()
    multiply(4 * by, lambda t: (rim(t // by, bx, 0, bx + 4), 4 + lax.rem(t, by)))
    multiply(16, lambda t: (rim(t // 4, bx, 2, bx + 2), rim(lax.rem(t, 4), by, 2, by + 2)))

    def at_x(t):
        a, y = rim(t // by, bx, 0, bx), lax.rem(t, by)
        return a + 2, y + 4, a, y

    arm_pass(4 * by, at_x, A0, f0)

    for c in turn_y + arm_y:
        c.wait_recv()

    def prepare_y(t, carry):
        x, k = t // 4, lax.rem(t, 4)
        side = k // 2
        c = x * by + jnp.where(k < 2, k + by - 2, k - 2)
        b = rim(k, by, 0, by)
        prepare(4 + x, b + 2, py[side], c, A1[x, b, 2:3])
        return carry

    lax.fori_loop(0, 4 * bx, prepare_y, 0, unroll=2)

    mine = part[gx, :, gz]
    for d, c in enumerate(first):
        c.wait_recv()
        mine = mine + got[d + 1]
    acc2[...] = mine

    for c in far_y:
        c.wait_recv()
    multiply(4 * bx, lambda t: (4 + t // 4, rim(lax.rem(t, 4), by, 0, by + 4)))

    second = []
    for d in range(1, ny):
        t, target = column(d)
        c = pltpu.make_async_remote_copy(
            src_ref=acc2.at[t], dst_ref=got2.at[d],
            send_sem=send2.at[d], recv_sem=recv2.at[d],
            device_id=target, device_id_type=MESH,
        )
        c.start()
        second.append(c)

    def at_y(t):
        x, b = t // 4, rim(lax.rem(t, 4), by, 0, by)
        return x + 4, b + 2, x, b

    arm_pass(4 * bx, at_y, A1, f1)

    for c in z_out:
        c.wait_recv()
    for j in range(nocc // 2):
        outer = ez[0, j] if nz == 2 else jnp.where((lane & 3) < 2, ez[1, j], ez[0, j])
        corr[j] = edge_terms(outer - E2[j], lane)
    for c in copies + first + second:
        c.wait_send()
    mine = acc2[gy]
    for d, c in enumerate(second):
        c.wait_recv()
        mine = mine + got2[d + 1]
    cas[...] = mine * (1.0 / (cells * lanes * nx * ny * nz))


def finish_kernel(f0, f1, base, corr, cas_in, pot_out, cas, pot, sem):
    bx, by, nocc, nvir, lanes = base.shape
    cells = bx * by
    half = lanes // 2
    cas[...] = cas_in[...]
    lane = lanes_of((nvir, lanes))
    at_edge = (lane < 2) | (lane >= lanes - 2)
    rows = nvir * cells

    def body(i, carry):
        deep = i // (nocc // 2)
        e = corr[lax.rem(i, nocc // 2)]
        row0 = pl.multiple_of(i * rows, rows)
        for y in range(by):
            a = [f0[x, y, i] for x in range(bx + 4)]
            for x in range(bx):
                c = x * by + y
                b = [f1[x, y + k, i] for k in (0, 1, 3, 4)]
                inner = (a[x + 3] - a[x + 1]) + (b[2] - b[1])
                outer = (a[x + 4] - a[x]) + (b[3] - b[0])
                turned = pltpu.roll(e, lax.rem(2 * lanes - 4 * c - half * deep, lanes), 1)
                v = base[x, y, i] - (8.0 * inner - outer)
                pot[pl.ds(row0 + c, nvir, stride=cells), :] = v - jnp.where(at_edge, turned, 0.0)
        pltpu.make_async_copy(pot.at[pl.ds(row0, rows)], pot_out.at[pl.ds(row0, rows)], sem.at[i]).start()
        return carry

    lax.fori_loop(0, nocc, body, 0)
    for i in range(nocc):
        block = pl.ds(i * rows, rows)
        pltpu.make_async_copy(pot.at[block], pot_out.at[block], sem.at[i]).wait()


def on_device(occupied, virtual, kernel_fields, density_grad):
    nocc, bx, by, lanes = occupied.shape
    nvir = virtual.shape[0]
    nx, ny, nz = (lax.axis_size(a) for a in ("gx", "gy", "gz"))
    devices = nx * ny * nz
    cells = bx * by
    pairs = nocc * nvir
    norb = nocc + nvir
    rows = pairs // devices
    sds = lambda *s: jax.ShapeDtypeStruct(s, F32)
    v32 = lambda *s: pltpu.VMEM(s, F32)
    v16 = lambda *s: pltpu.VMEM(s, BF16)
    dma = lambda n: pltpu.SemaphoreType.DMA((n,))
    vmem = pl.BlockSpec(memory_space=pltpu.VMEM)
    hbm = pl.BlockSpec(memory_space=pltpu.HBM)
    zs = 1 if nz == 2 else 2
    flat = lambda a: a.reshape(-1, lanes)
    outs = pl.pallas_call(
        flow_kernel,
        out_shape=(
            sds(bx + 4, by, nocc, nvir, lanes),
            sds(bx, by + 4, nocc, nvir, lanes),
            sds(bx, by, nocc, nvir, lanes),
            sds(nocc // 2, nvir, lanes),
            sds(rows, pairs),
        ),
        in_specs=[hbm] * 4,
        out_specs=[vmem] * 5,
        scratch_shapes=[
            v32(nocc * cells, lanes), v32(nvir * cells, lanes), v32(4 * cells, lanes), v32(3 * cells, lanes),
            v32(bx + 8, by + 8, norb, lanes),
            v32(bx + 8, by + 8, nocc, nvir, lanes),
            v32(4, bx + 4, by + 4, nocc, lanes),
            v32(4, bx + 4, by + 4, nvir, lanes),
            v32(bx, by, nocc, nvir, lanes), v32(bx, by, nocc, nvir, lanes), v32(bx, by, nocc, nvir, lanes),
            v32(bx, by, 8, lanes), v32(bx + 4, by, 4, lanes), v32(bx, by + 4, 4, lanes),
            v32(nocc, lanes), v32(zs, nocc, lanes), v32(nocc, lanes), v32(2, nocc, lanes), v32(2, nocc, lanes),
            v32(nocc // 2, nvir, lanes), v32(zs, nocc // 2, nvir, lanes),
            v16(bx, 2, 2 * pairs, 4 * lanes),
            v16(2 * pairs, 2 * lanes), v16(2 * pairs, 2 * lanes),
            v16(pairs, 6 * lanes), v16(pairs, 6 * lanes), v16(pairs, 6 * lanes), v16(pairs, 6 * lanes),
            v16(2 * pairs, lanes), v16(pairs, lanes), v16(pairs, lanes),
            v32(pairs, pairs),
            v32(nx, ny, nz, rows, pairs),
            v32(nx * nz, ny, rows, pairs),
            v32(ny, rows, pairs), v32(ny, rows, pairs),
            dma(28), dma(28), dma(4), dma(nx * nz), dma(nx * nz), dma(ny), dma(ny),
        ],
        compiler_params=pltpu.CompilerParams(
            collective_id=0, has_side_effects=True, vmem_limit_bytes=46 * MIB
        ),
        name="flow",
    )(flat(occupied), flat(virtual), flat(kernel_fields), flat(density_grad))
    pot, casida = pl.pallas_call(
        finish_kernel,
        out_shape=(sds(pairs * cells, lanes), sds(rows, pairs)),
        in_specs=[vmem] * 5,
        out_specs=(hbm, vmem),
        scratch_shapes=[v32(pairs * cells, lanes), dma(nocc)],
        compiler_params=pltpu.CompilerParams(vmem_limit_bytes=4 * MIB),
        name="finish",
    )(*outs)
    return pot.reshape(pairs, bx, by, lanes), casida


def solution(mesh):
    spec = P(None, "gx", "gy", "gz")
    return jax.shard_map(
        on_device,
        mesh=mesh,
        in_specs=(spec,) * 4,
        out_specs=(spec, P(("gx", "gy", "gz"), None)),
        check_vma=False,
    )
```

```python
import functools

import jax
import jax.numpy as jnp
from jax import lax
from jax.experimental import pallas as pl
from jax.experimental.pallas import tpu as pltpu
from jax.sharding import PartitionSpec as P

MESH = pl.DeviceIdType.MESH
F32 = jnp.float32
BF16 = jnp.bfloat16
SHIFTS = (1, -1, 2, -2)
MIB = 1024 * 1024


def difference(f):
    return 8.0 * (f(1) - f(-1)) - (f(2) - f(-2))


def lanes_of(shape):
    return lax.broadcasted_iota(jnp.int32, shape, len(shape) - 1)


def edge_terms(gap, lane):
    axis = gap.ndim - 1
    lanes = gap.shape[axis]
    at = lane & 3
    two = jnp.where(at >= 2, -pltpu.roll(gap, lanes - 2, axis), pltpu.roll(gap, 2, axis))
    one = jnp.where(at == 3, pltpu.roll(gap, lanes - 1, axis), -pltpu.roll(gap, 1, axis))
    return two + jnp.where((at == 3) | (at == 0), 8.0 * one, 0.0)


def split(v):
    hi = v.astype(BF16)
    return hi, (v - hi.astype(F32)).astype(BF16)


def dot(a, b):
    return lax.dot_general(a, b, (((1,), (1,)), ((), ())), preferred_element_type=F32)


def flow_kernel(
    occ_in, vir_in, ker_in, grd_in,
    f0, f1, base, corr, cas,
    occ, vir, ker, grd, W, N, oS, vS, S0, S2, AL, C, A0, A1,
    pk, wz, pkn, px, py, E2, ez, L, S1a, S1b, Rha, Rla, Rhb, Rlb, LE, RE, RL,
    acc, part, got, acc2, got2,
    send, recv, own, send1, recv1, send2, recv2,
):
    nx, ny, nz = (lax.axis_size(a) for a in ("gx", "gy", "gz"))
    gx, gy, gz = (lax.axis_index(a) for a in ("gx", "gy", "gz"))
    bx, by = base.shape[0], base.shape[1]
    cells = bx * by
    lanes = occ.shape[1]
    half = lanes // 2
    nocc, nvir = occ.shape[0] // cells, vir.shape[0] // cells
    pairs = nocc * nvir
    rows_out = cas.shape[0]
    n_plane = nx * nz
    me = gx * nz + gz

    def plane(d):
        t = lax.rem(me + d, n_plane)
        tx, tz = t // nz, lax.rem(t, nz)
        return tx, tz, {"gx": tx, "gy": gy, "gz": tz}

    def column(d):
        t = lax.rem(gy + d, ny)
        return t, {"gx": gx, "gy": t, "gz": gz}

    def beside(axis, side):
        v, n = {"gx": (gx, nx), "gy": (gy, ny), "gz": (gz, nz)}[axis]
        where = {"gx": gx, "gy": gy, "gz": gz}
        where[axis] = lax.rem(v + 1, n) if side == 0 else lax.rem(v + n - 1, n)
        return where

    taken = [
        pltpu.make_async_copy(a, b, own.at[k])
        for k, (a, b) in enumerate(((occ_in, occ), (vir_in, vir), (ker_in, ker), (grd_in, grd)))
    ]
    for c in taken:
        c.start()
    barrier = pltpu.get_barrier_semaphore()
    for d in range(1, n_plane):
        pl.semaphore_signal(barrier, inc=1, device_id=plane(d)[2], device_id_type=MESH)
    for d in range(1, ny):
        pl.semaphore_signal(barrier, inc=1, device_id=column(d)[1], device_id_type=MESH)

    acc[...] = jnp.zeros_like(acc)
    for r in (Rhb, Rlb):
        r[...] = jnp.zeros_like(r)
    S1b[...] = jnp.zeros_like(S1b)
    L[0, 1] = jnp.zeros_like(L[0, 1])
    E2[...] = jnp.zeros_like(E2)
    lane = lanes_of((nvir, lanes))
    lane1 = lanes_of((1, lanes))
    at_edge = (lane < 2) | (lane >= lanes - 2)
    slot = lax.rem((lane + 2) // 4, lanes // 4)

    for c in taken:
        c.wait()
    packed = jnp.zeros((nocc, lanes), F32)
    for c in range(cells):
        x, y = divmod(c, by)
        o = occ[pl.ds(c, nocc, stride=cells), :]
        v = vir[pl.ds(c, nvir, stride=cells), :]
        W[x + 4, y + 4, 0:nocc] = o
        W[x + 4, y + 4, nocc:nocc + nvir] = v
        packed += pltpu.roll(jnp.where(at_edge, o, 0.0), 4 * c, 1)
        packed += pltpu.roll(jnp.where(at_edge, v, 0.0), 4 * c + half, 1)
        g = [grd[pl.ds(k * cells + c, 1), :] for k in range(3)]
        f = [ker[pl.ds(k * cells + c, 1), :] for k in range(4)]
        k1, k2, k3 = f[1] * (1.0 / 12.0), f[2] * (1.0 / 144.0), f[3] * (1.0 / 144.0)
        C[x, y] = jnp.concatenate(g + [k1, k2, k3, f[0], f[0]], axis=0)
        for m, ref in ((0, A0.at[x + 2, y]), (1, A1.at[x, y + 2])):
            q = k2 * g[m]
            a = [q * g[k] + k3 if k == m else q * g[k] for k in range(3)]
            ref[...] = jnp.concatenate(a + [k1 * g[m]], axis=0)
    pk[...] = packed
    pl.semaphore_wait(barrier, n_plane - 1 + ny - 1)

    copies = []

    def put(src, dst, device):
        k = len(copies)
        c = pltpu.make_async_remote_copy(
            src_ref=src, dst_ref=dst, send_sem=send.at[k], recv_sem=recv.at[k],
            device_id=device, device_id_type=MESH,
        )
        c.start()
        copies.append(c)
        return c

    in_x, in_y = pl.ds(4, bx), pl.ds(4, by)

    def near_src(b, side):
        return pl.ds(b + 2, 2) if side == 0 else pl.ds(4, 2)

    def near_dst(b, side):
        return pl.ds(2, 2) if side == 0 else pl.ds(b + 4, 2)

    def far_src(b, side):
        return pl.ds(b, 2) if side == 0 else pl.ds(6, 2)

    def far_dst(b, side):
        return pl.ds(0, 2) if side == 0 else pl.ds(b + 6, 2)

    def arm_src(b, side):
        return pl.ds(b, 2) if side == 0 else pl.ds(2, 2)

    def arm_dst(b, side):
        return pl.ds(0, 2) if side == 0 else pl.ds(b + 2, 2)

    zsides = range(1 if nz == 2 else 2)
    both = range(2)
    near_y = [
        put(W.at[in_x, near_src(by, s)], W.at[in_x, near_dst(by, s)], beside("gy", s)) for s in both
    ]
    z_in = [put(pk, wz.at[s], beside("gz", s)) for s in zsides]
    near_x = [
        put(W.at[near_src(bx, s), in_y], W.at[near_dst(bx, s), in_y], beside("gx", s)) for s in both
    ]
    arm_x = [put(A0.at[arm_src(bx, s)], A0.at[arm_dst(bx, s)], beside("gx", s)) for s in both]
    arm_y = [
        put(A1.at[:, arm_src(by, s)], A1.at[:, arm_dst(by, s)], beside("gy", s)) for s in both
    ]
    far_x = [
        put(W.at[far_src(bx, s), in_y], W.at[far_dst(bx, s), in_y], beside("gx", s)) for s in both
    ]
    far_y = [
        put(W.at[in_x, far_src(by, s)], W.at[in_x, far_dst(by, s)], beside("gy", s)) for s in both
    ]

    def multiply(count, place):
        def body(t, carry):
            x, y = place(t)
            v = W[x, y, nocc:nocc + nvir]
            for i in range(nocc):
                N[x, y, i] = W[x, y, i:i + 1] * v
            return carry

        lax.fori_loop(0, count, body, 0)

    def rim(t, b, lo, hi):
        return jnp.where(t < 2, t + lo, t + hi)

    multiply(cells, lambda t: (4 + t // by, 4 + lax.rem(t, by)))

    for c in z_in:
        c.wait_recv()
    low = (lanes_of((nocc, lanes)) & 3) < 2
    z_edges = wz[0] if nz == 2 else jnp.where(low, wz[1], wz[0])
    pkn[...] = z_edges
    turn_x = [put(pkn, px.at[s], beside("gx", s)) for s in both]
    turn_y = [put(pkn, py.at[s], beside("gy", s)) for s in both]

    def prepare(x, y, edges, c, fold):
        ao = pltpu.roll(edges, lax.rem(lanes - 4 * c, lanes), 1)
        av = pltpu.roll(edges, lax.rem(lanes + half - 4 * c, lanes), 1)
        o_own, v_own = W[x, y, 0:nocc], W[x, y, nocc:nocc + nvir]
        for k, s in enumerate(SHIFTS):
            m = lane < s if s > 0 else lane >= lanes + s
            scale = 8.0 if abs(s) == 1 else 1.0
            factor = scale if fold is None else scale * fold
            oS[k, x - 2, y - 2] = factor * pltpu.roll(jnp.where(m, ao, o_own), (-s) % lanes, 1)
            vS[k, x - 2, y - 2] = pltpu.roll(jnp.where(m, av, v_own), (-s) % lanes, 1)

    def prepare_center(t, carry):
        prepare(4 + t // by, 4 + lax.rem(t, by), pkn[...], t, None)
        return carry

    lax.fori_loop(0, cells, prepare_center, 0, unroll=2)

    own_o, own_v = pk[...], pltpu.roll(pk[...], half, 1)
    nb_o, nb_v = z_edges, pltpu.roll(z_edges, half, 1)
    for i in range(nocc):
        gap = nb_o[i:i + 1] * nb_v - own_o[i:i + 1] * own_v
        e = jnp.where(slot < cells, edge_terms(gap, lane), 0.0)
        hi, lo = split(e)
        LE[i * nvir:(i + 1) * nvir] = hi
        LE[pairs + i * nvir:pairs + (i + 1) * nvir] = lo

    for c in near_x:
        c.wait_recv()
    multiply(4 * by, lambda t: (rim(t // by, bx, 2, bx + 2), 4 + lax.rem(t, by)))

    def slope_z(x, y, i, shifted):
        p = [oS[k, x - 2, y - 2, i:i + 1] * shifted[k] for k in range(4)]
        return (p[0] - p[1]) - (p[2] - p[3])

    def first_pass(x, carry):
        for y in range(by):
            g0, g2 = C[x, y, 0:1], C[x, y, 2:3]
            shifted = [vS[k, x + 2, y + 2] for k in range(4)]
            h, at = y // 2, (y % 2) * 2 * lanes
            for i in range(nocc):
                r = i * nvir
                n = N[x + 4, y + 4, i]
                hi, lo = split(n)
                L[x, h, r:r + nvir, at:at + lanes] = hi
                L[x, h, pairs + r:pairs + r + nvir, at:at + lanes] = lo
                s2 = slope_z(x + 4, y + 4, i, shifted)
                S2[x, y, i] = s2
                s0 = difference(lambda t: N[x + 4 + t, y + 4, i])
                S0[x, y, i] = s0
                hi, lo = split(s0)
                L[x, h, r:r + nvir, at + lanes:at + 2 * lanes] = hi
                L[x, h, pairs + r:pairs + r + nvir, at + lanes:at + 2 * lanes] = lo
                AL[x, y, i] = g0 * s0 + g2 * s2
        return carry

    lax.fori_loop(0, bx, first_pass, 0)

    for c in turn_x + arm_x:
        c.wait_recv()

    def prepare_x(t, carry):
        k, y = t // by, lax.rem(t, by)
        side = k // 2
        c = jnp.where(k < 2, k + bx - 2, k - 2) * by + y
        a = rim(k, bx, 0, bx)
        prepare(a + 2, 4 + y, px[side], c, A0[a, y, 2:3])
        return carry

    lax.fori_loop(0, 4 * by, prepare_x, 0, unroll=2)

    for c in near_y:
        c.wait_recv()
    corner = [
        put(
            W.at[near_src(bx, sx), near_dst(by, sy)],
            W.at[near_dst(bx, sx), near_dst(by, sy)],
            beside("gx", sx),
        )
        for sy in both
        for sx in both
    ]
    multiply(4 * bx, lambda t: (4 + t // 4, rim(lax.rem(t, 4), by, 2, by + 2)))

    def second_pass_cell(x, y, S1, Rh, Rl):
        g0, g1, g2, k1, k2, k3, kk = (C[x, y, k:k + 1] for k in range(7))
        at, at1 = (y % 2) * 2 * lanes, (y % 2) * lanes
        c = x * by + y
        for i in range(nocc):
            r = i * nvir
            n = N[x + 4, y + 4, i]
            s1 = difference(lambda t: N[x + 4, y + 4 + t, i])
            al = AL[x, y, i] + g1 * s1
            sc = k1 * n + k2 * al
            fl0 = sc * g0 + k3 * S0[x, y, i]
            fl1 = sc * g1 + k3 * s1
            fl2 = sc * g2 + k3 * S2[x, y, i]
            f0[x + 2, y, i] = fl0
            f1[x, y + 2, i] = fl1
            turned = difference(lambda t: pltpu.roll(fl2, (-t) % lanes, 1))
            b = (kk * n + k1 * al) - turned
            base[x, y, i] = b
            deep = 4 * c + half * (2 * i // nocc)
            s = c + cells * (2 * i // nocc)
            j = i % (nocc // 2)
            E2[j] = jnp.where(slot == s, pltpu.roll(fl2, deep, 1), E2[j])
            hi, lo = split(s1)
            S1[r:r + nvir, at1:at1 + lanes] = hi
            S1[pairs + r:pairs + r + nvir, at1:at1 + lanes] = lo
            for v, to in ((b, at), (fl0, at + lanes), (fl1, 4 * lanes + at1)):
                hi, lo = split(v)
                Rh[r:r + nvir, to:to + lanes] = hi
                Rl[r:r + nvir, to:to + lanes] = lo

    def gather(left, S1, Rh, Rl):
        k = 4 * lanes
        top = dot(left[...], Rh[:, 0:k]) + dot(S1[...], Rh[:, k:k + 2 * lanes])
        low_part = dot(left[0:pairs], Rl[:, 0:k]) + dot(S1[0:pairs], Rl[:, k:k + 2 * lanes])
        acc[...] += (top[0:pairs] + top[pairs:]) + low_part

    def second_pass(x, carry):
        gather(L.at[jnp.maximum(x - 1, 0), 1], S1b, Rhb, Rlb)
        for y in range(0, 2):
            second_pass_cell(x, y, S1a, Rha, Rla)
        gather(L.at[x, 0], S1a, Rha, Rla)
        for y in range(2, 4):
            second_pass_cell(x, y, S1b, Rhb, Rlb)
        return carry

    lax.fori_loop(0, bx, second_pass, 0)
    z_out = [put(E2, ez.at[s], beside("gz", s)) for s in zsides]
    gather(L.at[bx - 1, 1], S1b, Rhb, Rlb)
    for i in range(nocc):
        e = E2[i % (nocc // 2)]
        if 2 * i >= nocc:
            e = pltpu.roll(e, half, 1)
        hi, lo = split(e)
        RE[i * nvir:(i + 1) * nvir] = hi
        RL[i * nvir:(i + 1) * nvir] = lo
    ends = dot(LE[...], RE[...])
    total = acc[...] + (ends[0:pairs] + ends[pairs:]) + dot(LE[0:pairs], RL[...])
    for tx in range(nx):
        for ty in range(ny):
            for tz in range(nz):
                r = ((tx * ny + ty) * nz + tz) * rows_out
                part[tx, ty, tz] = total[r:r + rows_out]
    first = []
    for d in range(1, n_plane):
        tx, tz, target = plane(d)
        c = pltpu.make_async_remote_copy(
            src_ref=part.at[tx, :, tz], dst_ref=got.at[d],
            send_sem=send1.at[d], recv_sem=recv1.at[d],
            device_id=target, device_id_type=MESH,
        )
        c.start()
        first.append(c)

    def arm_pass(count, place, A, out):
        def body(t, carry):
            x, y, a, b = place(t)
            shifted = [vS[k, x - 2, y - 2] for k in range(4)]
            c0, c1, c3 = A[a, b, 0:1], A[a, b, 1:2], A[a, b, 3:4]
            for i in range(nocc):
                s0 = difference(lambda t: N[x + t, y, i])
                s1 = difference(lambda t: N[x, y + t, i])
                out[a, b, i] = (c0 * s0 + c1 * s1) + (slope_z(x, y, i, shifted) + c3 * N[x, y, i])
            return carry

        lax.fori_loop(0, count, body, 0)

    for c in far_x + corner:
        c.wait_recv()
    multiply(4 * by, lambda t: (rim(t // by, bx, 0, bx + 4), 4 + lax.rem(t, by)))
    multiply(16, lambda t: (rim(t // 4, bx, 2, bx + 2), rim(lax.rem(t, 4), by, 2, by + 2)))

    def at_x(t):
        a, y = rim(t // by, bx, 0, bx), lax.rem(t, by)
        return a + 2, y + 4, a, y

    arm_pass(4 * by, at_x, A0, f0)

    for c in turn_y + arm_y:
        c.wait_recv()

    def prepare_y(t, carry):
        x, k = t // 4, lax.rem(t, 4)
        side = k // 2
        c = x * by + jnp.where(k < 2, k + by - 2, k - 2)
        b = rim(k, by, 0, by)
        prepare(4 + x, b + 2, py[side], c, A1[x, b, 2:3])
        return carry

    lax.fori_loop(0, 4 * bx, prepare_y, 0, unroll=2)

    mine = part[gx, :, gz]
    for d, c in enumerate(first):
        c.wait_recv()
        mine = mine + got[d + 1]
    acc2[...] = mine

    for c in far_y:
        c.wait_recv()
    multiply(4 * bx, lambda t: (4 + t // 4, rim(lax.rem(t, 4), by, 0, by + 4)))

    second = []
    for d in range(1, ny):
        t, target = column(d)
        c = pltpu.make_async_remote_copy(
            src_ref=acc2.at[t], dst_ref=got2.at[d],
            send_sem=send2.at[d], recv_sem=recv2.at[d],
            device_id=target, device_id_type=MESH,
        )
        c.start()
        second.append(c)

    def at_y(t):
        x, b = t // 4, rim(lax.rem(t, 4), by, 0, by)
        return x + 4, b + 2, x, b

    arm_pass(4 * bx, at_y, A1, f1)

    for c in z_out:
        c.wait_recv()
    for j in range(nocc // 2):
        outer = ez[0, j] if nz == 2 else jnp.where((lane & 3) < 2, ez[1, j], ez[0, j])
        corr[j] = edge_terms(outer - E2[j], lane)
    for c in copies + first + second:
        c.wait_send()
    mine = acc2[gy]
    for d, c in enumerate(second):
        c.wait_recv()
        mine = mine + got2[d + 1]
    cas[...] = mine * (1.0 / (cells * lanes * nx * ny * nz))


def finish_kernel(f0, f1, base, corr, cas_in, pot_out, cas, pot, sem):
    bx, by, nocc, nvir, lanes = base.shape
    cells = bx * by
    half = lanes // 2
    cas[...] = cas_in[...]
    lane = lanes_of((nvir, lanes))
    at_edge = (lane < 2) | (lane >= lanes - 2)
    rows = nvir * cells

    def body(i, carry):
        deep = i // (nocc // 2)
        e = corr[lax.rem(i, nocc // 2)]
        row0 = pl.multiple_of(i * rows, rows)
        for y in range(by):
            a = [f0[x, y, i] for x in range(bx + 4)]
            for x in range(bx):
                c = x * by + y
                b = [f1[x, y + k, i] for k in (0, 1, 3, 4)]
                inner = (a[x + 3] - a[x + 1]) + (b[2] - b[1])
                outer = (a[x + 4] - a[x]) + (b[3] - b[0])
                turned = pltpu.roll(e, lax.rem(2 * lanes - 4 * c - half * deep, lanes), 1)
                v = base[x, y, i] - (8.0 * inner - outer)
                pot[pl.ds(row0 + c, nvir, stride=cells), :] = v - jnp.where(at_edge, turned, 0.0)
        pltpu.make_async_copy(pot.at[pl.ds(row0, rows)], pot_out.at[pl.ds(row0, rows)], sem.at[i]).start()
        return carry

    lax.fori_loop(0, nocc, body, 0)
    for i in range(nocc):
        block = pl.ds(i * rows, rows)
        pltpu.make_async_copy(pot.at[block], pot_out.at[block], sem.at[i]).wait()


def on_device(occupied, virtual, kernel_fields, density_grad):
    nocc, bx, by, lanes = occupied.shape
    nvir = virtual.shape[0]
    nx, ny, nz = (lax.axis_size(a) for a in ("gx", "gy", "gz"))
    devices = nx * ny * nz
    cells = bx * by
    pairs = nocc * nvir
    norb = nocc + nvir
    rows = pairs // devices
    sds = lambda *s: jax.ShapeDtypeStruct(s, F32)
    v32 = lambda *s: pltpu.VMEM(s, F32)
    v16 = lambda *s: pltpu.VMEM(s, BF16)
    dma = lambda n: pltpu.SemaphoreType.DMA((n,))
    vmem = pl.BlockSpec(memory_space=pltpu.VMEM)
    hbm = pl.BlockSpec(memory_space=pltpu.HBM)
    zs = 1 if nz == 2 else 2
    flat = lambda a: a.reshape(-1, lanes)
    outs = pl.pallas_call(
        flow_kernel,
        out_shape=(
            sds(bx + 4, by, nocc, nvir, lanes),
            sds(bx, by + 4, nocc, nvir, lanes),
            sds(bx, by, nocc, nvir, lanes),
            sds(nocc // 2, nvir, lanes),
            sds(rows, pairs),
        ),
        in_specs=[hbm] * 4,
        out_specs=[vmem] * 5,
        scratch_shapes=[
            v32(nocc * cells, lanes), v32(nvir * cells, lanes), v32(4 * cells, lanes), v32(3 * cells, lanes),
            v32(bx + 8, by + 8, norb, lanes),
            v32(bx + 8, by + 8, nocc, nvir, lanes),
            v32(4, bx + 4, by + 4, nocc, lanes),
            v32(4, bx + 4, by + 4, nvir, lanes),
            v32(bx, by, nocc, nvir, lanes), v32(bx, by, nocc, nvir, lanes), v32(bx, by, nocc, nvir, lanes),
            v32(bx, by, 8, lanes), v32(bx + 4, by, 4, lanes), v32(bx, by + 4, 4, lanes),
            v32(nocc, lanes), v32(zs, nocc, lanes), v32(nocc, lanes), v32(2, nocc, lanes), v32(2, nocc, lanes),
            v32(nocc // 2, nvir, lanes), v32(zs, nocc // 2, nvir, lanes),
            v16(bx, 2, 2 * pairs, 4 * lanes),
            v16(2 * pairs, 2 * lanes), v16(2 * pairs, 2 * lanes),
            v16(pairs, 6 * lanes), v16(pairs, 6 * lanes), v16(pairs, 6 * lanes), v16(pairs, 6 * lanes),
            v16(2 * pairs, lanes), v16(pairs, lanes), v16(pairs, lanes),
            v32(pairs, pairs),
            v32(nx, ny, nz, rows, pairs),
            v32(nx * nz, ny, rows, pairs),
            v32(ny, rows, pairs), v32(ny, rows, pairs),
            dma(28), dma(28), dma(4), dma(nx * nz), dma(nx * nz), dma(ny), dma(ny),
        ],
        compiler_params=pltpu.CompilerParams(
            collective_id=0, has_side_effects=True, vmem_limit_bytes=42 * MIB
        ),
        name="flow",
    )(*(pltpu.with_memory_space_constraint(flat(a), pltpu.HBM) for a in (occupied, virtual, kernel_fields, density_grad)))
    pot, casida = pl.pallas_call(
        finish_kernel,
        out_shape=(sds(pairs * cells, lanes), sds(rows, pairs)),
        in_specs=[vmem] * 5,
        out_specs=(hbm, vmem),
        scratch_shapes=[v32(pairs * cells, lanes), dma(nocc)],
        compiler_params=pltpu.CompilerParams(vmem_limit_bytes=4 * MIB),
        name="finish",
    )(*outs)
    return pot.reshape(pairs, bx, by, lanes), casida


def solution(mesh):
    spec = P(None, "gx", "gy", "gz")
    return jax.shard_map(
        on_device,
        mesh=mesh,
        in_specs=(spec,) * 4,
        out_specs=(spec, P(("gx", "gy", "gz"), None)),
        check_vma=False,
    )
```

```python
import functools

import jax
import jax.numpy as jnp
from jax import lax
from jax.experimental import pallas as pl
from jax.experimental.pallas import tpu as pltpu
from jax.sharding import PartitionSpec as P

MESH = pl.DeviceIdType.MESH
F32 = jnp.float32
BF16 = jnp.bfloat16
SHIFTS = (1, -1, 2, -2)
MIB = 1024 * 1024


def difference(f):
    return 8.0 * (f(1) - f(-1)) - (f(2) - f(-2))


def lanes_of(shape):
    return lax.broadcasted_iota(jnp.int32, shape, len(shape) - 1)


def edge_terms(gap, lane):
    axis = gap.ndim - 1
    lanes = gap.shape[axis]
    at = lane & 3
    two = jnp.where(at >= 2, -pltpu.roll(gap, lanes - 2, axis), pltpu.roll(gap, 2, axis))
    one = jnp.where(at == 3, pltpu.roll(gap, lanes - 1, axis), -pltpu.roll(gap, 1, axis))
    return two + jnp.where((at == 3) | (at == 0), 8.0 * one, 0.0)


def rest(v):
    return v - v.astype(BF16).astype(F32)


def dot(a, b):
    return lax.dot_general(a, b, (((1,), (1,)), ((), ())), preferred_element_type=F32)


def flow_kernel(
    occ_in, vir_in, ker_in, grd_in,
    pot, cas,
    occ, vir, ker, grd, W, N, oS, vS, S0, S1, S2, AL, NL, S0L, LO, f0, f1, base, C, A0, A1,
    pk, wz, pkn, px, py, E2, ez, corr, LE, LEL,
    acc, part, got, acc2, got2,
    send, recv, own, send1, recv1, send2, recv2,
):
    nx, ny, nz = (lax.axis_size(a) for a in ("gx", "gy", "gz"))
    gx, gy, gz = (lax.axis_index(a) for a in ("gx", "gy", "gz"))
    bx, by = base.shape[0], base.shape[1]
    cells = bx * by
    lanes = occ.shape[1]
    half = lanes // 2
    nocc, nvir = occ.shape[0] // cells, vir.shape[0] // cells
    pairs = nocc * nvir
    rows_out = cas.shape[0]
    n_plane = nx * nz
    me = gx * nz + gz

    def plane(d):
        t = lax.rem(me + d, n_plane)
        tx, tz = t // nz, lax.rem(t, nz)
        return tx, tz, {"gx": tx, "gy": gy, "gz": tz}

    def column(d):
        t = lax.rem(gy + d, ny)
        return t, {"gx": gx, "gy": t, "gz": gz}

    def beside(axis, side):
        v, n = {"gx": (gx, nx), "gy": (gy, ny), "gz": (gz, nz)}[axis]
        where = {"gx": gx, "gy": gy, "gz": gz}
        where[axis] = lax.rem(v + 1, n) if side == 0 else lax.rem(v + n - 1, n)
        return where

    taken = [
        pltpu.make_async_copy(a, b, own.at[k])
        for k, (a, b) in enumerate(((occ_in, occ), (vir_in, vir), (ker_in, ker), (grd_in, grd)))
    ]
    for c in taken:
        c.start()
    barrier = pltpu.get_barrier_semaphore()
    for d in range(1, n_plane):
        pl.semaphore_signal(barrier, inc=1, device_id=plane(d)[2], device_id_type=MESH)
    for d in range(1, ny):
        pl.semaphore_signal(barrier, inc=1, device_id=column(d)[1], device_id_type=MESH)

    E2[...] = jnp.zeros_like(E2)
    lane = lanes_of((nvir, lanes))
    at_edge = (lane < 2) | (lane >= lanes - 2)
    slot = lax.rem((lane + 2) // 4, lanes // 4)

    def own_rows(c):
        x, y = divmod(c, by)
        o = occ[pl.ds(c, nocc, stride=cells), :]
        v = vir[pl.ds(c, nvir, stride=cells), :]
        return x, y, o, v

    taken[0].wait()
    taken[1].wait()
    for c in range(cells):
        x, y, o, v = own_rows(c)
        W[x + 4, y + 4, 0:nocc] = o
        W[x + 4, y + 4, nocc:nocc + nvir] = v
    pl.semaphore_wait(barrier, n_plane - 1 + ny - 1)

    copies = []

    def put(src, dst, device):
        k = len(copies)
        c = pltpu.make_async_remote_copy(
            src_ref=src, dst_ref=dst, send_sem=send.at[k], recv_sem=recv.at[k],
            device_id=device, device_id_type=MESH,
        )
        c.start()
        copies.append(c)
        return c

    in_x, in_y = pl.ds(4, bx), pl.ds(4, by)

    def near_src(b, side):
        return pl.ds(b + 2, 2) if side == 0 else pl.ds(4, 2)

    def near_dst(b, side):
        return pl.ds(2, 2) if side == 0 else pl.ds(b + 4, 2)

    def layer_src(b, side, depth):
        return pl.ds(b + 4 - depth, 1) if side == 0 else pl.ds(3 + depth, 1)

    def layer_dst(b, side, depth):
        return pl.ds(4 - depth, 1) if side == 0 else pl.ds(b + 3 + depth, 1)

    def far_src(b, side):
        return pl.ds(b, 2) if side == 0 else pl.ds(6, 2)

    def far_dst(b, side):
        return pl.ds(0, 2) if side == 0 else pl.ds(b + 6, 2)

    def arm_src(b, side):
        return pl.ds(b, 2) if side == 0 else pl.ds(2, 2)

    def arm_dst(b, side):
        return pl.ds(0, 2) if side == 0 else pl.ds(b + 2, 2)

    zsides = range(1 if nz == 2 else 2)
    both = range(2)
    near_y = [
        [
            put(
                W.at[in_x, layer_src(by, s, depth)],
                W.at[in_x, layer_dst(by, s, depth)],
                beside("gy", s),
            )
            for s in both
        ]
        for depth in (1, 2)
    ]
    near_x = [
        put(W.at[near_src(bx, s), in_y], W.at[near_dst(bx, s), in_y], beside("gx", s)) for s in both
    ]
    taken[2].wait()
    taken[3].wait()
    packed = jnp.zeros((nocc, lanes), F32)
    for c in range(cells):
        x, y, o, v = own_rows(c)
        packed += pltpu.roll(jnp.where(at_edge, o, 0.0), 4 * c, 1)
        packed += pltpu.roll(jnp.where(at_edge, v, 0.0), 4 * c + half, 1)
        g = [grd[pl.ds(k * cells + c, 1), :] for k in range(3)]
        f = [ker[pl.ds(k * cells + c, 1), :] for k in range(4)]
        k1, k2, k3 = f[1] * (1.0 / 12.0), f[2] * (1.0 / 144.0), f[3] * (1.0 / 144.0)
        C[x, y] = jnp.concatenate(g + [k1, k2, k3, f[0], f[0]], axis=0)
        for m, ref in ((0, A0.at[x + 2, y]), (1, A1.at[x, y + 2])):
            q = k2 * g[m]
            a = [q * g[k] + k3 if k == m else q * g[k] for k in range(3)]
            ref[...] = jnp.concatenate(a + [k1 * g[m]], axis=0)
    pk[...] = packed
    z_in = [put(pk, wz.at[s], beside("gz", s)) for s in zsides]
    arm_x = [put(A0.at[arm_src(bx, s)], A0.at[arm_dst(bx, s)], beside("gx", s)) for s in both]
    arm_y = [
        put(A1.at[:, arm_src(by, s)], A1.at[:, arm_dst(by, s)], beside("gy", s)) for s in both
    ]

    def multiply(count, place, unroll=2):
        def body(t, carry):
            x, y = place(t)
            v = W[x, y, nocc:nocc + nvir]
            for i in range(nocc):
                N[x, y - 2, i] = W[x, y, i:i + 1] * v
            return carry

        lax.fori_loop(0, count, body, 0, unroll=unroll)

    def rim(t, b, lo, hi):
        return jnp.where(t < 2, t + lo, t + hi)

    multiply(cells, lambda t: (4 + t // by, 4 + lax.rem(t, by)))

    for c in z_in:
        c.wait_recv()
    low = (lanes_of((nocc, lanes)) & 3) < 2
    z_edges = wz[0] if nz == 2 else jnp.where(low, wz[1], wz[0])
    pkn[...] = z_edges
    turn_x = [put(pkn, px.at[s], beside("gx", s)) for s in both]
    turn_y = [put(pkn, py.at[s], beside("gy", s)) for s in both]
    far_x = [
        put(W.at[far_src(bx, s), in_y], W.at[far_dst(bx, s), in_y], beside("gx", s)) for s in both
    ]
    far_y = [
        put(W.at[in_x, far_src(by, s)], W.at[in_x, far_dst(by, s)], beside("gy", s)) for s in both
    ]

    def prepare(x, y, edges, c, fold):
        ao = pltpu.roll(edges, lax.rem(lanes - 4 * c, lanes), 1)
        av = pltpu.roll(edges, lax.rem(lanes + half - 4 * c, lanes), 1)
        o_own, v_own = W[x, y, 0:nocc], W[x, y, nocc:nocc + nvir]
        for k, s in enumerate(SHIFTS):
            m = lane < s if s > 0 else lane >= lanes + s
            scale = 8.0 if abs(s) == 1 else 1.0
            factor = scale if fold is None else scale * fold
            oS[k, x - 2, y - 2] = factor * pltpu.roll(jnp.where(m, ao, o_own), (-s) % lanes, 1)
            vS[k, x - 2, y - 2] = pltpu.roll(jnp.where(m, av, v_own), (-s) % lanes, 1)

    def prepare_center(t, carry):
        prepare(4 + t // by, 4 + lax.rem(t, by), pkn[...], t, None)
        return carry

    lax.fori_loop(0, cells, prepare_center, 0, unroll=4)

    own_o, own_v = pk[...], pltpu.roll(pk[...], half, 1)
    nb_o, nb_v = z_edges, pltpu.roll(z_edges, half, 1)
    for i in range(nocc):
        gap = nb_o[i:i + 1] * nb_v - own_o[i:i + 1] * own_v
        e = jnp.where(slot < cells, edge_terms(gap, lane), 0.0)
        LE[i] = e
        LEL[i] = rest(e)

    for c in near_x:
        c.wait_recv()
    multiply(4 * by, lambda t: (rim(t // by, bx, 2, bx + 2), 4 + lax.rem(t, by)))

    def slope_z(x, y, i, shifted):
        p = [oS[k, x + 2, y + 2, i:i + 1] * shifted[k] for k in range(4)]
        return (p[0] - p[1]) - (p[2] - p[3])

    def n_at(x, y, i):
        return N[x + 4, y + 2, i]

    def first_pass(x, carry):
        for y in range(by):
            g0, g2 = C[x, y, 0:1], C[x, y, 2:3]
            shifted = [vS[k, x + 2, y + 2] for k in range(4)]
            for i in range(nocc):
                NL[x, y, i] = rest(n_at(x, y, i))
                s2 = slope_z(x, y, i, shifted)
                S2[x, y, i] = s2
                s0 = difference(lambda t: n_at(x + t, y, i))
                S0[x, y, i] = s0
                S0L[x, y, i] = rest(s0)
                AL[x, y, i] = g0 * s0 + g2 * s2
        return carry

    lax.fori_loop(0, bx, first_pass, 0)

    for c in turn_x + arm_x:
        c.wait_recv()

    def prepare_x(t, carry):
        k, y = t // by, lax.rem(t, by)
        side = k // 2
        c = jnp.where(k < 2, k + bx - 2, k - 2) * by + y
        a = rim(k, bx, 0, bx)
        prepare(a + 2, 4 + y, px[side], c, A0[a, y, 2:3])
        return carry

    lax.fori_loop(0, 4 * by, prepare_x, 0, unroll=4)

    def second_pass_cell(x, y, lo):
        g0, g1, g2, k1, k2, k3, kk = (C[x, y, k:k + 1] for k in range(7))
        c = x * by + y
        for i in range(nocc):
            n = n_at(x, y, i)
            s1 = difference(lambda t: n_at(x, y + t, i))
            al = AL[x, y, i] + g1 * s1
            sc = k1 * n + k2 * al
            fl0 = sc * g0 + k3 * S0[x, y, i]
            fl1 = sc * g1 + k3 * s1
            fl2 = sc * g2 + k3 * S2[x, y, i]
            b = (kk * n + k1 * al) - difference(lambda t: pltpu.roll(fl2, (-t) % lanes, 1))
            S1[x, y, i] = s1
            f0[x + 2, y, i] = fl0
            f1[x, y + 2, i] = fl1
            base[x, y, i] = b
            deep = (2 * i) // nocc
            j = i % (nocc // 2)
            E2[j] = jnp.where(slot == c + cells * deep, pltpu.roll(fl2, 4 * c + half * deep, 1), E2[j])
            for k, v in enumerate((s1, b, fl0, fl1)):
                LO[lo, k, i] = rest(v)

    def wide(parts):
        return jnp.concatenate([p.reshape(pairs, lanes) for p in parts], axis=1)

    def gather(x, ys, at, start):
        (l0, l1), (y0, y1) = at, ys

        def pair(high, low):
            return wide(high), wide(low)

        def orbit(lo, y):
            left = pair([N[x + 4, y + 2], S0[x, y]], [NL[x, y], S0L[x, y]])
            return left, pair([base[x, y], f0[x + 2, y]], [LO[lo, 1], LO[lo, 2]])

        def products(left, right):
            return dot(left[0], right[0]), dot(left[1], right[0]), dot(left[0], right[1])

        p, q = products(*orbit(l0, y0)), products(*orbit(l1, y1))
        r = products(
            pair([S1[x, y0], S1[x, y1]], [LO[l0, 0], LO[l1, 0]]),
            pair([f1[x, y0 + 2], f1[x, y1 + 2]], [LO[l0, 3], LO[l1, 3]]),
        )
        one, two = sum(p[1:], p[0]), sum(q[1:], q[0])
        one, two = (one + r[0], two + (r[1] + r[2])) if x % 2 else (one + (r[1] + r[2]), two + r[0])
        for k, total in enumerate((one, two)):
            acc[k] = total if start else acc[k] + total

    def second_pass(ys, start, late):
        for x in range(bx):
            at = [2 * (x % 2), 2 * (x % 2) + 1]
            if late is not None:
                gather(*late)
            for lo, y in zip(at, ys):
                second_pass_cell(x, y, lo)
            late = (x, ys, at, start and x == 0)
        return late

    def across(depth):
        y = (4 - depth, by + 3 + depth)
        return lambda t: (4 + t // 2, jnp.where(lax.rem(t, 2) == 0, y[0], y[1]))

    for c in near_y[0]:
        c.wait_recv()
    multiply(2 * bx, across(1))
    late = second_pass((1, 2), True, None)
    for c in near_y[1]:
        c.wait_recv()
    corner = [
        put(
            W.at[near_src(bx, sx), near_dst(by, sy)],
            W.at[near_dst(bx, sx), near_dst(by, sy)],
            beside("gx", sx),
        )
        for sy in both
        for sx in both
    ]
    multiply(2 * bx, across(2))
    late = second_pass((0, 3), False, late)
    gather(*late)
    ends = [E2[i % (nocc // 2)] for i in range(nocc)]
    ends = [e if 2 * i < nocc else pltpu.roll(e, half, 1) for i, e in enumerate(ends)]
    right = jnp.concatenate(ends, axis=0)
    left, left_lo = LE[...].reshape(pairs, lanes), LEL[...].reshape(pairs, lanes)
    total = (acc[0] + acc[1]) + (dot(left, right) + dot(left_lo, right) + dot(left, rest(right)))
    for tx in range(nx):
        for ty in range(ny):
            for tz in range(nz):
                r = ((tx * ny + ty) * nz + tz) * rows_out
                part[tx, ty, tz] = total[r:r + rows_out]
    first = []
    for d in range(1, n_plane):
        tx, tz, target = plane(d)
        c = pltpu.make_async_remote_copy(
            src_ref=part.at[tx, :, tz], dst_ref=got.at[d],
            send_sem=send1.at[d], recv_sem=recv1.at[d],
            device_id=target, device_id_type=MESH,
        )
        c.start()
        first.append(c)
    z_out = [put(E2, ez.at[s], beside("gz", s)) for s in zsides]

    for c in far_x + corner:
        c.wait_recv()
    multiply(4 * by, lambda t: (rim(t // by, bx, 0, bx + 4), 4 + lax.rem(t, by)))
    multiply(16, lambda t: (rim(t // 4, bx, 2, bx + 2), rim(lax.rem(t, 4), by, 2, by + 2)))

    def at_x(t, carry):
        a, y = rim(t // by, bx, 0, bx), lax.rem(t, by)
        x = a - 2
        shifted = [vS[k, a, y + 2] for k in range(4)]
        c0, c1, c3 = A0[a, y, 0:1], A0[a, y, 1:2], A0[a, y, 3:4]
        for i in range(nocc):
            s0 = difference(lambda t: n_at(x + t, y, i))
            s1 = difference(lambda t: n_at(x, y + t, i))
            f0[a, y, i] = (c0 * s0 + c1 * s1) + (slope_z(x, y, i, shifted) + c3 * n_at(x, y, i))
        return carry

    lax.fori_loop(0, 4 * by, at_x, 0)

    for c in turn_y + arm_y:
        c.wait_recv()

    def prepare_y(t, carry):
        x, k = t // 4, lax.rem(t, 4)
        side = k // 2
        c = x * by + jnp.where(k < 2, k + by - 2, k - 2)
        b = rim(k, by, 0, by)
        prepare(4 + x, b + 2, py[side], c, A1[x, b, 2:3])
        return carry

    lax.fori_loop(0, 4 * bx, prepare_y, 0, unroll=4)

    def at_y(x, carry):
        for y in (-2, -1, by, by + 1):
            b = y + 2
            shifted = [vS[k, x + 2, b] for k in range(4)]
            c0, c1, c3 = A1[x, b, 0:1], A1[x, b, 1:2], A1[x, b, 3:4]
            for i in range(nocc):
                s0 = difference(lambda t: n_at(x + t, y, i))
                n = lambda t: n_at(x, y + t, i)
                if y == -2:
                    s1 = 8.0 * n(1) - n(2)
                elif y == -1:
                    s1 = 8.0 * (n(1) - n(-1)) - n(2)
                elif y == by:
                    s1 = 8.0 * (n(1) - n(-1)) + n(-2)
                else:
                    s1 = n(-2) - 8.0 * n(-1)
                f1[x, b, i] = (c0 * s0 + c1 * s1) + (slope_z(x, y, i, shifted) + c3 * n(0))
        return carry

    lax.fori_loop(0, bx, at_y, 0)

    for c in first:
        c.wait_recv()
    mine = part[gx, :, gz]
    for d in range(1, n_plane):
        mine = mine + got[d]
    acc2[...] = mine
    second = []
    for d in range(1, ny):
        t, target = column(d)
        c = pltpu.make_async_remote_copy(
            src_ref=acc2.at[t], dst_ref=got2.at[d],
            send_sem=send2.at[d], recv_sem=recv2.at[d],
            device_id=target, device_id_type=MESH,
        )
        c.start()
        second.append(c)

    for c in z_out:
        c.wait_recv()
    for j in range(nocc // 2):
        outer = ez[0, j] if nz == 2 else jnp.where((lane & 3) < 2, ez[1, j], ez[0, j])
        corr[j] = edge_terms(outer - E2[j], lane)
    for c in far_y:
        c.wait_recv()

    def assemble(x, carry):
        def far(y):
            return W[x + 4, y + 4, nocc:nocc + nvir]

        def slope_of(y):
            return A1[x, y + 2, 1:2]

        low1 = slope_of(-1) * far(-3)
        low2 = (slope_of(-2) * far(-4), -8.0 * slope_of(-2) * far(-3))
        top1 = -1.0 * slope_of(by) * far(by + 2)
        top2 = (8.0 * slope_of(by + 1) * far(by + 2), -1.0 * slope_of(by + 1) * far(by + 3))
        for i in range(nocc):
            o = [W[x + 4, y + 4, i:i + 1] for y in (-4, -3, by + 2, by + 3)]
            a = [f1[x, b, i] for b in range(by + 4)]
            a[0] = a[0] + (o[0] * low2[0] + o[1] * low2[1])
            a[1] = a[1] + o[1] * low1
            a[by + 2] = a[by + 2] + o[2] * top1
            a[by + 3] = a[by + 3] + (o[2] * top2[0] + o[3] * top2[1])
            deep = (2 * i) // nocc
            e = corr[i % (nocc // 2)]
            for y in range(by):
                c = x * by + y
                b = [f0[x + k, y, i] for k in (0, 1, 3, 4)]
                inner = (b[2] - b[1]) + (a[y + 3] - a[y + 1])
                outer = (b[3] - b[0]) + (a[y + 4] - a[y])
                turned = pltpu.roll(e, lax.rem(2 * lanes - 4 * c - half * deep, lanes), 1)
                v = base[x, y, i] - (8.0 * inner - outer)
                v = v - jnp.where(at_edge, turned, 0.0)
                pot[pl.ds(i * nvir * cells + c, nvir, stride=cells), :] = v
        return carry

    lax.fori_loop(0, bx, assemble, 0)
    for c in copies + first + second:
        c.wait_send()
    mine = acc2[gy]
    for d, c in enumerate(second):
        c.wait_recv()
        mine = mine + got2[d + 1]
    cas[...] = mine * (1.0 / (cells * lanes * nx * ny * nz))


def write_kernel(pot_in, cas_in, pot, cas, sem):
    rows = pot_in.shape[0] // sem.shape[0]
    out = []
    for k in range(sem.shape[0]):
        block = pl.ds(k * rows, rows)
        c = pltpu.make_async_copy(pot_in.at[block], pot.at[block], sem.at[k])
        c.start()
        out.append(c)
    cas[...] = cas_in[...]
    for c in out:
        c.wait()


def on_device(occupied, virtual, kernel_fields, density_grad):
    nocc, bx, by, lanes = occupied.shape
    nvir = virtual.shape[0]
    nx, ny, nz = (lax.axis_size(a) for a in ("gx", "gy", "gz"))
    devices = nx * ny * nz
    cells = bx * by
    pairs = nocc * nvir
    norb = nocc + nvir
    rows = pairs // devices
    sds = lambda *s: jax.ShapeDtypeStruct(s, F32)
    v32 = lambda *s: pltpu.VMEM(s, F32)
    dma = lambda n: pltpu.SemaphoreType.DMA((n,))
    vmem = pl.BlockSpec(memory_space=pltpu.VMEM)
    hbm = pl.BlockSpec(memory_space=pltpu.HBM)
    zs = 1 if nz == 2 else 2
    flat = lambda a: a.reshape(-1, lanes)
    outs = pl.pallas_call(
        flow_kernel,
        out_shape=(v32(pairs * cells, lanes), v32(rows, pairs)),
        in_specs=[hbm] * 4,
        out_specs=[vmem] * 2,
        scratch_shapes=[
            v32(nocc * cells, lanes), v32(nvir * cells, lanes), v32(4 * cells, lanes), v32(3 * cells, lanes),
            v32(bx + 8, by + 8, norb, lanes),
            v32(bx + 8, by + 4, nocc, nvir, lanes),
            v32(4, bx + 4, by + 4, nocc, lanes),
            v32(4, bx + 4, by + 4, nvir, lanes),
        ]
        + [v32(bx, by, nocc, nvir, lanes)] * 6
        + [
            v32(4, 4, nocc, nvir, lanes),
            v32(bx + 4, by, nocc, nvir, lanes),
            v32(bx, by + 4, nocc, nvir, lanes),
            v32(bx, by, nocc, nvir, lanes),
            v32(bx, by, 8, lanes), v32(bx + 4, by, 4, lanes), v32(bx, by + 4, 4, lanes),
            v32(nocc, lanes), v32(zs, nocc, lanes), v32(nocc, lanes), v32(2, nocc, lanes), v32(2, nocc, lanes),
            v32(nocc // 2, nvir, lanes), v32(zs, nocc // 2, nvir, lanes), v32(nocc // 2, nvir, lanes),
            v32(nocc, nvir, lanes), v32(nocc, nvir, lanes),
            v32(2, pairs, pairs),
            v32(nx, ny, nz, rows, pairs),
            v32(nx * nz, ny, rows, pairs),
            v32(ny, rows, pairs), v32(ny, rows, pairs),
            dma(28), dma(28), dma(4), dma(nx * nz), dma(nx * nz), dma(ny), dma(ny),
        ],
        compiler_params=pltpu.CompilerParams(
            collective_id=0, has_side_effects=True, vmem_limit_bytes=54 * MIB
        ),
        name="flow",
    )(*(pltpu.with_memory_space_constraint(flat(a), pltpu.HBM) for a in (occupied, virtual, kernel_fields, density_grad)))
    pot, casida = pl.pallas_call(
        write_kernel,
        out_shape=(sds(pairs * cells, lanes), sds(rows, pairs)),
        in_specs=[vmem] * 2,
        out_specs=(hbm, vmem),
        scratch_shapes=[dma(8)],
        compiler_params=pltpu.CompilerParams(vmem_limit_bytes=4 * MIB),
        name="write",
    )(*outs)
    return pot.reshape(pairs, bx, by, lanes), casida


def solution(mesh):
    spec = P(None, "gx", "gy", "gz")
    return jax.shard_map(
        on_device,
        mesh=mesh,
        in_specs=(spec,) * 4,
        out_specs=(spec, P(("gx", "gy", "gz"), None)),
        check_vma=False,
    )
```

```python
import functools

import jax
import jax.numpy as jnp
from jax import lax
from jax.experimental import pallas as pl
from jax.experimental.pallas import tpu as pltpu
from jax.sharding import PartitionSpec as P

MESH = pl.DeviceIdType.MESH
F32 = jnp.float32
BF16 = jnp.bfloat16
SHIFTS = (1, -1, 2, -2)
MIB = 1024 * 1024


def difference(f):
    return 8.0 * (f(1) - f(-1)) - (f(2) - f(-2))


def lanes_of(shape):
    return lax.broadcasted_iota(jnp.int32, shape, len(shape) - 1)


def edge_terms(gap, lane):
    axis = gap.ndim - 1
    lanes = gap.shape[axis]
    at = lane & 3
    two = jnp.where(at >= 2, -pltpu.roll(gap, lanes - 2, axis), pltpu.roll(gap, 2, axis))
    one = jnp.where(at == 3, pltpu.roll(gap, lanes - 1, axis), -pltpu.roll(gap, 1, axis))
    return two + jnp.where((at == 3) | (at == 0), 8.0 * one, 0.0)


def rest(v):
    return v - v.astype(BF16).astype(F32)


def dot(a, b):
    return lax.dot_general(a, b, (((1,), (1,)), ((), ())), preferred_element_type=F32)


def flow_kernel(
    occ_in, vir_in, ker_in, grd_in,
    pot, cas,
    occ, vir, ker, grd, W, N, oS, vS, S0, S1, S2, AL, NL, S0L, LO, f0, f1, base, C, A0, A1,
    pk, wz, pkn, px, py, E2, ez, corr, LE, LEL,
    acc, part, got, acc2, got2,
    send, recv, sendy, recvy, own, send1, recv1, send2, recv2,
):
    nx, ny, nz = (lax.axis_size(a) for a in ("gx", "gy", "gz"))
    gx, gy, gz = (lax.axis_index(a) for a in ("gx", "gy", "gz"))
    bx, by = base.shape[0], base.shape[1]
    cells = bx * by
    lanes = occ.shape[1]
    half = lanes // 2
    nocc, nvir = occ.shape[0] // cells, vir.shape[0] // cells
    pairs = nocc * nvir
    rows_out = cas.shape[0]
    n_plane = nx * nz
    me = gx * nz + gz

    def plane(d):
        t = lax.rem(me + d, n_plane)
        tx, tz = t // nz, lax.rem(t, nz)
        return tx, tz, {"gx": tx, "gy": gy, "gz": tz}

    def column(d):
        t = lax.rem(gy + d, ny)
        return t, {"gx": gx, "gy": t, "gz": gz}

    def beside(axis, side):
        v, n = {"gx": (gx, nx), "gy": (gy, ny), "gz": (gz, nz)}[axis]
        where = {"gx": gx, "gy": gy, "gz": gz}
        step = (1, n - 1)[side] if isinstance(side, int) else jnp.where(side == 0, 1, n - 1)
        where[axis] = lax.rem(v + step, n)
        return where

    taken = [
        pltpu.make_async_copy(a, b, own.at[k])
        for k, (a, b) in enumerate(((occ_in, occ), (vir_in, vir), (ker_in, ker), (grd_in, grd)))
    ]
    for c in taken:
        c.start()
    barrier = pltpu.get_barrier_semaphore()
    for d in range(1, n_plane):
        pl.semaphore_signal(barrier, inc=1, device_id=plane(d)[2], device_id_type=MESH)
    for d in range(1, ny):
        pl.semaphore_signal(barrier, inc=1, device_id=column(d)[1], device_id_type=MESH)

    E2[...] = jnp.zeros_like(E2)
    lane = lanes_of((nvir, lanes))
    at_edge = (lane < 2) | (lane >= lanes - 2)
    slot = lax.rem((lane + 2) // 4, lanes // 4)

    def own_rows(c):
        x, y = divmod(c, by)
        o = occ[pl.ds(c, nocc, stride=cells), :]
        v = vir[pl.ds(c, nvir, stride=cells), :]
        return x, y, o, v

    taken[0].wait()
    taken[1].wait()
    for c in range(cells):
        x, y, o, v = own_rows(c)
        W[x + 4, y + 4, 0:nocc] = o
        W[x + 4, y + 4, nocc:nocc + nvir] = v
    pl.semaphore_wait(barrier, n_plane - 1 + ny - 1)

    copies = []

    def put(src, dst, device):
        k = len(copies)
        c = pltpu.make_async_remote_copy(
            src_ref=src, dst_ref=dst, send_sem=send.at[k], recv_sem=recv.at[k],
            device_id=device, device_id_type=MESH,
        )
        c.start()
        copies.append(c)
        return c

    in_x, in_y = pl.ds(4, bx), pl.ds(4, by)

    def near_src(b, side):
        return pl.ds(b + 2, 2) if side == 0 else pl.ds(4, 2)

    def near_dst(b, side):
        return pl.ds(2, 2) if side == 0 else pl.ds(b + 4, 2)

    def layer_src(side, depth):
        return pl.ds(jnp.where(side == 0, by + 4 - depth, 3 + depth), 1)

    def layer_dst(side, depth):
        return pl.ds(jnp.where(side == 0, 4 - depth, by + 3 + depth), 1)

    def far_src(b, side):
        return pl.ds(b, 2) if side == 0 else pl.ds(6, 2)

    def far_dst(b, side):
        return pl.ds(0, 2) if side == 0 else pl.ds(b + 6, 2)

    def arm_src(b, side):
        return pl.ds(b, 2) if side == 0 else pl.ds(2, 2)

    def arm_dst(b, side):
        return pl.ds(0, 2) if side == 0 else pl.ds(b + 2, 2)

    zsides = range(1 if nz == 2 else 2)
    both = range(2)
    def layer_copy(s, depth):
        k = 2 * (depth - 1) + s
        return pltpu.make_async_remote_copy(
            src_ref=W.at[in_x, layer_src(s, depth)], dst_ref=W.at[in_x, layer_dst(s, depth)],
            send_sem=sendy.at[k], recv_sem=recvy.at[k],
            device_id=beside("gy", s), device_id_type=MESH,
        )

    far_round = jnp.where(gy == ny - 1, 0, 1)
    for depth in (1, 2):
        layer_copy(far_round, depth).start()
        layer_copy(1 - far_round, depth).start()
    near_y = [[layer_copy(s, depth) for s in both] for depth in (1, 2)]
    near_x = [
        put(W.at[near_src(bx, s), in_y], W.at[near_dst(bx, s), in_y], beside("gx", s)) for s in both
    ]
    taken[2].wait()
    taken[3].wait()
    packed = jnp.zeros((nocc, lanes), F32)
    for c in range(cells):
        x, y, o, v = own_rows(c)
        packed += pltpu.roll(jnp.where(at_edge, o, 0.0), 4 * c, 1)
        packed += pltpu.roll(jnp.where(at_edge, v, 0.0), 4 * c + half, 1)
        g = [grd[pl.ds(k * cells + c, 1), :] for k in range(3)]
        f = [ker[pl.ds(k * cells + c, 1), :] for k in range(4)]
        k1, k2, k3 = f[1] * (1.0 / 12.0), f[2] * (1.0 / 144.0), f[3] * (1.0 / 144.0)
        C[x, y] = jnp.concatenate(g + [k1, k2, k3, f[0], f[0]], axis=0)
        for m, ref in ((0, A0.at[x + 2, y]), (1, A1.at[x, y + 2])):
            q = k2 * g[m]
            a = [q * g[k] + k3 if k == m else q * g[k] for k in range(3)]
            ref[...] = jnp.concatenate(a + [k1 * g[m]], axis=0)
    pk[...] = packed
    z_in = [put(pk, wz.at[s], beside("gz", s)) for s in zsides]
    arm_x = [put(A0.at[arm_src(bx, s)], A0.at[arm_dst(bx, s)], beside("gx", s)) for s in both]
    arm_y = [
        put(A1.at[:, arm_src(by, s)], A1.at[:, arm_dst(by, s)], beside("gy", s)) for s in both
    ]

    def multiply(count, place, unroll=2):
        def body(t, carry):
            x, y = place(t)
            v = W[x, y, nocc:nocc + nvir]
            for i in range(nocc):
                N[x, y - 2, i] = W[x, y, i:i + 1] * v
            return carry

        lax.fori_loop(0, count, body, 0, unroll=unroll)

    def rim(t, b, lo, hi):
        return jnp.where(t < 2, t + lo, t + hi)

    multiply(cells, lambda t: (4 + t // by, 4 + lax.rem(t, by)))

    for c in z_in:
        c.wait_recv()
    low = (lanes_of((nocc, lanes)) & 3) < 2
    z_edges = wz[0] if nz == 2 else jnp.where(low, wz[1], wz[0])
    pkn[...] = z_edges
    turn_x = [put(pkn, px.at[s], beside("gx", s)) for s in both]
    turn_y = [put(pkn, py.at[s], beside("gy", s)) for s in both]
    far_x = [
        put(W.at[far_src(bx, s), in_y], W.at[far_dst(bx, s), in_y], beside("gx", s)) for s in both
    ]
    far_y = [
        put(W.at[in_x, far_src(by, s)], W.at[in_x, far_dst(by, s)], beside("gy", s)) for s in both
    ]

    def prepare(x, y, edges, c, fold):
        ao = pltpu.roll(edges, lax.rem(lanes - 4 * c, lanes), 1)
        av = pltpu.roll(edges, lax.rem(lanes + half - 4 * c, lanes), 1)
        o_own, v_own = W[x, y, 0:nocc], W[x, y, nocc:nocc + nvir]
        for k, s in enumerate(SHIFTS):
            m = lane < s if s > 0 else lane >= lanes + s
            scale = 8.0 if abs(s) == 1 else 1.0
            factor = scale if fold is None else scale * fold
            oS[k, x - 2, y - 2] = factor * pltpu.roll(jnp.where(m, ao, o_own), (-s) % lanes, 1)
            vS[k, x - 2, y - 2] = pltpu.roll(jnp.where(m, av, v_own), (-s) % lanes, 1)

    def prepare_center(t, carry):
        prepare(4 + t // by, 4 + lax.rem(t, by), pkn[...], t, None)
        return carry

    lax.fori_loop(0, cells, prepare_center, 0, unroll=4)

    own_o, own_v = pk[...], pltpu.roll(pk[...], half, 1)
    nb_o, nb_v = z_edges, pltpu.roll(z_edges, half, 1)
    for i in range(nocc):
        gap = nb_o[i:i + 1] * nb_v - own_o[i:i + 1] * own_v
        e = jnp.where(slot < cells, edge_terms(gap, lane), 0.0)
        LE[i] = e
        LEL[i] = rest(e)

    for c in near_x:
        c.wait_recv()
    multiply(4 * by, lambda t: (rim(t // by, bx, 2, bx + 2), 4 + lax.rem(t, by)))

    def slope_z(x, y, i, shifted):
        p = [oS[k, x + 2, y + 2, i:i + 1] * shifted[k] for k in range(4)]
        return (p[0] - p[1]) - (p[2] - p[3])

    def n_at(x, y, i):
        return N[x + 4, y + 2, i]

    def first_pass(x, carry):
        for y in range(by):
            g0, g2 = C[x, y, 0:1], C[x, y, 2:3]
            shifted = [vS[k, x + 2, y + 2] for k in range(4)]
            for i in range(nocc):
                NL[x, y, i] = rest(n_at(x, y, i))
                s2 = slope_z(x, y, i, shifted)
                S2[x, y, i] = s2
                s0 = difference(lambda t: n_at(x + t, y, i))
                S0[x, y, i] = s0
                S0L[x, y, i] = rest(s0)
                AL[x, y, i] = g0 * s0 + g2 * s2
        return carry

    lax.fori_loop(0, bx, first_pass, 0)

    for c in turn_x + arm_x:
        c.wait_recv()

    def prepare_x(t, carry):
        k, y = t // by, lax.rem(t, by)
        side = k // 2
        c = jnp.where(k < 2, k + bx - 2, k - 2) * by + y
        a = rim(k, bx, 0, bx)
        prepare(a + 2, 4 + y, px[side], c, A0[a, y, 2:3])
        return carry

    lax.fori_loop(0, 4 * by, prepare_x, 0, unroll=4)

    def second_pass_cell(x, y, lo):
        g0, g1, g2, k1, k2, k3, kk = (C[x, y, k:k + 1] for k in range(7))
        c = x * by + y
        for i in range(nocc):
            n = n_at(x, y, i)
            s1 = difference(lambda t: n_at(x, y + t, i))
            al = AL[x, y, i] + g1 * s1
            sc = k1 * n + k2 * al
            fl0 = sc * g0 + k3 * S0[x, y, i]
            fl1 = sc * g1 + k3 * s1
            fl2 = sc * g2 + k3 * S2[x, y, i]
            b = (kk * n + k1 * al) - difference(lambda t: pltpu.roll(fl2, (-t) % lanes, 1))
            S1[x, y, i] = s1
            f0[x + 2, y, i] = fl0
            f1[x, y + 2, i] = fl1
            base[x, y, i] = b
            deep = (2 * i) // nocc
            j = i % (nocc // 2)
            E2[j] = jnp.where(slot == c + cells * deep, pltpu.roll(fl2, 4 * c + half * deep, 1), E2[j])
            for k, v in enumerate((s1, b, fl0, fl1)):
                LO[lo, k, i] = rest(v)

    def wide(parts):
        return jnp.concatenate([p.reshape(pairs, lanes) for p in parts], axis=1)

    def gather(x, ys, at, start):
        (l0, l1), (y0, y1) = at, ys

        def pair(high, low):
            return wide(high), wide(low)

        def orbit(lo, y):
            left = pair([N[x + 4, y + 2], S0[x, y]], [NL[x, y], S0L[x, y]])
            return left, pair([base[x, y], f0[x + 2, y]], [LO[lo, 1], LO[lo, 2]])

        first, second = orbit(l0, y0), orbit(l1, y1)
        third = (
            pair([S1[x, y0], S1[x, y1]], [LO[l0, 0], LO[l1, 0]]),
            pair([f1[x, y0 + 2], f1[x, y1 + 2]], [LO[l0, 3], LO[l1, 3]]),
        )

        def beside_(parts):
            return jnp.concatenate(parts, axis=1)

        left = [beside_([first[0][k], second[0][k]]) for k in range(2)]
        right = [beside_([first[1][k], second[1][k]]) for k in range(2)]
        top = dot(jnp.concatenate(left, axis=0), right[0])
        low_part = dot(
            beside_([left[0], third[0][0], third[0][0], third[0][1]]),
            beside_([right[1], third[1][0], third[1][1], third[1][0]]),
        )
        total = (top[0:pairs] + top[pairs:]) + low_part
        acc[...] = total if start else acc[...] + total

    def second_pass(ys, start, late):
        for x in range(bx):
            at = [2 * (x % 2), 2 * (x % 2) + 1]
            if late is not None:
                gather(*late)
            for lo, y in zip(at, ys):
                second_pass_cell(x, y, lo)
            late = (x, ys, at, start and x == 0)
        return late

    def across(depth):
        y = (4 - depth, by + 3 + depth)
        return lambda t: (4 + t // 2, jnp.where(lax.rem(t, 2) == 0, y[0], y[1]))

    def turn_corner(depth):
        return [
            put(
                W.at[near_src(bx, sx), layer_dst(sy, depth)],
                W.at[near_dst(bx, sx), layer_dst(sy, depth)],
                beside("gx", sx),
            )
            for sy in both
            for sx in both
        ]

    for c in near_y[0]:
        c.wait_recv()
    corner = turn_corner(1)
    multiply(2 * bx, across(1))
    late = second_pass((1, 2), True, None)
    for c in near_y[1]:
        c.wait_recv()
    corner += turn_corner(2)
    multiply(2 * bx, across(2))
    late = second_pass((0, 3), False, late)
    gather(*late)
    ends = [E2[i % (nocc // 2)] for i in range(nocc)]
    ends = [e if 2 * i < nocc else pltpu.roll(e, half, 1) for i, e in enumerate(ends)]
    right = jnp.concatenate(ends, axis=0)
    left, left_lo = LE[...].reshape(pairs, lanes), LEL[...].reshape(pairs, lanes)
    total = acc[...] + (dot(left, right) + dot(left_lo, right) + dot(left, rest(right)))
    for tx in range(nx):
        for ty in range(ny):
            for tz in range(nz):
                r = ((tx * ny + ty) * nz + tz) * rows_out
                part[tx, ty, tz] = total[r:r + rows_out]
    first = []
    for d in sorted(range(1, n_plane), key=lambda d: abs(2 * d - n_plane)):
        tx, tz, target = plane(d)
        c = pltpu.make_async_remote_copy(
            src_ref=part.at[tx, :, tz], dst_ref=got.at[d],
            send_sem=send1.at[d], recv_sem=recv1.at[d],
            device_id=target, device_id_type=MESH,
        )
        c.start()
        first.append(c)
    z_out = [put(E2, ez.at[s], beside("gz", s)) for s in zsides]

    for c in far_x + corner:
        c.wait_recv()
    multiply(4 * by, lambda t: (rim(t // by, bx, 0, bx + 4), 4 + lax.rem(t, by)))
    multiply(16, lambda t: (rim(t // 4, bx, 2, bx + 2), rim(lax.rem(t, 4), by, 2, by + 2)))

    def at_x(t, carry):
        a, y = rim(t // by, bx, 0, bx), lax.rem(t, by)
        x = a - 2
        shifted = [vS[k, a, y + 2] for k in range(4)]
        c0, c1, c3 = A0[a, y, 0:1], A0[a, y, 1:2], A0[a, y, 3:4]
        for i in range(nocc):
            s0 = difference(lambda t: n_at(x + t, y, i))
            s1 = difference(lambda t: n_at(x, y + t, i))
            f0[a, y, i] = (c0 * s0 + c1 * s1) + (slope_z(x, y, i, shifted) + c3 * n_at(x, y, i))
        return carry

    lax.fori_loop(0, 4 * by, at_x, 0)

    for c in turn_y + arm_y:
        c.wait_recv()

    def prepare_y(t, carry):
        x, k = t // 4, lax.rem(t, 4)
        side = k // 2
        c = x * by + jnp.where(k < 2, k + by - 2, k - 2)
        b = rim(k, by, 0, by)
        prepare(4 + x, b + 2, py[side], c, A1[x, b, 2:3])
        return carry

    lax.fori_loop(0, 4 * bx, prepare_y, 0, unroll=4)

    def at_y(x, carry):
        for y in (-2, -1, by, by + 1):
            b = y + 2
            shifted = [vS[k, x + 2, b] for k in range(4)]
            c0, c1, c3 = A1[x, b, 0:1], A1[x, b, 1:2], A1[x, b, 3:4]
            for i in range(nocc):
                s0 = difference(lambda t: n_at(x + t, y, i))
                n = lambda t: n_at(x, y + t, i)
                if y == -2:
                    s1 = 8.0 * n(1) - n(2)
                elif y == -1:
                    s1 = 8.0 * (n(1) - n(-1)) - n(2)
                elif y == by:
                    s1 = 8.0 * (n(1) - n(-1)) + n(-2)
                else:
                    s1 = n(-2) - 8.0 * n(-1)
                f1[x, b, i] = (c0 * s0 + c1 * s1) + (slope_z(x, y, i, shifted) + c3 * n(0))
        return carry

    lax.fori_loop(0, bx, at_y, 0)

    for c in first:
        c.wait_recv()
    mine = part[gx, :, gz]
    for d in range(1, n_plane):
        mine = mine + got[d]
    acc2[...] = mine
    second = []
    for d in range(1, ny):
        t, target = column(d)
        c = pltpu.make_async_remote_copy(
            src_ref=acc2.at[t], dst_ref=got2.at[d],
            send_sem=send2.at[d], recv_sem=recv2.at[d],
            device_id=target, device_id_type=MESH,
        )
        c.start()
        second.append(c)

    for c in z_out:
        c.wait_recv()
    for j in range(nocc // 2):
        outer = ez[0, j] if nz == 2 else jnp.where((lane & 3) < 2, ez[1, j], ez[0, j])
        corr[j] = edge_terms(outer - E2[j], lane)
    for c in far_y:
        c.wait_recv()

    def assemble(x, carry):
        def far(y):
            return W[x + 4, y + 4, nocc:nocc + nvir]

        def slope_of(y):
            return A1[x, y + 2, 1:2]

        low1 = slope_of(-1) * far(-3)
        low2 = (slope_of(-2) * far(-4), -8.0 * slope_of(-2) * far(-3))
        top1 = -1.0 * slope_of(by) * far(by + 2)
        top2 = (8.0 * slope_of(by + 1) * far(by + 2), -1.0 * slope_of(by + 1) * far(by + 3))
        for i in range(nocc):
            o = [W[x + 4, y + 4, i:i + 1] for y in (-4, -3, by + 2, by + 3)]
            a = [f1[x, b, i] for b in range(by + 4)]
            a[0] = a[0] + (o[0] * low2[0] + o[1] * low2[1])
            a[1] = a[1] + o[1] * low1
            a[by + 2] = a[by + 2] + o[2] * top1
            a[by + 3] = a[by + 3] + (o[2] * top2[0] + o[3] * top2[1])
            deep = (2 * i) // nocc
            e = corr[i % (nocc // 2)]
            for y in range(by):
                c = x * by + y
                b = [f0[x + k, y, i] for k in (0, 1, 3, 4)]
                inner = (b[2] - b[1]) + (a[y + 3] - a[y + 1])
                outer = (b[3] - b[0]) + (a[y + 4] - a[y])
                turned = pltpu.roll(e, lax.rem(2 * lanes - 4 * c - half * deep, lanes), 1)
                v = base[x, y, i] - (8.0 * inner - outer)
                v = v - jnp.where(at_edge, turned, 0.0)
                pot[pl.ds(i * nvir * cells + c, nvir, stride=cells), :] = v
        return carry

    lax.fori_loop(0, bx, assemble, 0)
    for c in copies + near_y[0] + near_y[1] + first + second:
        c.wait_send()
    mine = acc2[gy]
    for d, c in enumerate(second):
        c.wait_recv()
        mine = mine + got2[d + 1]
    cas[...] = mine * (1.0 / (cells * lanes * nx * ny * nz))


def write_kernel(pot_in, cas_in, pot, cas, sem):
    rows = pot_in.shape[0] // sem.shape[0]
    out = []
    for k in range(sem.shape[0]):
        block = pl.ds(k * rows, rows)
        c = pltpu.make_async_copy(pot_in.at[block], pot.at[block], sem.at[k])
        c.start()
        out.append(c)
    cas[...] = cas_in[...]
    for c in out:
        c.wait()


def on_device(occupied, virtual, kernel_fields, density_grad):
    nocc, bx, by, lanes = occupied.shape
    nvir = virtual.shape[0]
    nx, ny, nz = (lax.axis_size(a) for a in ("gx", "gy", "gz"))
    devices = nx * ny * nz
    cells = bx * by
    pairs = nocc * nvir
    norb = nocc + nvir
    rows = pairs // devices
    sds = lambda *s: jax.ShapeDtypeStruct(s, F32)
    v32 = lambda *s: pltpu.VMEM(s, F32)
    dma = lambda n: pltpu.SemaphoreType.DMA((n,))
    vmem = pl.BlockSpec(memory_space=pltpu.VMEM)
    hbm = pl.BlockSpec(memory_space=pltpu.HBM)
    zs = 1 if nz == 2 else 2
    flat = lambda a: a.reshape(-1, lanes)
    outs = pl.pallas_call(
        flow_kernel,
        out_shape=(v32(pairs * cells, lanes), v32(rows, pairs)),
        in_specs=[hbm] * 4,
        out_specs=[vmem] * 2,
        scratch_shapes=[
            v32(nocc * cells, lanes), v32(nvir * cells, lanes), v32(4 * cells, lanes), v32(3 * cells, lanes),
            v32(bx + 8, by + 8, norb, lanes),
            v32(bx + 8, by + 4, nocc, nvir, lanes),
            v32(4, bx + 4, by + 4, nocc, lanes),
            v32(4, bx + 4, by + 4, nvir, lanes),
        ]
        + [v32(bx, by, nocc, nvir, lanes)] * 6
        + [
            v32(4, 4, nocc, nvir, lanes),
            v32(bx + 4, by, nocc, nvir, lanes),
            v32(bx, by + 4, nocc, nvir, lanes),
            v32(bx, by, nocc, nvir, lanes),
            v32(bx, by, 8, lanes), v32(bx + 4, by, 4, lanes), v32(bx, by + 4, 4, lanes),
            v32(nocc, lanes), v32(zs, nocc, lanes), v32(nocc, lanes), v32(2, nocc, lanes), v32(2, nocc, lanes),
            v32(nocc // 2, nvir, lanes), v32(zs, nocc // 2, nvir, lanes), v32(nocc // 2, nvir, lanes),
            v32(nocc, nvir, lanes), v32(nocc, nvir, lanes),
            v32(pairs, pairs),
            v32(nx, ny, nz, rows, pairs),
            v32(nx * nz, ny, rows, pairs),
            v32(ny, rows, pairs), v32(ny, rows, pairs),
            dma(28), dma(28), dma(4), dma(4), dma(4), dma(nx * nz), dma(nx * nz), dma(ny), dma(ny),
        ],
        compiler_params=pltpu.CompilerParams(
            collective_id=0, has_side_effects=True, vmem_limit_bytes=54 * MIB
        ),
        name="flow",
    )(*(pltpu.with_memory_space_constraint(flat(a), pltpu.HBM) for a in (occupied, virtual, kernel_fields, density_grad)))
    pot, casida = pl.pallas_call(
        write_kernel,
        out_shape=(sds(pairs * cells, lanes), sds(rows, pairs)),
        in_specs=[vmem] * 2,
        out_specs=(hbm, vmem),
        scratch_shapes=[dma(8)],
        compiler_params=pltpu.CompilerParams(vmem_limit_bytes=4 * MIB),
        name="write",
    )(*outs)
    return pot.reshape(pairs, bx, by, lanes), casida


def solution(mesh):
    spec = P(None, "gx", "gy", "gz")
    return jax.shard_map(
        on_device,
        mesh=mesh,
        in_specs=(spec,) * 4,
        out_specs=(spec, P(("gx", "gy", "gz"), None)),
        check_vma=False,
    )
```

```python
import functools

import jax
import jax.numpy as jnp
from jax import lax
from jax.experimental import pallas as pl
from jax.experimental.pallas import tpu as pltpu
from jax.sharding import PartitionSpec as P

MESH = pl.DeviceIdType.MESH
F32 = jnp.float32
BF16 = jnp.bfloat16
SHIFTS = (1, -1, 2, -2)
MIB = 1024 * 1024


def difference(f):
    return 8.0 * (f(1) - f(-1)) - (f(2) - f(-2))


def lanes_of(shape):
    return lax.broadcasted_iota(jnp.int32, shape, len(shape) - 1)


def edge_terms(gap, lane):
    axis = gap.ndim - 1
    lanes = gap.shape[axis]
    at = lane & 3
    two = jnp.where(at >= 2, -pltpu.roll(gap, lanes - 2, axis), pltpu.roll(gap, 2, axis))
    one = jnp.where(at == 3, pltpu.roll(gap, lanes - 1, axis), -pltpu.roll(gap, 1, axis))
    return two + jnp.where((at == 3) | (at == 0), 8.0 * one, 0.0)


def rest(v):
    return v - v.astype(BF16).astype(F32)


def dot(a, b):
    return lax.dot_general(a, b, (((1,), (1,)), ((), ())), preferred_element_type=F32)


def flow_kernel(
    occ_in, vir_in, ker_in, grd_in,
    pot, cas,
    occ, vir, ker, grd, W, N, oS, vS, S0, S1, S2, AL, NL, S0L, LO, f0, f1, base, C, A0, A1,
    pk, wz, pkn, px, py, E2, ez, corr, LE, LEL,
    acc, part, got, acc2, got2,
    send, recv, sendy, recvy, own, send1, recv1, send2, recv2,
):
    nx, ny, nz = (lax.axis_size(a) for a in ("gx", "gy", "gz"))
    gx, gy, gz = (lax.axis_index(a) for a in ("gx", "gy", "gz"))
    bx, by = base.shape[0], base.shape[1]
    cells = bx * by
    lanes = occ.shape[1]
    half = lanes // 2
    nocc, nvir = occ.shape[0] // cells, vir.shape[0] // cells
    pairs = nocc * nvir
    rows_out = cas.shape[0]
    n_plane = nx * nz
    me = gx * nz + gz

    def plane(d):
        t = lax.rem(me + d, n_plane)
        tx, tz = t // nz, lax.rem(t, nz)
        return tx, tz, {"gx": tx, "gy": gy, "gz": tz}

    def column(d):
        t = lax.rem(gy + d, ny)
        return t, {"gx": gx, "gy": t, "gz": gz}

    def beside(axis, side):
        v, n = {"gx": (gx, nx), "gy": (gy, ny), "gz": (gz, nz)}[axis]
        where = {"gx": gx, "gy": gy, "gz": gz}
        step = (1, n - 1)[side] if isinstance(side, int) else jnp.where(side == 0, 1, n - 1)
        where[axis] = lax.rem(v + step, n)
        return where

    taken = [
        pltpu.make_async_copy(a, b, own.at[k])
        for k, (a, b) in enumerate(((occ_in, occ), (vir_in, vir), (ker_in, ker), (grd_in, grd)))
    ]
    for c in taken:
        c.start()
    barrier = pltpu.get_barrier_semaphore()
    for d in range(1, n_plane):
        pl.semaphore_signal(barrier, inc=1, device_id=plane(d)[2], device_id_type=MESH)
    for d in range(1, ny):
        pl.semaphore_signal(barrier, inc=1, device_id=column(d)[1], device_id_type=MESH)

    E2[...] = jnp.zeros_like(E2)
    lane = lanes_of((nvir, lanes))
    at_edge = (lane < 2) | (lane >= lanes - 2)
    slot = lax.rem((lane + 2) // 4, lanes // 4)

    def own_rows(c):
        x, y = divmod(c, by)
        o = occ[pl.ds(c, nocc, stride=cells), :]
        v = vir[pl.ds(c, nvir, stride=cells), :]
        return x, y, o, v

    taken[0].wait()
    taken[1].wait()
    for c in range(cells):
        x, y, o, v = own_rows(c)
        W[x + 4, y + 4, 0:nocc] = o
        W[x + 4, y + 4, nocc:nocc + nvir] = v
    pl.semaphore_wait(barrier, n_plane - 1 + ny - 1)

    copies = []

    def put(src, dst, device):
        k = len(copies)
        c = pltpu.make_async_remote_copy(
            src_ref=src, dst_ref=dst, send_sem=send.at[k], recv_sem=recv.at[k],
            device_id=device, device_id_type=MESH,
        )
        c.start()
        copies.append(c)
        return c

    in_x, in_y = pl.ds(4, bx), pl.ds(4, by)

    def near_src(b, side):
        return pl.ds(b + 2, 2) if side == 0 else pl.ds(4, 2)

    def near_dst(b, side):
        return pl.ds(2, 2) if side == 0 else pl.ds(b + 4, 2)

    def layer_src(side, depth):
        return pl.ds(jnp.where(side == 0, by + 4 - depth, 3 + depth), 1)

    def layer_dst(side, depth):
        return pl.ds(jnp.where(side == 0, 4 - depth, by + 3 + depth), 1)

    def far_src(b, side):
        return pl.ds(b, 2) if side == 0 else pl.ds(6, 2)

    def far_dst(b, side):
        return pl.ds(0, 2) if side == 0 else pl.ds(b + 6, 2)

    def arm_src(b, side):
        return pl.ds(b, 2) if side == 0 else pl.ds(2, 2)

    def arm_dst(b, side):
        return pl.ds(0, 2) if side == 0 else pl.ds(b + 2, 2)

    zsides = range(1 if nz == 2 else 2)
    both = range(2)
    def layer_copy(s, depth):
        k = 2 * (depth - 1) + s
        return pltpu.make_async_remote_copy(
            src_ref=W.at[in_x, layer_src(s, depth)], dst_ref=W.at[in_x, layer_dst(s, depth)],
            send_sem=sendy.at[k], recv_sem=recvy.at[k],
            device_id=beside("gy", s), device_id_type=MESH,
        )

    far_round = jnp.where(gy == ny - 1, 0, 1)
    for depth in (1, 2):
        layer_copy(far_round, depth).start()
        layer_copy(1 - far_round, depth).start()
    near_y = [[layer_copy(s, depth) for s in both] for depth in (1, 2)]
    near_x = [
        put(W.at[near_src(bx, s), in_y], W.at[near_dst(bx, s), in_y], beside("gx", s)) for s in both
    ]
    taken[2].wait()
    taken[3].wait()
    packed = jnp.zeros((nocc, lanes), F32)
    for c in range(cells):
        x, y, o, v = own_rows(c)
        packed += pltpu.roll(jnp.where(at_edge, o, 0.0), 4 * c, 1)
        packed += pltpu.roll(jnp.where(at_edge, v, 0.0), 4 * c + half, 1)
        g = [grd[pl.ds(k * cells + c, 1), :] for k in range(3)]
        f = [ker[pl.ds(k * cells + c, 1), :] for k in range(4)]
        k1, k2, k3 = f[1] * (1.0 / 12.0), f[2] * (1.0 / 144.0), f[3] * (1.0 / 144.0)
        C[x, y] = jnp.concatenate(g + [k1, k2, k3, f[0], f[0]], axis=0)
        for m, ref in ((0, A0.at[x + 2, y]), (1, A1.at[x, y + 2])):
            q = k2 * g[m]
            a = [q * g[k] + k3 if k == m else q * g[k] for k in range(3)]
            ref[...] = jnp.concatenate(a + [k1 * g[m]], axis=0)
    pk[...] = packed
    z_in = [put(pk, wz.at[s], beside("gz", s)) for s in zsides]
    arm_x = [put(A0.at[arm_src(bx, s)], A0.at[arm_dst(bx, s)], beside("gx", s)) for s in both]
    arm_y = [
        put(A1.at[:, arm_src(by, s)], A1.at[:, arm_dst(by, s)], beside("gy", s)) for s in both
    ]

    def multiply(count, place, unroll=2):
        def body(t, carry):
            x, y = place(t)
            v = W[x, y, nocc:nocc + nvir]
            for i in range(nocc):
                N[x, y - 2, i] = W[x, y, i:i + 1] * v
            return carry

        lax.fori_loop(0, count, body, 0, unroll=unroll)

    def rim(t, b, lo, hi):
        return jnp.where(t < 2, t + lo, t + hi)

    multiply(cells, lambda t: (4 + t // by, 4 + lax.rem(t, by)))

    for c in z_in:
        c.wait_recv()
    low = (lanes_of((nocc, lanes)) & 3) < 2
    z_edges = wz[0] if nz == 2 else jnp.where(low, wz[1], wz[0])
    pkn[...] = z_edges
    turn_x = [put(pkn, px.at[s], beside("gx", s)) for s in both]
    turn_y = [put(pkn, py.at[s], beside("gy", s)) for s in both]
    far_x = [
        put(W.at[far_src(bx, s), in_y], W.at[far_dst(bx, s), in_y], beside("gx", s)) for s in both
    ]
    far_y = [
        put(W.at[in_x, far_src(by, s)], W.at[in_x, far_dst(by, s)], beside("gy", s)) for s in both
    ]

    def prepare(x, y, edges, c, fold):
        ao = pltpu.roll(edges, lax.rem(lanes - 4 * c, lanes), 1)
        av = pltpu.roll(edges, lax.rem(lanes + half - 4 * c, lanes), 1)
        o_own, v_own = W[x, y, 0:nocc], W[x, y, nocc:nocc + nvir]
        for k, s in enumerate(SHIFTS):
            m = lane < s if s > 0 else lane >= lanes + s
            scale = 8.0 if abs(s) == 1 else 1.0
            factor = scale if fold is None else scale * fold
            oS[k, x - 2, y - 2] = factor * pltpu.roll(jnp.where(m, ao, o_own), (-s) % lanes, 1)
            vS[k, x - 2, y - 2] = pltpu.roll(jnp.where(m, av, v_own), (-s) % lanes, 1)

    def prepare_center(t, carry):
        prepare(4 + t // by, 4 + lax.rem(t, by), pkn[...], t, None)
        return carry

    lax.fori_loop(0, cells, prepare_center, 0, unroll=4)

    own_o, own_v = pk[...], pltpu.roll(pk[...], half, 1)
    nb_o, nb_v = z_edges, pltpu.roll(z_edges, half, 1)
    for i in range(nocc):
        gap = nb_o[i:i + 1] * nb_v - own_o[i:i + 1] * own_v
        e = jnp.where(slot < cells, edge_terms(gap, lane), 0.0)
        LE[i] = e
        LEL[i] = rest(e)

    def slope_z(x, y, i, shifted):
        p = [oS[k, x + 2, y + 2, i:i + 1] * shifted[k] for k in range(4)]
        return (p[0] - p[1]) - (p[2] - p[3])

    def n_at(x, y, i):
        return N[x + 4, y + 2, i]

    def own_pass(x, carry):
        for y in range(by):
            shifted = [vS[k, x + 2, y + 2] for k in range(4)]
            for i in range(nocc):
                NL[x, y, i] = rest(n_at(x, y, i))
                S2[x, y, i] = slope_z(x, y, i, shifted)
        return carry

    lax.fori_loop(0, bx, own_pass, 0)

    for c in near_x:
        c.wait_recv()
    multiply(4 * by, lambda t: (rim(t // by, bx, 2, bx + 2), 4 + lax.rem(t, by)))

    def x_pass(x, carry):
        for y in range(by):
            g0, g2 = C[x, y, 0:1], C[x, y, 2:3]
            for i in range(nocc):
                s0 = difference(lambda t: n_at(x + t, y, i))
                S0[x, y, i] = s0
                S0L[x, y, i] = rest(s0)
                AL[x, y, i] = g0 * s0 + g2 * S2[x, y, i]
        return carry

    lax.fori_loop(0, bx, x_pass, 0)

    def second_pass_cell(x, y, lo):
        g0, g1, g2, k1, k2, k3, kk = (C[x, y, k:k + 1] for k in range(7))
        c = x * by + y
        for i in range(nocc):
            n = n_at(x, y, i)
            s1 = difference(lambda t: n_at(x, y + t, i))
            al = AL[x, y, i] + g1 * s1
            sc = k1 * n + k2 * al
            fl0 = sc * g0 + k3 * S0[x, y, i]
            fl1 = sc * g1 + k3 * s1
            fl2 = sc * g2 + k3 * S2[x, y, i]
            b = (kk * n + k1 * al) - difference(lambda t: pltpu.roll(fl2, (-t) % lanes, 1))
            S1[x, y, i] = s1
            f0[x + 2, y, i] = fl0
            f1[x, y + 2, i] = fl1
            base[x, y, i] = b
            deep = (2 * i) // nocc
            j = i % (nocc // 2)
            E2[j] = jnp.where(slot == c + cells * deep, pltpu.roll(fl2, 4 * c + half * deep, 1), E2[j])
            for k, v in enumerate((s1, b, fl0, fl1)):
                LO[lo, k, i] = rest(v)

    def wide(parts):
        return jnp.concatenate([p.reshape(pairs, lanes) for p in parts], axis=1)

    def gather(x, ys, at, start):
        (l0, l1), (y0, y1) = at, ys

        def pair(high, low):
            return wide(high), wide(low)

        def orbit(lo, y):
            left = pair([N[x + 4, y + 2], S0[x, y]], [NL[x, y], S0L[x, y]])
            return left, pair([base[x, y], f0[x + 2, y]], [LO[lo, 1], LO[lo, 2]])

        first, second = orbit(l0, y0), orbit(l1, y1)
        third = (
            pair([S1[x, y0], S1[x, y1]], [LO[l0, 0], LO[l1, 0]]),
            pair([f1[x, y0 + 2], f1[x, y1 + 2]], [LO[l0, 3], LO[l1, 3]]),
        )

        def beside_(parts):
            return jnp.concatenate(parts, axis=1)

        left = [beside_([first[0][k], second[0][k]]) for k in range(2)]
        right = [beside_([first[1][k], second[1][k]]) for k in range(2)]
        top = dot(jnp.concatenate(left, axis=0), right[0])
        low_part = dot(
            beside_([left[0], third[0][0], third[0][0], third[0][1]]),
            beside_([right[1], third[1][0], third[1][1], third[1][0]]),
        )
        total = (top[0:pairs] + top[pairs:]) + low_part
        acc[...] = total if start else acc[...] + total

    def second_pass(ys, start, late):
        for x in range(bx):
            at = [2 * (x % 2), 2 * (x % 2) + 1]
            if late is not None:
                gather(*late)
            for lo, y in zip(at, ys):
                second_pass_cell(x, y, lo)
            late = (x, ys, at, start and x == 0)
        return late

    def across(depth):
        y = (4 - depth, by + 3 + depth)
        return lambda t: (4 + t // 2, jnp.where(lax.rem(t, 2) == 0, y[0], y[1]))

    def turn_corner(depth):
        return [
            put(
                W.at[near_src(bx, sx), layer_dst(sy, depth)],
                W.at[near_dst(bx, sx), layer_dst(sy, depth)],
                beside("gx", sx),
            )
            for sy in both
            for sx in both
        ]

    for c in near_y[0]:
        c.wait_recv()
    corner = turn_corner(1)
    multiply(2 * bx, across(1))
    late = second_pass((1, 2), True, None)
    for c in near_y[1]:
        c.wait_recv()
    corner += turn_corner(2)
    multiply(2 * bx, across(2))
    late = second_pass((0, 3), False, late)
    gather(*late)
    ends = [E2[i % (nocc // 2)] for i in range(nocc)]
    ends = [e if 2 * i < nocc else pltpu.roll(e, half, 1) for i, e in enumerate(ends)]
    right = jnp.concatenate(ends, axis=0)
    left, left_lo = LE[...].reshape(pairs, lanes), LEL[...].reshape(pairs, lanes)
    total = acc[...] + (dot(left, right) + dot(left_lo, right) + dot(left, rest(right)))
    for tx in range(nx):
        for ty in range(ny):
            for tz in range(nz):
                r = ((tx * ny + ty) * nz + tz) * rows_out
                part[tx, ty, tz] = total[r:r + rows_out]
    first = []
    for d in sorted(range(1, n_plane), key=lambda d: abs(2 * d - n_plane)):
        tx, tz, target = plane(d)
        c = pltpu.make_async_remote_copy(
            src_ref=part.at[tx, :, tz], dst_ref=got.at[d],
            send_sem=send1.at[d], recv_sem=recv1.at[d],
            device_id=target, device_id_type=MESH,
        )
        c.start()
        first.append(c)
    z_out = [put(E2, ez.at[s], beside("gz", s)) for s in zsides]

    for c in turn_x + arm_x:
        c.wait_recv()

    def prepare_x(t, carry):
        k, y = t // by, lax.rem(t, by)
        side = k // 2
        c = jnp.where(k < 2, k + bx - 2, k - 2) * by + y
        a = rim(k, bx, 0, bx)
        prepare(a + 2, 4 + y, px[side], c, A0[a, y, 2:3])
        return carry

    lax.fori_loop(0, 4 * by, prepare_x, 0, unroll=4)

    for c in far_x + corner:
        c.wait_recv()
    multiply(4 * by, lambda t: (rim(t // by, bx, 0, bx + 4), 4 + lax.rem(t, by)))
    multiply(16, lambda t: (rim(t // 4, bx, 2, bx + 2), rim(lax.rem(t, 4), by, 2, by + 2)))

    def at_x(t, carry):
        a, y = rim(t // by, bx, 0, bx), lax.rem(t, by)
        x = a - 2
        shifted = [vS[k, a, y + 2] for k in range(4)]
        c0, c1, c3 = A0[a, y, 0:1], A0[a, y, 1:2], A0[a, y, 3:4]
        for i in range(nocc):
            s0 = difference(lambda t: n_at(x + t, y, i))
            s1 = difference(lambda t: n_at(x, y + t, i))
            f0[a, y, i] = (c0 * s0 + c1 * s1) + (slope_z(x, y, i, shifted) + c3 * n_at(x, y, i))
        return carry

    lax.fori_loop(0, 4 * by, at_x, 0)

    for c in turn_y + arm_y:
        c.wait_recv()

    def prepare_y(t, carry):
        x, k = t // 4, lax.rem(t, 4)
        side = k // 2
        c = x * by + jnp.where(k < 2, k + by - 2, k - 2)
        b = rim(k, by, 0, by)
        prepare(4 + x, b + 2, py[side], c, A1[x, b, 2:3])
        return carry

    lax.fori_loop(0, 4 * bx, prepare_y, 0, unroll=4)

    def at_y(x, carry):
        for y in (-2, -1, by, by + 1):
            b = y + 2
            shifted = [vS[k, x + 2, b] for k in range(4)]
            c0, c1, c3 = A1[x, b, 0:1], A1[x, b, 1:2], A1[x, b, 3:4]
            for i in range(nocc):
                s0 = difference(lambda t: n_at(x + t, y, i))
                n = lambda t: n_at(x, y + t, i)
                if y == -2:
                    s1 = 8.0 * n(1) - n(2)
                elif y == -1:
                    s1 = 8.0 * (n(1) - n(-1)) - n(2)
                elif y == by:
                    s1 = 8.0 * (n(1) - n(-1)) + n(-2)
                else:
                    s1 = n(-2) - 8.0 * n(-1)
                f1[x, b, i] = (c0 * s0 + c1 * s1) + (slope_z(x, y, i, shifted) + c3 * n(0))
        return carry

    lax.fori_loop(0, bx, at_y, 0)

    for c in first:
        c.wait_recv()
    mine = part[gx, :, gz]
    for d in range(1, n_plane):
        mine = mine + got[d]
    acc2[...] = mine
    second = []
    for d in range(1, ny):
        t, target = column(d)
        c = pltpu.make_async_remote_copy(
            src_ref=acc2.at[t], dst_ref=got2.at[d],
            send_sem=send2.at[d], recv_sem=recv2.at[d],
            device_id=target, device_id_type=MESH,
        )
        c.start()
        second.append(c)

    for c in z_out:
        c.wait_recv()
    for j in range(nocc // 2):
        outer = ez[0, j] if nz == 2 else jnp.where((lane & 3) < 2, ez[1, j], ez[0, j])
        corr[j] = edge_terms(outer - E2[j], lane)
    for c in far_y:
        c.wait_recv()

    def assemble(x, carry):
        def far(y):
            return W[x + 4, y + 4, nocc:nocc + nvir]

        def slope_of(y):
            return A1[x, y + 2, 1:2]

        low1 = slope_of(-1) * far(-3)
        low2 = (slope_of(-2) * far(-4), -8.0 * slope_of(-2) * far(-3))
        top1 = -1.0 * slope_of(by) * far(by + 2)
        top2 = (8.0 * slope_of(by + 1) * far(by + 2), -1.0 * slope_of(by + 1) * far(by + 3))
        for i in range(nocc):
            o = [W[x + 4, y + 4, i:i + 1] for y in (-4, -3, by + 2, by + 3)]
            a = [f1[x, b, i] for b in range(by + 4)]
            a[0] = a[0] + (o[0] * low2[0] + o[1] * low2[1])
            a[1] = a[1] + o[1] * low1
            a[by + 2] = a[by + 2] + o[2] * top1
            a[by + 3] = a[by + 3] + (o[2] * top2[0] + o[3] * top2[1])
            deep = (2 * i) // nocc
            e = corr[i % (nocc // 2)]
            for y in range(by):
                c = x * by + y
                b = [f0[x + k, y, i] for k in (0, 1, 3, 4)]
                inner = (b[2] - b[1]) + (a[y + 3] - a[y + 1])
                outer = (b[3] - b[0]) + (a[y + 4] - a[y])
                turned = pltpu.roll(e, lax.rem(2 * lanes - 4 * c - half * deep, lanes), 1)
                v = base[x, y, i] - (8.0 * inner - outer)
                v = v - jnp.where(at_edge, turned, 0.0)
                pot[pl.ds(i * nvir * cells + c, nvir, stride=cells), :] = v
        return carry

    lax.fori_loop(0, bx, assemble, 0)
    for c in copies + near_y[0] + near_y[1] + first + second:
        c.wait_send()
    mine = acc2[gy]
    for d, c in enumerate(second):
        c.wait_recv()
        mine = mine + got2[d + 1]
    cas[...] = mine * (1.0 / (cells * lanes * nx * ny * nz))


def write_kernel(pot_in, cas_in, pot, cas, sem):
    parts = sem.shape[0] - 1
    rows = pot_in.shape[0] // parts
    out = [pltpu.make_async_copy(cas_in, cas, sem.at[parts])]
    for k in range(parts):
        block = pl.ds(k * rows, rows)
        out.append(pltpu.make_async_copy(pot_in.at[block], pot.at[block], sem.at[k]))
    for c in out:
        c.start()
    for c in out:
        c.wait()


def on_device(occupied, virtual, kernel_fields, density_grad):
    nocc, bx, by, lanes = occupied.shape
    nvir = virtual.shape[0]
    nx, ny, nz = (lax.axis_size(a) for a in ("gx", "gy", "gz"))
    devices = nx * ny * nz
    cells = bx * by
    pairs = nocc * nvir
    norb = nocc + nvir
    rows = pairs // devices
    sds = lambda *s: jax.ShapeDtypeStruct(s, F32)
    v32 = lambda *s: pltpu.VMEM(s, F32)
    dma = lambda n: pltpu.SemaphoreType.DMA((n,))
    vmem = pl.BlockSpec(memory_space=pltpu.VMEM)
    hbm = pl.BlockSpec(memory_space=pltpu.HBM)
    zs = 1 if nz == 2 else 2
    flat = lambda a: a.reshape(-1, lanes)
    outs = pl.pallas_call(
        flow_kernel,
        out_shape=(v32(pairs * cells, lanes), v32(rows, pairs)),
        in_specs=[hbm] * 4,
        out_specs=[vmem] * 2,
        scratch_shapes=[
            v32(nocc * cells, lanes), v32(nvir * cells, lanes), v32(4 * cells, lanes), v32(3 * cells, lanes),
            v32(bx + 8, by + 8, norb, lanes),
            v32(bx + 8, by + 4, nocc, nvir, lanes),
            v32(4, bx + 4, by + 4, nocc, lanes),
            v32(4, bx + 4, by + 4, nvir, lanes),
        ]
        + [v32(bx, by, nocc, nvir, lanes)] * 6
        + [
            v32(4, 4, nocc, nvir, lanes),
            v32(bx + 4, by, nocc, nvir, lanes),
            v32(bx, by + 4, nocc, nvir, lanes),
            v32(bx, by, nocc, nvir, lanes),
            v32(bx, by, 8, lanes), v32(bx + 4, by, 4, lanes), v32(bx, by + 4, 4, lanes),
            v32(nocc, lanes), v32(zs, nocc, lanes), v32(nocc, lanes), v32(2, nocc, lanes), v32(2, nocc, lanes),
            v32(nocc // 2, nvir, lanes), v32(zs, nocc // 2, nvir, lanes), v32(nocc // 2, nvir, lanes),
            v32(nocc, nvir, lanes), v32(nocc, nvir, lanes),
            v32(pairs, pairs),
            v32(nx, ny, nz, rows, pairs),
            v32(nx * nz, ny, rows, pairs),
            v32(ny, rows, pairs), v32(ny, rows, pairs),
            dma(28), dma(28), dma(4), dma(4), dma(4), dma(nx * nz), dma(nx * nz), dma(ny), dma(ny),
        ],
        compiler_params=pltpu.CompilerParams(
            collective_id=0, has_side_effects=True, vmem_limit_bytes=54 * MIB
        ),
        name="flow",
    )(*(pltpu.with_memory_space_constraint(flat(a), pltpu.HBM) for a in (occupied, virtual, kernel_fields, density_grad)))
    pot, casida = pl.pallas_call(
        write_kernel,
        out_shape=(sds(pairs * cells, lanes), sds(rows, pairs)),
        in_specs=[vmem] * 2,
        out_specs=(hbm, hbm),
        scratch_shapes=[dma(9)],
        compiler_params=pltpu.CompilerParams(vmem_limit_bytes=4 * MIB),
        name="write",
    )(*outs)
    return pot.reshape(pairs, bx, by, lanes), casida


def solution(mesh):
    spec = P(None, "gx", "gy", "gz")
    return jax.shard_map(
        on_device,
        mesh=mesh,
        in_specs=(spec,) * 4,
        out_specs=(spec, P(("gx", "gy", "gz"), None)),
        check_vma=False,
    )
```

```python
import functools

import jax
import jax.numpy as jnp
from jax import lax
from jax.experimental import pallas as pl
from jax.experimental.pallas import tpu as pltpu
from jax.sharding import PartitionSpec as P

MESH = pl.DeviceIdType.MESH
F32 = jnp.float32
BF16 = jnp.bfloat16
SHIFTS = (1, -1, 2, -2)
MIB = 1024 * 1024


def difference(f):
    return 8.0 * (f(1) - f(-1)) - (f(2) - f(-2))


def lanes_of(shape):
    return lax.broadcasted_iota(jnp.int32, shape, len(shape) - 1)


def edge_terms(gap, lane):
    axis = gap.ndim - 1
    lanes = gap.shape[axis]
    at = lane & 3
    two = jnp.where(at >= 2, -pltpu.roll(gap, lanes - 2, axis), pltpu.roll(gap, 2, axis))
    one = jnp.where(at == 3, pltpu.roll(gap, lanes - 1, axis), -pltpu.roll(gap, 1, axis))
    return two + jnp.where((at == 3) | (at == 0), 8.0 * one, 0.0)


def rest(v):
    return v - v.astype(BF16).astype(F32)


def dot(a, b):
    return lax.dot_general(a, b, (((1,), (1,)), ((), ())), preferred_element_type=F32)


def flow_kernel(
    occ_in, vir_in, ker_in, grd_in,
    pot, cas,
    occ, vir, ker, grd, W, N, oS, vS, S0, S1, S2, AL, NL, S0L, LO, f0, f1, base, C, A0, A1,
    pk, wz, pkn, px, py, E2, ez, corr, LE, LEL,
    acc, part, got, acc2, got2,
    send, recv, sendy, recvy, own, send1, recv1, send2, recv2,
):
    nx, ny, nz = (lax.axis_size(a) for a in ("gx", "gy", "gz"))
    gx, gy, gz = (lax.axis_index(a) for a in ("gx", "gy", "gz"))
    bx, by = base.shape[0], base.shape[1]
    cells = bx * by
    lanes = occ.shape[1]
    half = lanes // 2
    nocc, nvir = occ.shape[0] // cells, vir.shape[0] // cells
    pairs = nocc * nvir
    rows_out = cas.shape[0]
    n_plane = nx * nz
    me = gx * nz + gz

    def plane(d):
        t = lax.rem(me + d, n_plane)
        tx, tz = t // nz, lax.rem(t, nz)
        return tx, tz, {"gx": tx, "gy": gy, "gz": tz}

    def column(d):
        t = lax.rem(gy + d, ny)
        return t, {"gx": gx, "gy": t, "gz": gz}

    def beside(axis, side):
        v, n = {"gx": (gx, nx), "gy": (gy, ny), "gz": (gz, nz)}[axis]
        where = {"gx": gx, "gy": gy, "gz": gz}
        step = (1, n - 1)[side] if isinstance(side, int) else jnp.where(side == 0, 1, n - 1)
        where[axis] = lax.rem(v + step, n)
        return where

    taken = [
        pltpu.make_async_copy(a, b, own.at[k])
        for k, (a, b) in enumerate(((occ_in, occ), (vir_in, vir), (ker_in, ker), (grd_in, grd)))
    ]
    for c in taken:
        c.start()
    barrier = pltpu.get_barrier_semaphore()
    for d in range(1, n_plane):
        pl.semaphore_signal(barrier, inc=1, device_id=plane(d)[2], device_id_type=MESH)
    for d in range(1, ny):
        pl.semaphore_signal(barrier, inc=1, device_id=column(d)[1], device_id_type=MESH)

    E2[...] = jnp.zeros_like(E2)
    lane = lanes_of((nvir, lanes))
    at_edge = (lane < 2) | (lane >= lanes - 2)
    slot = lax.rem((lane + 2) // 4, lanes // 4)

    def own_rows(c):
        x, y = divmod(c, by)
        o = occ[pl.ds(c, nocc, stride=cells), :]
        v = vir[pl.ds(c, nvir, stride=cells), :]
        return x, y, o, v

    taken[0].wait()
    taken[1].wait()
    for c in range(cells):
        x, y, o, v = own_rows(c)
        W[x + 4, y + 4, 0:nocc] = o
        W[x + 4, y + 4, nocc:nocc + nvir] = v
    copies = []

    def put(src, dst, device):
        k = len(copies)
        c = pltpu.make_async_remote_copy(
            src_ref=src, dst_ref=dst, send_sem=send.at[k], recv_sem=recv.at[k],
            device_id=device, device_id_type=MESH,
        )
        c.start()
        copies.append(c)
        return c

    taken[2].wait()
    taken[3].wait()
    packed = jnp.zeros((nocc, lanes), F32)
    for c in range(cells):
        x, y, o, v = own_rows(c)
        packed += pltpu.roll(jnp.where(at_edge, o, 0.0), 4 * c, 1)
        packed += pltpu.roll(jnp.where(at_edge, v, 0.0), 4 * c + half, 1)
        g = [grd[pl.ds(k * cells + c, 1), :] for k in range(3)]
        f = [ker[pl.ds(k * cells + c, 1), :] for k in range(4)]
        k1, k2, k3 = f[1] * (1.0 / 12.0), f[2] * (1.0 / 144.0), f[3] * (1.0 / 144.0)
        C[x, y] = jnp.concatenate(g + [k1, k2, k3, f[0], f[0]], axis=0)
        for m, ref in ((0, A0.at[x + 2, y]), (1, A1.at[x, y + 2])):
            q = k2 * g[m]
            a = [q * g[k] + k3 if k == m else q * g[k] for k in range(3)]
            ref[...] = jnp.concatenate(a + [k1 * g[m]], axis=0)
    pk[...] = packed

    def multiply(count, place, unroll=2):
        def body(t, carry):
            x, y = place(t)
            v = W[x, y, nocc:nocc + nvir]
            for i in range(nocc):
                N[x, y - 2, i] = W[x, y, i:i + 1] * v
            return carry

        lax.fori_loop(0, count, body, 0, unroll=unroll)

    def rim(t, b, lo, hi):
        return jnp.where(t < 2, t + lo, t + hi)

    multiply(cells, lambda t: (4 + t // by, 4 + lax.rem(t, by)))

    pl.semaphore_wait(barrier, n_plane - 1 + ny - 1)
    in_x, in_y = pl.ds(4, bx), pl.ds(4, by)

    def near_src(b, side):
        return pl.ds(b + 2, 2) if side == 0 else pl.ds(4, 2)

    def near_dst(b, side):
        return pl.ds(2, 2) if side == 0 else pl.ds(b + 4, 2)

    def layer_src(side, depth):
        return pl.ds(jnp.where(side == 0, by + 4 - depth, 3 + depth), 1)

    def layer_dst(side, depth):
        return pl.ds(jnp.where(side == 0, 4 - depth, by + 3 + depth), 1)

    def far_src(b, side):
        return pl.ds(b, 2) if side == 0 else pl.ds(6, 2)

    def far_dst(b, side):
        return pl.ds(0, 2) if side == 0 else pl.ds(b + 6, 2)

    def arm_src(b, side):
        return pl.ds(b, 2) if side == 0 else pl.ds(2, 2)

    def arm_dst(b, side):
        return pl.ds(0, 2) if side == 0 else pl.ds(b + 2, 2)

    zsides = range(1 if nz == 2 else 2)
    both = range(2)
    def layer_copy(s, depth):
        k = 2 * (depth - 1) + s
        return pltpu.make_async_remote_copy(
            src_ref=W.at[in_x, layer_src(s, depth)], dst_ref=W.at[in_x, layer_dst(s, depth)],
            send_sem=sendy.at[k], recv_sem=recvy.at[k],
            device_id=beside("gy", s), device_id_type=MESH,
        )

    far_round = jnp.where(gy == ny - 1, 0, 1)
    for depth in (1, 2):
        layer_copy(far_round, depth).start()
        layer_copy(1 - far_round, depth).start()
    near_y = [[layer_copy(s, depth) for s in both] for depth in (1, 2)]
    z_in = [put(pk, wz.at[s], beside("gz", s)) for s in zsides]

    def x_copy(s):
        return pltpu.make_async_remote_copy(
            src_ref=W.at[pl.ds(jnp.where(s == 0, bx + 2, 4), 2), in_y],
            dst_ref=W.at[pl.ds(jnp.where(s == 0, 2, bx + 4), 2), in_y],
            send_sem=sendy.at[4 + s], recv_sem=recvy.at[4 + s],
            device_id=beside("gx", s), device_id_type=MESH,
        )

    near_x = [x_copy(s) for s in both]
    for c in near_x:
        c.start()
    arm_x = [put(A0.at[arm_src(bx, s)], A0.at[arm_dst(bx, s)], beside("gx", s)) for s in both]
    arm_y = [
        put(A1.at[:, arm_src(by, s)], A1.at[:, arm_dst(by, s)], beside("gy", s)) for s in both
    ]

    def low_pass(x, carry):
        for y in range(by):
            for i in range(nocc):
                NL[x, y, i] = rest(N[x + 4, y + 2, i])
        return carry

    lax.fori_loop(0, bx, low_pass, 0)
    for c in z_in:
        c.wait_recv()
    low = (lanes_of((nocc, lanes)) & 3) < 2
    z_edges = wz[0] if nz == 2 else jnp.where(low, wz[1], wz[0])
    pkn[...] = z_edges
    turn_x = [put(pkn, px.at[s], beside("gx", s)) for s in both]
    turn_y = [put(pkn, py.at[s], beside("gy", s)) for s in both]
    far_x = [
        put(W.at[far_src(bx, s), in_y], W.at[far_dst(bx, s), in_y], beside("gx", s)) for s in both
    ]
    far_y = [
        put(W.at[in_x, far_src(by, s)], W.at[in_x, far_dst(by, s)], beside("gy", s)) for s in both
    ]

    def prepare(x, y, edges, c, fold):
        ao = pltpu.roll(edges, (lanes - 4 * c) % lanes, 1)
        av = pltpu.roll(edges, (lanes + half - 4 * c) % lanes, 1)
        o_own, v_own = W[x, y, 0:nocc], W[x, y, nocc:nocc + nvir]
        for k, s in enumerate(SHIFTS):
            m = lane < s if s > 0 else lane >= lanes + s
            scale = 8.0 if abs(s) == 1 else 1.0
            factor = scale if fold is None else scale * fold
            oS[k, x - 2, y - 2] = factor * pltpu.roll(jnp.where(m, ao, o_own), (-s) % lanes, 1)
            vS[k, x - 2, y - 2] = pltpu.roll(jnp.where(m, av, v_own), (-s) % lanes, 1)

    for t in range(cells):
        prepare(4 + t // by, 4 + t % by, z_edges, t, None)

    own_o, own_v = pk[...], pltpu.roll(pk[...], half, 1)
    nb_o, nb_v = z_edges, pltpu.roll(z_edges, half, 1)
    for i in range(nocc):
        gap = nb_o[i:i + 1] * nb_v - own_o[i:i + 1] * own_v
        e = jnp.where(slot < cells, edge_terms(gap, lane), 0.0)
        LE[i] = e
        LEL[i] = rest(e)

    def slope_z(x, y, i, shifted):
        p = [oS[k, x + 2, y + 2, i:i + 1] * shifted[k] for k in range(4)]
        return (p[0] - p[1]) - (p[2] - p[3])

    def n_at(x, y, i):
        return N[x + 4, y + 2, i]

    def own_pass(x, carry):
        for y in range(by):
            shifted = [vS[k, x + 2, y + 2] for k in range(4)]
            for i in range(nocc):
                S2[x, y, i] = slope_z(x, y, i, shifted)
        return carry

    lax.fori_loop(0, bx, own_pass, 0)

    early = 1 - lax.rem(gx, 2)
    x_done = [early, 1 - early]
    def x_pass(x, carry):
        for y in range(by):
            g0, g2 = C[x, y, 0:1], C[x, y, 2:3]
            for i in range(nocc):
                s0 = difference(lambda t: n_at(x + t, y, i))
                S0[x, y, i] = s0
                S0L[x, y, i] = rest(s0)
                AL[x, y, i] = g0 * s0 + g2 * S2[x, y, i]
        return carry

    for s in x_done:
        x_copy(s).wait_recv()
        at = jnp.where(s == 0, 2, bx + 4)
        multiply(2 * by, lambda t: (at + t // by, 4 + lax.rem(t, by)))
        lo = jnp.where(s == 0, 0, bx - 2)
        lax.fori_loop(0, 2, lambda t, carry: x_pass(lo + t, carry), 0)

    def second_pass_cell(x, y, lo):
        g0, g1, g2, k1, k2, k3, kk = (C[x, y, k:k + 1] for k in range(7))
        c = x * by + y
        for i in range(nocc):
            n = n_at(x, y, i)
            s1 = difference(lambda t: n_at(x, y + t, i))
            al = AL[x, y, i] + g1 * s1
            sc = k1 * n + k2 * al
            fl0 = sc * g0 + k3 * S0[x, y, i]
            fl1 = sc * g1 + k3 * s1
            fl2 = sc * g2 + k3 * S2[x, y, i]
            b = (kk * n + k1 * al) - difference(lambda t: pltpu.roll(fl2, (-t) % lanes, 1))
            S1[x, y, i] = s1
            f0[x + 2, y, i] = fl0
            f1[x, y + 2, i] = fl1
            base[x, y, i] = b
            deep = (2 * i) // nocc
            j = i % (nocc // 2)
            E2[j] = jnp.where(slot == c + cells * deep, pltpu.roll(fl2, 4 * c + half * deep, 1), E2[j])
            for k, v in enumerate((s1, b, fl0, fl1)):
                LO[lo, k, i] = rest(v)

    def wide(parts):
        return jnp.concatenate([p.reshape(pairs, lanes) for p in parts], axis=1)

    def gather(x, ys, at, start):
        (l0, l1), (y0, y1) = at, ys

        def pair(high, low):
            return wide(high), wide(low)

        def orbit(lo, y):
            left = pair([N[x + 4, y + 2], S0[x, y]], [NL[x, y], S0L[x, y]])
            return left, pair([base[x, y], f0[x + 2, y]], [LO[lo, 1], LO[lo, 2]])

        first, second = orbit(l0, y0), orbit(l1, y1)
        third = (
            pair([S1[x, y0], S1[x, y1]], [LO[l0, 0], LO[l1, 0]]),
            pair([f1[x, y0 + 2], f1[x, y1 + 2]], [LO[l0, 3], LO[l1, 3]]),
        )

        def beside_(parts):
            return jnp.concatenate(parts, axis=1)

        left = [beside_([first[0][k], second[0][k]]) for k in range(2)]
        right = [beside_([first[1][k], second[1][k]]) for k in range(2)]
        top = dot(jnp.concatenate(left, axis=0), right[0])
        low_part = dot(
            beside_([left[0], third[0][0], third[0][0], third[0][1]]),
            beside_([right[1], third[1][0], third[1][1], third[1][0]]),
        )
        total = (top[0:pairs] + top[pairs:]) + low_part
        acc[...] = total if start else acc[...] + total

    def second_pass(ys, start, late):
        for x in range(bx):
            at = [2 * (x % 2), 2 * (x % 2) + 1]
            if late is not None:
                gather(*late)
            for lo, y in zip(at, ys):
                second_pass_cell(x, y, lo)
            late = (x, ys, at, start and x == 0)
        return late

    def across(depth):
        y = (4 - depth, by + 3 + depth)
        return lambda t: (4 + t // 2, jnp.where(lax.rem(t, 2) == 0, y[0], y[1]))

    def turn_corner(depth):
        return [
            put(
                W.at[near_src(bx, sx), layer_dst(sy, depth)],
                W.at[near_dst(bx, sx), layer_dst(sy, depth)],
                beside("gx", sx),
            )
            for sy in both
            for sx in both
        ]

    for c in near_y[0]:
        c.wait_recv()
    corner = turn_corner(1)
    multiply(2 * bx, across(1))
    late = second_pass((1, 2), True, None)
    for c in near_y[1]:
        c.wait_recv()
    corner += turn_corner(2)
    multiply(2 * bx, across(2))
    late = second_pass((0, 3), False, late)
    gather(*late)
    ends = [E2[i % (nocc // 2)] for i in range(nocc)]
    ends = [e if 2 * i < nocc else pltpu.roll(e, half, 1) for i, e in enumerate(ends)]
    right = jnp.concatenate(ends, axis=0)
    left, left_lo = LE[...].reshape(pairs, lanes), LEL[...].reshape(pairs, lanes)
    total = acc[...] + (dot(left, right) + dot(left_lo, right) + dot(left, rest(right)))
    for tx in range(nx):
        for ty in range(ny):
            for tz in range(nz):
                r = ((tx * ny + ty) * nz + tz) * rows_out
                part[tx, ty, tz] = total[r:r + rows_out]
    first = []
    for d in sorted(range(1, n_plane), key=lambda d: abs(2 * d - n_plane)):
        tx, tz, target = plane(d)
        c = pltpu.make_async_remote_copy(
            src_ref=part.at[tx, :, tz], dst_ref=got.at[d],
            send_sem=send1.at[d], recv_sem=recv1.at[d],
            device_id=target, device_id_type=MESH,
        )
        c.start()
        first.append(c)
    z_out = [put(E2, ez.at[s], beside("gz", s)) for s in zsides]

    for c in turn_x + arm_x:
        c.wait_recv()

    for a in (0, 1, bx + 2, bx + 3):
        edges = px[0] if a < 2 else px[1]
        for y in range(by):
            prepare(a + 2, 4 + y, edges, (a - 2) % bx * by + y, A0[a, y, 2:3])

    for c in far_x + corner:
        c.wait_recv()
    multiply(4 * by, lambda t: (rim(t // by, bx, 0, bx + 4), 4 + lax.rem(t, by)))
    multiply(16, lambda t: (rim(t // 4, bx, 2, bx + 2), rim(lax.rem(t, 4), by, 2, by + 2)))

    def at_x(t, carry):
        a, y = rim(t // by, bx, 0, bx), lax.rem(t, by)
        x = a - 2
        shifted = [vS[k, a, y + 2] for k in range(4)]
        c0, c1, c3 = A0[a, y, 0:1], A0[a, y, 1:2], A0[a, y, 3:4]
        for i in range(nocc):
            s0 = difference(lambda t: n_at(x + t, y, i))
            s1 = difference(lambda t: n_at(x, y + t, i))
            f0[a, y, i] = (c0 * s0 + c1 * s1) + (slope_z(x, y, i, shifted) + c3 * n_at(x, y, i))
        return carry

    lax.fori_loop(0, 4 * by, at_x, 0)

    for c in turn_y + arm_y:
        c.wait_recv()

    for b in (0, 1, by + 2, by + 3):
        edges = py[0] if b < 2 else py[1]
        for x in range(bx):
            prepare(4 + x, b + 2, edges, x * by + (b - 2) % by, A1[x, b, 2:3])

    def at_y(x, carry):
        for y in (-2, -1, by, by + 1):
            b = y + 2
            shifted = [vS[k, x + 2, b] for k in range(4)]
            c0, c1, c3 = A1[x, b, 0:1], A1[x, b, 1:2], A1[x, b, 3:4]
            for i in range(nocc):
                s0 = difference(lambda t: n_at(x + t, y, i))
                n = lambda t: n_at(x, y + t, i)
                if y == -2:
                    s1 = 8.0 * n(1) - n(2)
                elif y == -1:
                    s1 = 8.0 * (n(1) - n(-1)) - n(2)
                elif y == by:
                    s1 = 8.0 * (n(1) - n(-1)) + n(-2)
                else:
                    s1 = n(-2) - 8.0 * n(-1)
                f1[x, b, i] = (c0 * s0 + c1 * s1) + (slope_z(x, y, i, shifted) + c3 * n(0))
        return carry

    lax.fori_loop(0, bx, at_y, 0)

    for c in first:
        c.wait_recv()
    mine = part[gx, :, gz]
    for d in range(1, n_plane):
        mine = mine + got[d]
    acc2[...] = mine
    second = []
    for d in range(1, ny):
        t, target = column(d)
        c = pltpu.make_async_remote_copy(
            src_ref=acc2.at[t], dst_ref=got2.at[d],
            send_sem=send2.at[d], recv_sem=recv2.at[d],
            device_id=target, device_id_type=MESH,
        )
        c.start()
        second.append(c)

    for c in z_out:
        c.wait_recv()
    for j in range(nocc // 2):
        outer = ez[0, j] if nz == 2 else jnp.where((lane & 3) < 2, ez[1, j], ez[0, j])
        corr[j] = edge_terms(outer - E2[j], lane)
    for c in far_y:
        c.wait_recv()

    def assemble(x, carry):
        def far(y):
            return W[x + 4, y + 4, nocc:nocc + nvir]

        def slope_of(y):
            return A1[x, y + 2, 1:2]

        low1 = slope_of(-1) * far(-3)
        low2 = (slope_of(-2) * far(-4), -8.0 * slope_of(-2) * far(-3))
        top1 = -1.0 * slope_of(by) * far(by + 2)
        top2 = (8.0 * slope_of(by + 1) * far(by + 2), -1.0 * slope_of(by + 1) * far(by + 3))
        for i in range(nocc):
            o = [W[x + 4, y + 4, i:i + 1] for y in (-4, -3, by + 2, by + 3)]
            a = [f1[x, b, i] for b in range(by + 4)]
            a[0] = a[0] + (o[0] * low2[0] + o[1] * low2[1])
            a[1] = a[1] + o[1] * low1
            a[by + 2] = a[by + 2] + o[2] * top1
            a[by + 3] = a[by + 3] + (o[2] * top2[0] + o[3] * top2[1])
            deep = (2 * i) // nocc
            e = corr[i % (nocc // 2)]
            for y in range(by):
                c = x * by + y
                b = [f0[x + k, y, i] for k in (0, 1, 3, 4)]
                inner = (b[2] - b[1]) + (a[y + 3] - a[y + 1])
                outer = (b[3] - b[0]) + (a[y + 4] - a[y])
                turned = pltpu.roll(e, lax.rem(2 * lanes - 4 * c - half * deep, lanes), 1)
                v = base[x, y, i] - (8.0 * inner - outer)
                v = v - jnp.where(at_edge, turned, 0.0)
                pot[pl.ds(i * nvir * cells + c, nvir, stride=cells), :] = v
        return carry

    lax.fori_loop(0, bx, assemble, 0)
    for c in copies + near_y[0] + near_y[1] + near_x + first + second:
        c.wait_send()
    mine = acc2[gy]
    for d, c in enumerate(second):
        c.wait_recv()
        mine = mine + got2[d + 1]
    cas[...] = mine * (1.0 / (cells * lanes * nx * ny * nz))


def write_kernel(pot_in, cas_in, pot, cas, sem):
    parts = sem.shape[0] - 1
    rows = pot_in.shape[0] // parts
    out = [pltpu.make_async_copy(cas_in, cas, sem.at[parts])]
    for k in range(parts):
        block = pl.ds(k * rows, rows)
        out.append(pltpu.make_async_copy(pot_in.at[block], pot.at[block], sem.at[k]))
    for c in out:
        c.start()
    for c in out:
        c.wait()


def on_device(occupied, virtual, kernel_fields, density_grad):
    nocc, bx, by, lanes = occupied.shape
    nvir = virtual.shape[0]
    nx, ny, nz = (lax.axis_size(a) for a in ("gx", "gy", "gz"))
    devices = nx * ny * nz
    cells = bx * by
    pairs = nocc * nvir
    norb = nocc + nvir
    rows = pairs // devices
    sds = lambda *s: jax.ShapeDtypeStruct(s, F32)
    v32 = lambda *s: pltpu.VMEM(s, F32)
    dma = lambda n: pltpu.SemaphoreType.DMA((n,))
    vmem = pl.BlockSpec(memory_space=pltpu.VMEM)
    hbm = pl.BlockSpec(memory_space=pltpu.HBM)
    zs = 1 if nz == 2 else 2
    flat = lambda a: a.reshape(-1, lanes)
    outs = pl.pallas_call(
        flow_kernel,
        out_shape=(v32(pairs * cells, lanes), v32(rows, pairs)),
        in_specs=[hbm] * 4,
        out_specs=[vmem] * 2,
        scratch_shapes=[
            v32(nocc * cells, lanes), v32(nvir * cells, lanes), v32(4 * cells, lanes), v32(3 * cells, lanes),
            v32(bx + 8, by + 8, norb, lanes),
            v32(bx + 8, by + 4, nocc, nvir, lanes),
            v32(4, bx + 4, by + 4, nocc, lanes),
            v32(4, bx + 4, by + 4, nvir, lanes),
        ]
        + [v32(bx, by, nocc, nvir, lanes)] * 6
        + [
            v32(4, 4, nocc, nvir, lanes),
            v32(bx + 4, by, nocc, nvir, lanes),
            v32(bx, by + 4, nocc, nvir, lanes),
            v32(bx, by, nocc, nvir, lanes),
            v32(bx, by, 8, lanes), v32(bx + 4, by, 4, lanes), v32(bx, by + 4, 4, lanes),
            v32(nocc, lanes), v32(zs, nocc, lanes), v32(nocc, lanes), v32(2, nocc, lanes), v32(2, nocc, lanes),
            v32(nocc // 2, nvir, lanes), v32(zs, nocc // 2, nvir, lanes), v32(nocc // 2, nvir, lanes),
            v32(nocc, nvir, lanes), v32(nocc, nvir, lanes),
            v32(pairs, pairs),
            v32(nx, ny, nz, rows, pairs),
            v32(nx * nz, ny, rows, pairs),
            v32(ny, rows, pairs), v32(ny, rows, pairs),
            dma(28), dma(28), dma(6), dma(6), dma(4), dma(nx * nz), dma(nx * nz), dma(ny), dma(ny),
        ],
        compiler_params=pltpu.CompilerParams(
            collective_id=0, has_side_effects=True, vmem_limit_bytes=54 * MIB
        ),
        name="flow",
    )(*(pltpu.with_memory_space_constraint(flat(a), pltpu.HBM) for a in (occupied, virtual, kernel_fields, density_grad)))
    pot, casida = pl.pallas_call(
        write_kernel,
        out_shape=(sds(pairs * cells, lanes), sds(rows, pairs)),
        in_specs=[vmem] * 2,
        out_specs=(hbm, hbm),
        scratch_shapes=[dma(9)],
        compiler_params=pltpu.CompilerParams(vmem_limit_bytes=4 * MIB),
        name="write",
    )(*outs)
    return pot.reshape(pairs, bx, by, lanes), casida


def solution(mesh):
    spec = P(None, "gx", "gy", "gz")
    return jax.shard_map(
        on_device,
        mesh=mesh,
        in_specs=(spec,) * 4,
        out_specs=(spec, P(("gx", "gy", "gz"), None)),
        check_vma=False,
    )
```

```python
import functools

import jax
import jax.numpy as jnp
from jax import lax
from jax.experimental import pallas as pl
from jax.experimental.pallas import tpu as pltpu
from jax.sharding import PartitionSpec as P

MESH = pl.DeviceIdType.MESH
F32 = jnp.float32
BF16 = jnp.bfloat16
SHIFTS = (1, -1, 2, -2)
MIB = 1024 * 1024


def difference(f):
    return 8.0 * (f(1) - f(-1)) - (f(2) - f(-2))


def lanes_of(shape):
    return lax.broadcasted_iota(jnp.int32, shape, len(shape) - 1)


def edge_terms(gap, lane):
    axis = gap.ndim - 1
    lanes = gap.shape[axis]
    at = lane & 3
    two = jnp.where(at >= 2, -pltpu.roll(gap, lanes - 2, axis), pltpu.roll(gap, 2, axis))
    one = jnp.where(at == 3, pltpu.roll(gap, lanes - 1, axis), -pltpu.roll(gap, 1, axis))
    return two + jnp.where((at == 3) | (at == 0), 8.0 * one, 0.0)


def rest(v):
    return v - v.astype(BF16).astype(F32)


def dot(a, b):
    return lax.dot_general(a, b, (((1,), (1,)), ((), ())), preferred_element_type=F32)


def flow_kernel(
    occ_in, vir_in, ker_in, grd_in,
    pot, cas,
    occ, vir, ker, grd, W, N, oS, vS, S0, S1, S2, NL, S0L, LO, f0, f1, base, C, A0, A1,
    pk, wz, pkn, px, py, E2, ez, corr, LE, LEL,
    acc, part, got, acc2, got2,
    send, recv, sendy, recvy, own, send1, recv1, send2, recv2,
):
    nx, ny, nz = (lax.axis_size(a) for a in ("gx", "gy", "gz"))
    gx, gy, gz = (lax.axis_index(a) for a in ("gx", "gy", "gz"))
    bx, by = base.shape[0], base.shape[1]
    cells = bx * by
    lanes = occ.shape[1]
    half = lanes // 2
    nocc, nvir = occ.shape[0] // cells, vir.shape[0] // cells
    pairs = nocc * nvir
    rows_out = cas.shape[0]
    n_plane = nx * nz
    me = gx * nz + gz

    def plane(d):
        t = lax.rem(me + d, n_plane)
        tx, tz = t // nz, lax.rem(t, nz)
        return tx, tz, {"gx": tx, "gy": gy, "gz": tz}

    def column(d):
        t = lax.rem(gy + d, ny)
        return t, {"gx": gx, "gy": t, "gz": gz}

    def beside(axis, side):
        v, n = {"gx": (gx, nx), "gy": (gy, ny), "gz": (gz, nz)}[axis]
        where = {"gx": gx, "gy": gy, "gz": gz}
        step = (1, n - 1)[side] if isinstance(side, int) else jnp.where(side == 0, 1, n - 1)
        where[axis] = lax.rem(v + step, n)
        return where

    taken = [
        pltpu.make_async_copy(a, b, own.at[k])
        for k, (a, b) in enumerate(((occ_in, occ), (vir_in, vir), (ker_in, ker), (grd_in, grd)))
    ]
    for c in taken:
        c.start()
    barrier = pltpu.get_barrier_semaphore()
    for d in range(1, n_plane):
        pl.semaphore_signal(barrier, inc=1, device_id=plane(d)[2], device_id_type=MESH)
    for d in range(1, ny):
        pl.semaphore_signal(barrier, inc=1, device_id=column(d)[1], device_id_type=MESH)

    E2[...] = jnp.zeros_like(E2)
    lane = lanes_of((nvir, lanes))
    at_edge = (lane < 2) | (lane >= lanes - 2)
    slot = lax.rem((lane + 2) // 4, lanes // 4)

    def own_rows(c):
        x, y = divmod(c, by)
        o = occ[pl.ds(c, nocc, stride=cells), :]
        v = vir[pl.ds(c, nvir, stride=cells), :]
        return x, y, o, v

    taken[0].wait()
    taken[1].wait()
    for c in range(cells):
        x, y, o, v = own_rows(c)
        W[x + 4, y + 4, 0:nocc] = o
        W[x + 4, y + 4, nocc:nocc + nvir] = v
    pl.semaphore_wait(barrier, n_plane - 1 + ny - 1)

    copies = []

    def put(src, dst, device):
        k = len(copies)
        c = pltpu.make_async_remote_copy(
            src_ref=src, dst_ref=dst, send_sem=send.at[k], recv_sem=recv.at[k],
            device_id=device, device_id_type=MESH,
        )
        c.start()
        copies.append(c)
        return c

    in_x, in_y = pl.ds(4, bx), pl.ds(4, by)

    def near_src(b, side):
        return pl.ds(b + 2, 2) if side == 0 else pl.ds(4, 2)

    def near_dst(b, side):
        return pl.ds(2, 2) if side == 0 else pl.ds(b + 4, 2)

    def layer_src(side, depth):
        return pl.ds(jnp.where(side == 0, by + 4 - depth, 3 + depth), 1)

    def layer_dst(side, depth):
        return pl.ds(jnp.where(side == 0, 4 - depth, by + 3 + depth), 1)

    def far_src(b, side):
        return pl.ds(b, 2) if side == 0 else pl.ds(6, 2)

    def far_dst(b, side):
        return pl.ds(0, 2) if side == 0 else pl.ds(b + 6, 2)

    def arm_src(b, side):
        return pl.ds(b, 2) if side == 0 else pl.ds(2, 2)

    def arm_dst(b, side):
        return pl.ds(0, 2) if side == 0 else pl.ds(b + 2, 2)

    zsides = range(1 if nz == 2 else 2)
    both = range(2)
    def layer_copy(s, depth):
        k = 2 * (depth - 1) + s
        return pltpu.make_async_remote_copy(
            src_ref=W.at[in_x, layer_src(s, depth)], dst_ref=W.at[in_x, layer_dst(s, depth)],
            send_sem=sendy.at[k], recv_sem=recvy.at[k],
            device_id=beside("gy", s), device_id_type=MESH,
        )

    far_round = jnp.where(gy == ny - 1, 0, 1)
    for depth in (1, 2):
        layer_copy(far_round, depth).start()
        layer_copy(1 - far_round, depth).start()
    near_y = [[layer_copy(s, depth) for s in both] for depth in (1, 2)]

    def x_copy(s):
        return pltpu.make_async_remote_copy(
            src_ref=W.at[pl.ds(jnp.where(s == 0, bx + 2, 4), 2), in_y],
            dst_ref=W.at[pl.ds(jnp.where(s == 0, 2, bx + 4), 2), in_y],
            send_sem=sendy.at[4 + s], recv_sem=recvy.at[4 + s],
            device_id=beside("gx", s), device_id_type=MESH,
        )

    near_x = [x_copy(s) for s in both]
    for c in near_x:
        c.start()
    packed = jnp.zeros((nocc, lanes), F32)
    for c in range(cells):
        x, y, o, v = own_rows(c)
        packed += pltpu.roll(jnp.where(at_edge, o, 0.0), 4 * c, 1)
        packed += pltpu.roll(jnp.where(at_edge, v, 0.0), 4 * c + half, 1)
    pk[...] = packed
    z_in = [put(pk, wz.at[s], beside("gz", s)) for s in zsides]
    taken[2].wait()
    taken[3].wait()
    for c in range(cells):
        x, y = divmod(c, by)
        g = [grd[pl.ds(k * cells + c, 1), :] for k in range(3)]
        f = [ker[pl.ds(k * cells + c, 1), :] for k in range(4)]
        k1, k2, k3 = f[1] * (1.0 / 12.0), f[2] * (1.0 / 144.0), f[3] * (1.0 / 144.0)
        C[x, y] = jnp.concatenate(g + [k1, k2, k3, f[0], f[0]], axis=0)
        for m, ref in ((0, A0.at[x + 2, y]), (1, A1.at[x, y + 2])):
            q = k2 * g[m]
            a = [q * g[k] + k3 if k == m else q * g[k] for k in range(3)]
            ref[...] = jnp.concatenate(a + [k1 * g[m]], axis=0)
    arm_x = [put(A0.at[arm_src(bx, s)], A0.at[arm_dst(bx, s)], beside("gx", s)) for s in both]
    arm_y = [
        put(A1.at[:, arm_src(by, s)], A1.at[:, arm_dst(by, s)], beside("gy", s)) for s in both
    ]

    def multiply(count, place, unroll=2):
        def body(t, carry):
            x, y = place(t)
            v = W[x, y, nocc:nocc + nvir]
            for i in range(nocc):
                N[x, y - 2, i] = W[x, y, i:i + 1] * v
            return carry

        lax.fori_loop(0, count, body, 0, unroll=unroll)

    def rim(t, b, lo, hi):
        return jnp.where(t < 2, t + lo, t + hi)

    multiply(cells, lambda t: (4 + t // by, 4 + lax.rem(t, by)))

    for c in z_in:
        c.wait_recv()
    low = (lanes_of((nocc, lanes)) & 3) < 2
    z_edges = wz[0] if nz == 2 else jnp.where(low, wz[1], wz[0])
    pkn[...] = z_edges
    turn_x = [put(pkn, px.at[s], beside("gx", s)) for s in both]
    turn_y = [put(pkn, py.at[s], beside("gy", s)) for s in both]
    far_x = [
        put(W.at[far_src(bx, s), in_y], W.at[far_dst(bx, s), in_y], beside("gx", s)) for s in both
    ]
    far_y = [
        put(W.at[in_x, far_src(by, s)], W.at[in_x, far_dst(by, s)], beside("gy", s)) for s in both
    ]

    def prepare(x, y, edges, c, fold):
        ao = pltpu.roll(edges, lax.rem(lanes - 4 * c, lanes), 1)
        av = pltpu.roll(edges, lax.rem(lanes + half - 4 * c, lanes), 1)
        o_own, v_own = W[x, y, 0:nocc], W[x, y, nocc:nocc + nvir]
        for k, s in enumerate(SHIFTS):
            m = lane < s if s > 0 else lane >= lanes + s
            scale = 8.0 if abs(s) == 1 else 1.0
            factor = scale if fold is None else scale * fold
            oS[k, x - 2, y - 2] = factor * pltpu.roll(jnp.where(m, ao, o_own), (-s) % lanes, 1)
            vS[k, x - 2, y - 2] = pltpu.roll(jnp.where(m, av, v_own), (-s) % lanes, 1)

    def prepare_center(t, carry):
        prepare(4 + t // by, 4 + lax.rem(t, by), pkn[...], t, None)
        return carry

    lax.fori_loop(0, cells, prepare_center, 0, unroll=4)

    own_o, own_v = pk[...], pltpu.roll(pk[...], half, 1)
    nb_o, nb_v = z_edges, pltpu.roll(z_edges, half, 1)
    for i in range(nocc):
        gap = nb_o[i:i + 1] * nb_v - own_o[i:i + 1] * own_v
        e = jnp.where(slot < cells, edge_terms(gap, lane), 0.0)
        LE[i] = e
        LEL[i] = rest(e)

    def slope_z(x, y, i, shifted):
        p = [oS[k, x + 2, y + 2, i:i + 1] * shifted[k] for k in range(4)]
        return (p[0] - p[1]) - (p[2] - p[3])

    def n_at(x, y, i):
        return N[x + 4, y + 2, i]

    def own_pass(x, carry):
        for y in range(by):
            shifted = [vS[k, x + 2, y + 2] for k in range(4)]
            for i in range(nocc):
                NL[x, y, i] = rest(n_at(x, y, i))
                S2[x, y, i] = slope_z(x, y, i, shifted)
        return carry

    lax.fori_loop(0, bx, own_pass, 0)

    def x_pass(x, carry):
        for y in range(by):
            g0, g1, g2, k1, k2, k3, kk = (C[x, y, k:k + 1] for k in range(7))
            for i in range(nocc):
                n = n_at(x, y, i)
                s0 = difference(lambda t: n_at(x + t, y, i))
                S0[x, y, i] = s0
                S0L[x, y, i] = rest(s0)
                s2 = S2[x, y, i]
                al = g0 * s0 + g2 * s2
                sc = k1 * n + k2 * al
                f0[x + 2, y, i] = sc * g0 + k3 * s0
                f1[x, y + 2, i] = sc * g1
                S2[x, y, i] = sc * g2 + k3 * s2
                base[x, y, i] = kk * n + k1 * al
        return carry

    early = 1 - lax.rem(gx, 2)
    for s in (early, 1 - early):
        x_copy(s).wait_recv()
        at = jnp.where(s == 0, 2, bx + 4)
        multiply(2 * by, lambda t: (at + t // by, 4 + lax.rem(t, by)))
        lo = jnp.where(s == 0, 0, bx - 2)
        lax.fori_loop(0, 2, lambda t, carry: x_pass(lo + t, carry), 0)

    def second_pass_cell(x, y, lo):
        w0, w1, w2, wb = (A1[x, y + 2, k:k + 1] for k in range(4))
        c = x * by + y
        for i in range(nocc):
            s1 = difference(lambda t: n_at(x, y + t, i))
            fl0 = f0[x + 2, y, i] + w0 * s1
            fl1 = f1[x, y + 2, i] + w1 * s1
            fl2 = S2[x, y, i] + w2 * s1
            turned = difference(lambda t: pltpu.roll(fl2, (-t) % lanes, 1))
            b = (base[x, y, i] + wb * s1) - turned
            S1[x, y, i] = s1
            f0[x + 2, y, i] = fl0
            f1[x, y + 2, i] = fl1
            base[x, y, i] = b
            deep = (2 * i) // nocc
            j = i % (nocc // 2)
            E2[j] = jnp.where(slot == c + cells * deep, pltpu.roll(fl2, 4 * c + half * deep, 1), E2[j])
            for k, v in enumerate((s1, b, fl0, fl1)):
                LO[lo, k, i] = rest(v)

    def wide(parts):
        return jnp.concatenate([p.reshape(pairs, lanes) for p in parts], axis=1)

    def gather(x, ys, at, start):
        (l0, l1), (y0, y1) = at, ys

        def pair(high, low):
            return wide(high), wide(low)

        def orbit(lo, y):
            left = pair([N[x + 4, y + 2], S0[x, y]], [NL[x, y], S0L[x, y]])
            return left, pair([base[x, y], f0[x + 2, y]], [LO[lo, 1], LO[lo, 2]])

        first, second = orbit(l0, y0), orbit(l1, y1)
        third = (
            pair([S1[x, y0], S1[x, y1]], [LO[l0, 0], LO[l1, 0]]),
            pair([f1[x, y0 + 2], f1[x, y1 + 2]], [LO[l0, 3], LO[l1, 3]]),
        )

        def beside_(parts):
            return jnp.concatenate(parts, axis=1)

        left = [beside_([first[0][k], second[0][k]]) for k in range(2)]
        right = [beside_([first[1][k], second[1][k]]) for k in range(2)]
        top = dot(jnp.concatenate(left, axis=0), right[0])
        low_part = dot(
            beside_([left[0], third[0][0], third[0][0], third[0][1]]),
            beside_([right[1], third[1][0], third[1][1], third[1][0]]),
        )
        total = (top[0:pairs] + top[pairs:]) + low_part
        acc[...] = total if start else acc[...] + total

    def second_pass(ys, start, late):
        for x in range(bx):
            at = [2 * (x % 2), 2 * (x % 2) + 1]
            if late is not None:
                gather(*late)
            for lo, y in zip(at, ys):
                second_pass_cell(x, y, lo)
            late = (x, ys, at, start and x == 0)
        return late

    def across(depth):
        y = (4 - depth, by + 3 + depth)
        return lambda t: (4 + t // 2, jnp.where(lax.rem(t, 2) == 0, y[0], y[1]))

    def turn_corner(depth):
        return [
            put(
                W.at[near_src(bx, sx), layer_dst(sy, depth)],
                W.at[near_dst(bx, sx), layer_dst(sy, depth)],
                beside("gx", sx),
            )
            for sy in both
            for sx in both
        ]

    for c in near_y[0]:
        c.wait_recv()
    corner = turn_corner(1)
    multiply(2 * bx, across(1))
    late = second_pass((1, 2), True, None)
    for c in near_y[1]:
        c.wait_recv()
    corner += turn_corner(2)
    multiply(2 * bx, across(2))
    late = second_pass((0, 3), False, late)
    gather(*late)
    ends = [E2[i % (nocc // 2)] for i in range(nocc)]
    ends = [e if 2 * i < nocc else pltpu.roll(e, half, 1) for i, e in enumerate(ends)]
    right = jnp.concatenate(ends, axis=0)
    left, left_lo = LE[...].reshape(pairs, lanes), LEL[...].reshape(pairs, lanes)
    total = acc[...] + (dot(left, right) + dot(left_lo, right) + dot(left, rest(right)))
    for tx in range(nx):
        for ty in range(ny):
            for tz in range(nz):
                r = ((tx * ny + ty) * nz + tz) * rows_out
                part[tx, ty, tz] = total[r:r + rows_out]
    first = []
    for d in sorted(range(1, n_plane), key=lambda d: abs(2 * d - n_plane)):
        tx, tz, target = plane(d)
        c = pltpu.make_async_remote_copy(
            src_ref=part.at[tx, :, tz], dst_ref=got.at[d],
            send_sem=send1.at[d], recv_sem=recv1.at[d],
            device_id=target, device_id_type=MESH,
        )
        c.start()
        first.append(c)
    z_out = [put(E2, ez.at[s], beside("gz", s)) for s in zsides]

    for c in turn_x + arm_x:
        c.wait_recv()

    def prepare_x(t, carry):
        k, y = t // by, lax.rem(t, by)
        side = k // 2
        c = jnp.where(k < 2, k + bx - 2, k - 2) * by + y
        a = rim(k, bx, 0, bx)
        prepare(a + 2, 4 + y, px[side], c, A0[a, y, 2:3])
        return carry

    lax.fori_loop(0, 4 * by, prepare_x, 0, unroll=4)

    for c in far_x + corner:
        c.wait_recv()
    multiply(4 * by, lambda t: (rim(t // by, bx, 0, bx + 4), 4 + lax.rem(t, by)))
    multiply(16, lambda t: (rim(t // 4, bx, 2, bx + 2), rim(lax.rem(t, 4), by, 2, by + 2)))

    def at_x(t, carry):
        a, y = rim(t // by, bx, 0, bx), lax.rem(t, by)
        x = a - 2
        shifted = [vS[k, a, y + 2] for k in range(4)]
        c0, c1, c3 = A0[a, y, 0:1], A0[a, y, 1:2], A0[a, y, 3:4]
        for i in range(nocc):
            s0 = difference(lambda t: n_at(x + t, y, i))
            s1 = difference(lambda t: n_at(x, y + t, i))
            f0[a, y, i] = (c0 * s0 + c1 * s1) + (slope_z(x, y, i, shifted) + c3 * n_at(x, y, i))
        return carry

    lax.fori_loop(0, 4 * by, at_x, 0)

    for c in turn_y + arm_y:
        c.wait_recv()

    def prepare_y(t, carry):
        x, k = t // 4, lax.rem(t, 4)
        side = k // 2
        c = x * by + jnp.where(k < 2, k + by - 2, k - 2)
        b = rim(k, by, 0, by)
        prepare(4 + x, b + 2, py[side], c, A1[x, b, 2:3])
        return carry

    lax.fori_loop(0, 4 * bx, prepare_y, 0, unroll=4)

    def at_y(x, carry):
        for y in (-2, -1, by, by + 1):
            b = y + 2
            shifted = [vS[k, x + 2, b] for k in range(4)]
            c0, c1, c3 = A1[x, b, 0:1], A1[x, b, 1:2], A1[x, b, 3:4]
            for i in range(nocc):
                s0 = difference(lambda t: n_at(x + t, y, i))
                n = lambda t: n_at(x, y + t, i)
                if y == -2:
                    s1 = 8.0 * n(1) - n(2)
                elif y == -1:
                    s1 = 8.0 * (n(1) - n(-1)) - n(2)
                elif y == by:
                    s1 = 8.0 * (n(1) - n(-1)) + n(-2)
                else:
                    s1 = n(-2) - 8.0 * n(-1)
                f1[x, b, i] = (c0 * s0 + c1 * s1) + (slope_z(x, y, i, shifted) + c3 * n(0))
        return carry

    lax.fori_loop(0, bx, at_y, 0)

    for c in first:
        c.wait_recv()
    mine = part[gx, :, gz]
    for d in range(1, n_plane):
        mine = mine + got[d]
    acc2[...] = mine
    second = []
    for d in range(1, ny):
        t, target = column(d)
        c = pltpu.make_async_remote_copy(
            src_ref=acc2.at[t], dst_ref=got2.at[d],
            send_sem=send2.at[d], recv_sem=recv2.at[d],
            device_id=target, device_id_type=MESH,
        )
        c.start()
        second.append(c)

    for c in z_out:
        c.wait_recv()
    for j in range(nocc // 2):
        outer = ez[0, j] if nz == 2 else jnp.where((lane & 3) < 2, ez[1, j], ez[0, j])
        corr[j] = edge_terms(outer - E2[j], lane)
    for c in far_y:
        c.wait_recv()

    def assemble(x, carry):
        def far(y):
            return W[x + 4, y + 4, nocc:nocc + nvir]

        def slope_of(y):
            return A1[x, y + 2, 1:2]

        low1 = slope_of(-1) * far(-3)
        low2 = (slope_of(-2) * far(-4), -8.0 * slope_of(-2) * far(-3))
        top1 = -1.0 * slope_of(by) * far(by + 2)
        top2 = (8.0 * slope_of(by + 1) * far(by + 2), -1.0 * slope_of(by + 1) * far(by + 3))
        for i in range(nocc):
            o = [W[x + 4, y + 4, i:i + 1] for y in (-4, -3, by + 2, by + 3)]
            a = [f1[x, b, i] for b in range(by + 4)]
            a[0] = a[0] + (o[0] * low2[0] + o[1] * low2[1])
            a[1] = a[1] + o[1] * low1
            a[by + 2] = a[by + 2] + o[2] * top1
            a[by + 3] = a[by + 3] + (o[2] * top2[0] + o[3] * top2[1])
            deep = (2 * i) // nocc
            e = corr[i % (nocc // 2)]
            for y in range(by):
                c = x * by + y
                b = [f0[x + k, y, i] for k in (0, 1, 3, 4)]
                inner = (b[2] - b[1]) + (a[y + 3] - a[y + 1])
                outer = (b[3] - b[0]) + (a[y + 4] - a[y])
                turned = pltpu.roll(e, lax.rem(2 * lanes - 4 * c - half * deep, lanes), 1)
                v = base[x, y, i] - (8.0 * inner - outer)
                v = v - jnp.where(at_edge, turned, 0.0)
                pot[pl.ds(i * nvir * cells + c, nvir, stride=cells), :] = v
        return carry

    lax.fori_loop(0, bx, assemble, 0)
    for c in copies + near_y[0] + near_y[1] + near_x + first + second:
        c.wait_send()
    mine = acc2[gy]
    for d, c in enumerate(second):
        c.wait_recv()
        mine = mine + got2[d + 1]
    cas[...] = mine * (1.0 / (cells * lanes * nx * ny * nz))


def write_kernel(pot_in, cas_in, pot, cas, sem):
    parts = sem.shape[0] - 1
    rows = pot_in.shape[0] // parts
    out = [pltpu.make_async_copy(cas_in, cas, sem.at[parts])]
    for k in range(parts):
        block = pl.ds(k * rows, rows)
        out.append(pltpu.make_async_copy(pot_in.at[block], pot.at[block], sem.at[k]))
    for c in out:
        c.start()
    for c in out:
        c.wait()


def on_device(occupied, virtual, kernel_fields, density_grad):
    nocc, bx, by, lanes = occupied.shape
    nvir = virtual.shape[0]
    nx, ny, nz = (lax.axis_size(a) for a in ("gx", "gy", "gz"))
    devices = nx * ny * nz
    cells = bx * by
    pairs = nocc * nvir
    norb = nocc + nvir
    rows = pairs // devices
    sds = lambda *s: jax.ShapeDtypeStruct(s, F32)
    v32 = lambda *s: pltpu.VMEM(s, F32)
    dma = lambda n: pltpu.SemaphoreType.DMA((n,))
    vmem = pl.BlockSpec(memory_space=pltpu.VMEM)
    hbm = pl.BlockSpec(memory_space=pltpu.HBM)
    zs = 1 if nz == 2 else 2
    flat = lambda a: a.reshape(-1, lanes)
    outs = pl.pallas_call(
        flow_kernel,
        out_shape=(v32(pairs * cells, lanes), v32(rows, pairs)),
        in_specs=[hbm] * 4,
        out_specs=[vmem] * 2,
        scratch_shapes=[
            v32(nocc * cells, lanes), v32(nvir * cells, lanes), v32(4 * cells, lanes), v32(3 * cells, lanes),
            v32(bx + 8, by + 8, norb, lanes),
            v32(bx + 8, by + 4, nocc, nvir, lanes),
            v32(4, bx + 4, by + 4, nocc, lanes),
            v32(4, bx + 4, by + 4, nvir, lanes),
        ]
        + [v32(bx, by, nocc, nvir, lanes)] * 5
        + [
            v32(4, 4, nocc, nvir, lanes),
            v32(bx + 4, by, nocc, nvir, lanes),
            v32(bx, by + 4, nocc, nvir, lanes),
            v32(bx, by, nocc, nvir, lanes),
            v32(bx, by, 8, lanes), v32(bx + 4, by, 4, lanes), v32(bx, by + 4, 4, lanes),
            v32(nocc, lanes), v32(zs, nocc, lanes), v32(nocc, lanes), v32(2, nocc, lanes), v32(2, nocc, lanes),
            v32(nocc // 2, nvir, lanes), v32(zs, nocc // 2, nvir, lanes), v32(nocc // 2, nvir, lanes),
            v32(nocc, nvir, lanes), v32(nocc, nvir, lanes),
            v32(pairs, pairs),
            v32(nx, ny, nz, rows, pairs),
            v32(nx * nz, ny, rows, pairs),
            v32(ny, rows, pairs), v32(ny, rows, pairs),
            dma(28), dma(28), dma(6), dma(6), dma(4), dma(nx * nz), dma(nx * nz), dma(ny), dma(ny),
        ],
        compiler_params=pltpu.CompilerParams(
            collective_id=0, has_side_effects=True, vmem_limit_bytes=54 * MIB
        ),
        name="flow",
    )(*(pltpu.with_memory_space_constraint(flat(a), pltpu.HBM) for a in (occupied, virtual, kernel_fields, density_grad)))
    pot, casida = pl.pallas_call(
        write_kernel,
        out_shape=(sds(pairs * cells, lanes), sds(rows, pairs)),
        in_specs=[vmem] * 2,
        out_specs=(hbm, hbm),
        scratch_shapes=[dma(9)],
        compiler_params=pltpu.CompilerParams(vmem_limit_bytes=4 * MIB),
        name="write",
    )(*outs)
    return pot.reshape(pairs, bx, by, lanes), casida


def solution(mesh):
    spec = P(None, "gx", "gy", "gz")
    return jax.shard_map(
        on_device,
        mesh=mesh,
        in_specs=(spec,) * 4,
        out_specs=(spec, P(("gx", "gy", "gz"), None)),
        check_vma=False,
    )
```

```python
import functools

import jax
import jax.numpy as jnp
from jax import lax
from jax.experimental import pallas as pl
from jax.experimental.pallas import tpu as pltpu
from jax.sharding import PartitionSpec as P

MESH = pl.DeviceIdType.MESH
F32 = jnp.float32
BF16 = jnp.bfloat16
SHIFTS = (1, -1, 2, -2)
MIB = 1024 * 1024


def difference(f):
    return 8.0 * (f(1) - f(-1)) - (f(2) - f(-2))


def lanes_of(shape):
    return lax.broadcasted_iota(jnp.int32, shape, len(shape) - 1)


def edge_terms(gap, lane):
    axis = gap.ndim - 1
    lanes = gap.shape[axis]
    at = lane & 3
    two = jnp.where(at >= 2, -pltpu.roll(gap, lanes - 2, axis), pltpu.roll(gap, 2, axis))
    one = jnp.where(at == 3, pltpu.roll(gap, lanes - 1, axis), -pltpu.roll(gap, 1, axis))
    return two + jnp.where((at == 3) | (at == 0), 8.0 * one, 0.0)


def rest(v):
    return v - v.astype(BF16).astype(F32)


def dot(a, b):
    return lax.dot_general(a, b, (((1,), (1,)), ((), ())), preferred_element_type=F32)


def flow_kernel(
    occ_in, vir_in, ker_in, grd_in,
    pot, cas,
    occ, vir, ker, grd, W, N, oS, vS, S0, S1, S2, NL, S0L, LO, f0, f1, base, C, A0, A1,
    pk, wz, pkn, px, py, E2, ez, corr, LE, LEL,
    acc, part, got, acc2, got2,
    send, recv, sendy, recvy, own, send1, recv1, send2, recv2,
):
    nx, ny, nz = (lax.axis_size(a) for a in ("gx", "gy", "gz"))
    gx, gy, gz = (lax.axis_index(a) for a in ("gx", "gy", "gz"))
    bx, by = base.shape[0], base.shape[1]
    cells = bx * by
    lanes = occ.shape[1]
    half = lanes // 2
    nocc, nvir = occ.shape[0] // cells, vir.shape[0] // cells
    pairs = nocc * nvir
    rows_out = cas.shape[0]
    n_plane = nx * nz
    me = gx * nz + gz

    def plane(d):
        t = lax.rem(me + d, n_plane)
        tx, tz = t // nz, lax.rem(t, nz)
        return tx, tz, {"gx": tx, "gy": gy, "gz": tz}

    def column(d):
        t = lax.rem(gy + d, ny)
        return t, {"gx": gx, "gy": t, "gz": gz}

    def beside(axis, side):
        v, n = {"gx": (gx, nx), "gy": (gy, ny), "gz": (gz, nz)}[axis]
        where = {"gx": gx, "gy": gy, "gz": gz}
        step = (1, n - 1)[side] if isinstance(side, int) else jnp.where(side == 0, 1, n - 1)
        where[axis] = lax.rem(v + step, n)
        return where

    taken = [
        pltpu.make_async_copy(a, b, own.at[k])
        for k, (a, b) in enumerate(((occ_in, occ), (vir_in, vir), (ker_in, ker), (grd_in, grd)))
    ]
    for c in taken:
        c.start()
    barrier = pltpu.get_barrier_semaphore()
    for d in range(1, n_plane):
        pl.semaphore_signal(barrier, inc=1, device_id=plane(d)[2], device_id_type=MESH)
    for d in range(1, ny):
        pl.semaphore_signal(barrier, inc=1, device_id=column(d)[1], device_id_type=MESH)

    E2[...] = jnp.zeros_like(E2)
    lane = lanes_of((nvir, lanes))
    at_edge = (lane < 2) | (lane >= lanes - 2)
    slot = lax.rem((lane + 2) // 4, lanes // 4)

    def own_rows(c):
        x, y = divmod(c, by)
        o = occ[pl.ds(c, nocc, stride=cells), :]
        v = vir[pl.ds(c, nvir, stride=cells), :]
        return x, y, o, v

    taken[0].wait()
    taken[1].wait()
    for c in range(cells):
        x, y, o, v = own_rows(c)
        W[x + 4, y + 4, 0:nocc] = o
        W[x + 4, y + 4, nocc:nocc + nvir] = v
    pl.semaphore_wait(barrier, n_plane - 1 + ny - 1)

    copies = []

    def put(src, dst, device):
        k = len(copies)
        c = pltpu.make_async_remote_copy(
            src_ref=src, dst_ref=dst, send_sem=send.at[k], recv_sem=recv.at[k],
            device_id=device, device_id_type=MESH,
        )
        c.start()
        copies.append(c)
        return c

    in_x, in_y = pl.ds(4, bx), pl.ds(4, by)

    def near_src(b, side):
        return pl.ds(b + 2, 2) if side == 0 else pl.ds(4, 2)

    def near_dst(b, side):
        return pl.ds(2, 2) if side == 0 else pl.ds(b + 4, 2)

    def layer_src(side, depth):
        return pl.ds(jnp.where(side == 0, by + 4 - depth, 3 + depth), 1)

    def layer_dst(side, depth):
        return pl.ds(jnp.where(side == 0, 4 - depth, by + 3 + depth), 1)

    def far_src(b, side):
        return pl.ds(b, 2) if side == 0 else pl.ds(6, 2)

    def far_dst(b, side):
        return pl.ds(0, 2) if side == 0 else pl.ds(b + 6, 2)

    def arm_src(b, side):
        return pl.ds(b, 2) if side == 0 else pl.ds(2, 2)

    def arm_dst(b, side):
        return pl.ds(0, 2) if side == 0 else pl.ds(b + 2, 2)

    zsides = range(1 if nz == 2 else 2)
    both = range(2)
    def layer_copy(s, depth):
        k = 2 * (depth - 1) + s
        return pltpu.make_async_remote_copy(
            src_ref=W.at[in_x, layer_src(s, depth)], dst_ref=W.at[in_x, layer_dst(s, depth)],
            send_sem=sendy.at[k], recv_sem=recvy.at[k],
            device_id=beside("gy", s), device_id_type=MESH,
        )

    far_round = jnp.where(gy == ny - 1, 0, 1)
    for depth in (1, 2):
        layer_copy(far_round, depth).start()
        layer_copy(1 - far_round, depth).start()
    near_y = [[layer_copy(s, depth) for s in both] for depth in (1, 2)]

    def x_copy(s):
        return pltpu.make_async_remote_copy(
            src_ref=W.at[pl.ds(jnp.where(s == 0, bx + 2, 4), 2), in_y],
            dst_ref=W.at[pl.ds(jnp.where(s == 0, 2, bx + 4), 2), in_y],
            send_sem=sendy.at[4 + s], recv_sem=recvy.at[4 + s],
            device_id=beside("gx", s), device_id_type=MESH,
        )

    near_x = [x_copy(s) for s in both]
    for c in near_x:
        c.start()
    packed = jnp.zeros((nocc, lanes), F32)
    for c in range(cells):
        x, y, o, v = own_rows(c)
        packed += pltpu.roll(jnp.where(at_edge, o, 0.0), 4 * c, 1)
        packed += pltpu.roll(jnp.where(at_edge, v, 0.0), 4 * c + half, 1)
    pk[...] = packed
    z_in = [put(pk, wz.at[s], beside("gz", s)) for s in zsides]
    taken[2].wait()
    taken[3].wait()
    for c in range(cells):
        x, y = divmod(c, by)
        g = [grd[pl.ds(k * cells + c, 1), :] for k in range(3)]
        f = [ker[pl.ds(k * cells + c, 1), :] for k in range(4)]
        k1, k2, k3 = f[1] * (1.0 / 12.0), f[2] * (1.0 / 144.0), f[3] * (1.0 / 144.0)
        C[x, y] = jnp.concatenate(g + [k1, k2, k3, f[0], f[0]], axis=0)
        for m, ref in ((0, A0.at[x + 2, y]), (1, A1.at[x, y + 2])):
            q = k2 * g[m]
            a = [q * g[k] + k3 if k == m else q * g[k] for k in range(3)]
            ref[...] = jnp.concatenate(a + [k1 * g[m]], axis=0)
    arm_x = [put(A0.at[arm_src(bx, s)], A0.at[arm_dst(bx, s)], beside("gx", s)) for s in both]
    arm_y = [
        put(A1.at[:, arm_src(by, s)], A1.at[:, arm_dst(by, s)], beside("gy", s)) for s in both
    ]

    def multiply(count, place, unroll=2):
        def body(t, carry):
            x, y = place(t)
            v = W[x, y, nocc:nocc + nvir]
            for i in range(nocc):
                N[x, y - 2, i] = W[x, y, i:i + 1] * v
            return carry

        lax.fori_loop(0, count, body, 0, unroll=unroll)

    def rim(t, b, lo, hi):
        return jnp.where(t < 2, t + lo, t + hi)

    multiply(cells, lambda t: (4 + t // by, 4 + lax.rem(t, by)))

    def low_pass(x, carry):
        for y in range(by):
            for i in range(nocc):
                NL[x, y, i] = rest(N[x + 4, y + 2, i])
        return carry

    lax.fori_loop(0, bx, low_pass, 0)
    for c in z_in:
        c.wait_recv()
    low = (lanes_of((nocc, lanes)) & 3) < 2
    z_edges = wz[0] if nz == 2 else jnp.where(low, wz[1], wz[0])
    pkn[...] = z_edges
    turn_x = [put(pkn, px.at[s], beside("gx", s)) for s in both]
    turn_y = [put(pkn, py.at[s], beside("gy", s)) for s in both]
    far_x = [
        put(W.at[far_src(bx, s), in_y], W.at[far_dst(bx, s), in_y], beside("gx", s)) for s in both
    ]
    far_y = [
        put(W.at[in_x, far_src(by, s)], W.at[in_x, far_dst(by, s)], beside("gy", s)) for s in both
    ]

    def prepare(x, y, edges, c, fold):
        ao = pltpu.roll(edges, lax.rem(lanes - 4 * c, lanes), 1)
        av = pltpu.roll(edges, lax.rem(lanes + half - 4 * c, lanes), 1)
        o_own, v_own = W[x, y, 0:nocc], W[x, y, nocc:nocc + nvir]
        for k, s in enumerate(SHIFTS):
            m = lane < s if s > 0 else lane >= lanes + s
            scale = 8.0 if abs(s) == 1 else 1.0
            factor = scale if fold is None else scale * fold
            oS[k, x - 2, y - 2] = factor * pltpu.roll(jnp.where(m, ao, o_own), (-s) % lanes, 1)
            vS[k, x - 2, y - 2] = pltpu.roll(jnp.where(m, av, v_own), (-s) % lanes, 1)

    def prepare_center(t, carry):
        prepare(4 + t // by, 4 + lax.rem(t, by), pkn[...], t, None)
        return carry

    lax.fori_loop(0, cells, prepare_center, 0, unroll=4)

    own_o, own_v = pk[...], pltpu.roll(pk[...], half, 1)
    nb_o, nb_v = z_edges, pltpu.roll(z_edges, half, 1)
    for i in range(nocc):
        gap = nb_o[i:i + 1] * nb_v - own_o[i:i + 1] * own_v
        e = jnp.where(slot < cells, edge_terms(gap, lane), 0.0)
        LE[i] = e
        LEL[i] = rest(e)

    def slope_z(x, y, i, shifted):
        p = [oS[k, x + 2, y + 2, i:i + 1] * shifted[k] for k in range(4)]
        return (p[0] - p[1]) - (p[2] - p[3])

    def n_at(x, y, i):
        return N[x + 4, y + 2, i]

    def own_pass(x, carry):
        for y in range(by):
            shifted = [vS[k, x + 2, y + 2] for k in range(4)]
            for i in range(nocc):
                S2[x, y, i] = slope_z(x, y, i, shifted)
        return carry

    lax.fori_loop(0, bx, own_pass, 0)

    def x_pass(x, carry):
        for y in range(by):
            g0, g1, g2, k1, k2, k3, kk = (C[x, y, k:k + 1] for k in range(7))
            for i in range(nocc):
                n = n_at(x, y, i)
                s0 = difference(lambda t: n_at(x + t, y, i))
                S0[x, y, i] = s0
                S0L[x, y, i] = rest(s0)
                s2 = S2[x, y, i]
                al = g0 * s0 + g2 * s2
                sc = k1 * n + k2 * al
                f0[x + 2, y, i] = sc * g0 + k3 * s0
                f1[x, y + 2, i] = sc * g1
                S2[x, y, i] = sc * g2 + k3 * s2
                base[x, y, i] = kk * n + k1 * al
        return carry

    early = 1 - lax.rem(gx, 2)
    for s in (early, 1 - early):
        x_copy(s).wait_recv()
        at = jnp.where(s == 0, 2, bx + 4)
        multiply(2 * by, lambda t: (at + t // by, 4 + lax.rem(t, by)))
        lo = jnp.where(s == 0, 0, bx - 2)
        lax.fori_loop(0, 2, lambda t, carry: x_pass(lo + t, carry), 0)

    def second_pass_cell(x, y, lo):
        w0, w1, w2, wb = (A1[x, y + 2, k:k + 1] for k in range(4))
        c = x * by + y
        for i in range(nocc):
            s1 = difference(lambda t: n_at(x, y + t, i))
            fl0 = f0[x + 2, y, i] + w0 * s1
            fl1 = f1[x, y + 2, i] + w1 * s1
            fl2 = S2[x, y, i] + w2 * s1
            turned = difference(lambda t: pltpu.roll(fl2, (-t) % lanes, 1))
            b = (base[x, y, i] + wb * s1) - turned
            S1[x, y, i] = s1
            f0[x + 2, y, i] = fl0
            f1[x, y + 2, i] = fl1
            base[x, y, i] = b
            deep = (2 * i) // nocc
            j = i % (nocc // 2)
            E2[j] = jnp.where(slot == c + cells * deep, pltpu.roll(fl2, 4 * c + half * deep, 1), E2[j])
            for k, v in enumerate((s1, b, fl0, fl1)):
                LO[lo, k, i] = rest(v)

    def wide(parts):
        return jnp.concatenate([p.reshape(pairs, lanes) for p in parts], axis=1)

    def gather(x, ys, at, start):
        (l0, l1), (y0, y1) = at, ys

        def pair(high, low):
            return wide(high), wide(low)

        def orbit(lo, y):
            left = pair([N[x + 4, y + 2], S0[x, y]], [NL[x, y], S0L[x, y]])
            return left, pair([base[x, y], f0[x + 2, y]], [LO[lo, 1], LO[lo, 2]])

        first, second = orbit(l0, y0), orbit(l1, y1)
        third = (
            pair([S1[x, y0], S1[x, y1]], [LO[l0, 0], LO[l1, 0]]),
            pair([f1[x, y0 + 2], f1[x, y1 + 2]], [LO[l0, 3], LO[l1, 3]]),
        )

        def beside_(parts):
            return jnp.concatenate(parts, axis=1)

        left = [beside_([first[0][k], second[0][k]]) for k in range(2)]
        right = [beside_([first[1][k], second[1][k]]) for k in range(2)]
        top = dot(jnp.concatenate(left, axis=0), right[0])
        low_part = dot(
            beside_([left[0], third[0][0], third[0][0], third[0][1]]),
            beside_([right[1], third[1][0], third[1][1], third[1][0]]),
        )
        total = (top[0:pairs] + top[pairs:]) + low_part
        acc[...] = total if start else acc[...] + total

    def second_pass(ys, start, late):
        for x in range(bx):
            at = [2 * (x % 2), 2 * (x % 2) + 1]
            if late is not None:
                gather(*late)
            for lo, y in zip(at, ys):
                second_pass_cell(x, y, lo)
            late = (x, ys, at, start and x == 0)
        return late

    def across(depth):
        y = (4 - depth, by + 3 + depth)
        return lambda t: (4 + t // 2, jnp.where(lax.rem(t, 2) == 0, y[0], y[1]))

    def turn_corner(depth):
        return [
            put(
                W.at[near_src(bx, sx), layer_dst(sy, depth)],
                W.at[near_dst(bx, sx), layer_dst(sy, depth)],
                beside("gx", sx),
            )
            for sy in both
            for sx in both
        ]

    for c in near_y[0]:
        c.wait_recv()
    corner = turn_corner(1)
    multiply(2 * bx, across(1))
    late = second_pass((1, 2), True, None)
    for c in near_y[1]:
        c.wait_recv()
    corner += turn_corner(2)
    multiply(2 * bx, across(2))
    late = second_pass((0, 3), False, late)
    gather(*late)
    ends = [E2[i % (nocc // 2)] for i in range(nocc)]
    ends = [e if 2 * i < nocc else pltpu.roll(e, half, 1) for i, e in enumerate(ends)]
    right = jnp.concatenate(ends, axis=0)
    left, left_lo = LE[...].reshape(pairs, lanes), LEL[...].reshape(pairs, lanes)
    total = acc[...] + (dot(left, right) + dot(left_lo, right) + dot(left, rest(right)))
    for tx in range(nx):
        for ty in range(ny):
            for tz in range(nz):
                r = ((tx * ny + ty) * nz + tz) * rows_out
                part[tx, ty, tz] = total[r:r + rows_out]
    first = []
    for d in sorted(range(1, n_plane), key=lambda d: abs(2 * d - n_plane)):
        tx, tz, target = plane(d)
        c = pltpu.make_async_remote_copy(
            src_ref=part.at[tx, :, tz], dst_ref=got.at[d],
            send_sem=send1.at[d], recv_sem=recv1.at[d],
            device_id=target, device_id_type=MESH,
        )
        c.start()
        first.append(c)
    z_out = [put(E2, ez.at[s], beside("gz", s)) for s in zsides]

    for c in turn_x + arm_x:
        c.wait_recv()

    def prepare_x(t, carry):
        k, y = t // by, lax.rem(t, by)
        side = k // 2
        c = jnp.where(k < 2, k + bx - 2, k - 2) * by + y
        a = rim(k, bx, 0, bx)
        prepare(a + 2, 4 + y, px[side], c, A0[a, y, 2:3])
        return carry

    lax.fori_loop(0, 4 * by, prepare_x, 0, unroll=4)

    for c in far_x + corner:
        c.wait_recv()
    multiply(4 * by, lambda t: (rim(t // by, bx, 0, bx + 4), 4 + lax.rem(t, by)))
    multiply(16, lambda t: (rim(t // 4, bx, 2, bx + 2), rim(lax.rem(t, 4), by, 2, by + 2)))

    def at_x(t, carry):
        a, y = rim(t // by, bx, 0, bx), lax.rem(t, by)
        x = a - 2
        shifted = [vS[k, a, y + 2] for k in range(4)]
        c0, c1, c3 = A0[a, y, 0:1], A0[a, y, 1:2], A0[a, y, 3:4]
        for i in range(nocc):
            s0 = difference(lambda t: n_at(x + t, y, i))
            s1 = difference(lambda t: n_at(x, y + t, i))
            f0[a, y, i] = (c0 * s0 + c1 * s1) + (slope_z(x, y, i, shifted) + c3 * n_at(x, y, i))
        return carry

    lax.fori_loop(0, 4 * by, at_x, 0)

    for c in turn_y + arm_y:
        c.wait_recv()

    def prepare_y(t, carry):
        x, k = t // 4, lax.rem(t, 4)
        side = k // 2
        c = x * by + jnp.where(k < 2, k + by - 2, k - 2)
        b = rim(k, by, 0, by)
        prepare(4 + x, b + 2, py[side], c, A1[x, b, 2:3])
        return carry

    lax.fori_loop(0, 4 * bx, prepare_y, 0, unroll=4)

    def at_y(x, carry):
        for y in (-2, -1, by, by + 1):
            b = y + 2
            shifted = [vS[k, x + 2, b] for k in range(4)]
            c0, c1, c3 = A1[x, b, 0:1], A1[x, b, 1:2], A1[x, b, 3:4]
            for i in range(nocc):
                s0 = difference(lambda t: n_at(x + t, y, i))
                n = lambda t: n_at(x, y + t, i)
                if y == -2:
                    s1 = 8.0 * n(1) - n(2)
                elif y == -1:
                    s1 = 8.0 * (n(1) - n(-1)) - n(2)
                elif y == by:
                    s1 = 8.0 * (n(1) - n(-1)) + n(-2)
                else:
                    s1 = n(-2) - 8.0 * n(-1)
                f1[x, b, i] = (c0 * s0 + c1 * s1) + (slope_z(x, y, i, shifted) + c3 * n(0))
        return carry

    lax.fori_loop(0, bx - 1, at_y, 0)

    for c in first:
        c.wait_recv()
    mine = part[gx, :, gz]
    for d in range(1, n_plane):
        mine = mine + got[d]
    acc2[...] = mine
    second = []
    for d in range(1, ny):
        t, target = column(d)
        c = pltpu.make_async_remote_copy(
            src_ref=acc2.at[t], dst_ref=got2.at[d],
            send_sem=send2.at[d], recv_sem=recv2.at[d],
            device_id=target, device_id_type=MESH,
        )
        c.start()
        second.append(c)

    lax.fori_loop(bx - 1, bx, at_y, 0)
    for c in z_out:
        c.wait_recv()
    for j in range(nocc // 2):
        outer = ez[0, j] if nz == 2 else jnp.where((lane & 3) < 2, ez[1, j], ez[0, j])
        corr[j] = edge_terms(outer - E2[j], lane)
    for c in far_y:
        c.wait_recv()

    def assemble(x, carry):
        def far(y):
            return W[x + 4, y + 4, nocc:nocc + nvir]

        def slope_of(y):
            return A1[x, y + 2, 1:2]

        low1 = slope_of(-1) * far(-3)
        low2 = (slope_of(-2) * far(-4), -8.0 * slope_of(-2) * far(-3))
        top1 = -1.0 * slope_of(by) * far(by + 2)
        top2 = (8.0 * slope_of(by + 1) * far(by + 2), -1.0 * slope_of(by + 1) * far(by + 3))
        for i in range(nocc):
            o = [W[x + 4, y + 4, i:i + 1] for y in (-4, -3, by + 2, by + 3)]
            a = [f1[x, b, i] for b in range(by + 4)]
            a[0] = a[0] + (o[0] * low2[0] + o[1] * low2[1])
            a[1] = a[1] + o[1] * low1
            a[by + 2] = a[by + 2] + o[2] * top1
            a[by + 3] = a[by + 3] + (o[2] * top2[0] + o[3] * top2[1])
            deep = (2 * i) // nocc
            e = corr[i % (nocc // 2)]
            for y in range(by):
                c = x * by + y
                b = [f0[x + k, y, i] for k in (0, 1, 3, 4)]
                inner = (b[2] - b[1]) + (a[y + 3] - a[y + 1])
                outer = (b[3] - b[0]) + (a[y + 4] - a[y])
                turned = pltpu.roll(e, lax.rem(2 * lanes - 4 * c - half * deep, lanes), 1)
                v = base[x, y, i] - (8.0 * inner - outer)
                v = v - jnp.where(at_edge, turned, 0.0)
                pot[pl.ds(i * nvir * cells + c, nvir, stride=cells), :] = v
        return carry

    lax.fori_loop(0, bx, assemble, 0)
    for c in copies + near_y[0] + near_y[1] + near_x + first + second:
        c.wait_send()
    mine = acc2[gy]
    for d, c in enumerate(second):
        c.wait_recv()
        mine = mine + got2[d + 1]
    cas[...] = mine * (1.0 / (cells * lanes * nx * ny * nz))


def write_kernel(pot_in, cas_in, pot, cas, sem):
    parts = sem.shape[0] - 1
    rows = pot_in.shape[0] // parts
    out = [pltpu.make_async_copy(cas_in, cas, sem.at[parts])]
    for k in range(parts):
        block = pl.ds(k * rows, rows)
        out.append(pltpu.make_async_copy(pot_in.at[block], pot.at[block], sem.at[k]))
    for c in out:
        c.start()
    for c in out:
        c.wait()


def on_device(occupied, virtual, kernel_fields, density_grad):
    nocc, bx, by, lanes = occupied.shape
    nvir = virtual.shape[0]
    nx, ny, nz = (lax.axis_size(a) for a in ("gx", "gy", "gz"))
    devices = nx * ny * nz
    cells = bx * by
    pairs = nocc * nvir
    norb = nocc + nvir
    rows = pairs // devices
    sds = lambda *s: jax.ShapeDtypeStruct(s, F32)
    v32 = lambda *s: pltpu.VMEM(s, F32)
    dma = lambda n: pltpu.SemaphoreType.DMA((n,))
    vmem = pl.BlockSpec(memory_space=pltpu.VMEM)
    hbm = pl.BlockSpec(memory_space=pltpu.HBM)
    zs = 1 if nz == 2 else 2
    flat = lambda a: a.reshape(-1, lanes)
    outs = pl.pallas_call(
        flow_kernel,
        out_shape=(v32(pairs * cells, lanes), v32(rows, pairs)),
        in_specs=[hbm] * 4,
        out_specs=[vmem] * 2,
        scratch_shapes=[
            v32(nocc * cells, lanes), v32(nvir * cells, lanes), v32(4 * cells, lanes), v32(3 * cells, lanes),
            v32(bx + 8, by + 8, norb, lanes),
            v32(bx + 8, by + 4, nocc, nvir, lanes),
            v32(4, bx + 4, by + 4, nocc, lanes),
            v32(4, bx + 4, by + 4, nvir, lanes),
        ]
        + [v32(bx, by, nocc, nvir, lanes)] * 5
        + [
            v32(4, 4, nocc, nvir, lanes),
            v32(bx + 4, by, nocc, nvir, lanes),
            v32(bx, by + 4, nocc, nvir, lanes),
            v32(bx, by, nocc, nvir, lanes),
            v32(bx, by, 8, lanes), v32(bx + 4, by, 4, lanes), v32(bx, by + 4, 4, lanes),
            v32(nocc, lanes), v32(zs, nocc, lanes), v32(nocc, lanes), v32(2, nocc, lanes), v32(2, nocc, lanes),
            v32(nocc // 2, nvir, lanes), v32(zs, nocc // 2, nvir, lanes), v32(nocc // 2, nvir, lanes),
            v32(nocc, nvir, lanes), v32(nocc, nvir, lanes),
            v32(pairs, pairs),
            v32(nx, ny, nz, rows, pairs),
            v32(nx * nz, ny, rows, pairs),
            v32(ny, rows, pairs), v32(ny, rows, pairs),
            dma(28), dma(28), dma(6), dma(6), dma(4), dma(nx * nz), dma(nx * nz), dma(ny), dma(ny),
        ],
        compiler_params=pltpu.CompilerParams(
            collective_id=0, has_side_effects=True, vmem_limit_bytes=54 * MIB
        ),
        name="flow",
    )(*(pltpu.with_memory_space_constraint(flat(a), pltpu.HBM) for a in (occupied, virtual, kernel_fields, density_grad)))
    pot, casida = pl.pallas_call(
        write_kernel,
        out_shape=(sds(pairs * cells, lanes), sds(rows, pairs)),
        in_specs=[vmem] * 2,
        out_specs=(hbm, hbm),
        scratch_shapes=[dma(9)],
        compiler_params=pltpu.CompilerParams(vmem_limit_bytes=4 * MIB),
        name="write",
    )(*outs)
    return pot.reshape(pairs, bx, by, lanes), casida


def solution(mesh):
    spec = P(None, "gx", "gy", "gz")
    return jax.shard_map(
        on_device,
        mesh=mesh,
        in_specs=(spec,) * 4,
        out_specs=(spec, P(("gx", "gy", "gz"), None)),
        check_vma=False,
    )
```
